32 devices in a mesh: seq: 8 (over z, y), head: 4 (over x, core).
Axes of the slice: x: 2, y: 2, z: 4, core: 2. Of those that a mesh axis runs over, the one named last changes fastest.
Arguments:
- residual: bfloat16 [4096, 3072], P('seq', 'head'), may hold values from -6 to 6
- q_self: bfloat16 [4096, 3072], P('seq', 'head'), may hold values from -6 to 6
- k_self: bfloat16 [4096, 3072], P('seq', 'head'), may hold values from -6 to 6
- v_self: bfloat16 [4096, 3072], P('seq', 'head'), may hold values from -6 to 6
- w_out: bfloat16 [3072, 3072], P('head'), may hold values from -0.109375 to 0.109375
- norm_gain: float32 [3072], replicated, may hold values from 0.5 to 1.5
- w_query: bfloat16 [3072, 3072], P('seq', 'head')
- w_cache: bfloat16 [3072, 2048], P('seq', 'head')
- block_doc: int32 [8], replicated, may hold values from 0 to 2, never falling along the last dimension, each value on 1 to 4 neighbouring positions
- tail_len: int32 [8], replicated, may hold values from 1 to 512
Outputs:
- hidden: bfloat16 [4096, 3072], P('seq', 'head')
- cross_context: bfloat16 [4096, 3072], P('seq', 'head')
The draws below stay inside these ranges and needn't reach their ends.
Inputs may be any that keep to these rules, and one draw needn't show every extreme that they name: block_doc never falls along the blocks; each document covers 1 to 4 consecutive blocks, and some document covers exactly 4. `tail_len`: read only for the last block of a document.
All inputs are finite; a program needn't handle non-finite values.
Results may differ from the reference program's by a relative error of at most 0.0078.
Values may be sent and summed in bfloat16 or wider, within the bound.
A program may use at most 128 MiB of HBM per device.

```python
import math
import jax
import jax.numpy as jnp
import numpy as np
from jax import lax

D = 3072
HEADS = 24
KV_HEADS = 8
HEAD_DIM = 128
TOK_DEV = 512
WINDOW = 2048
DOC_MAX = 2560
WIN_BLOCKS = 4
DOC_BLOCKS = 5
NBLK = 8
TOKENS = 4096
SPAN_MAX = 4
DOC_COUNT = 3
N_HEAD = 4


def sign_vector(key, length):
    return jnp.where(jax.random.randint(key, (length,), 0, 2) == 0, -1.0, 1.0).astype(jnp.float32)


def picked_rows(key):
    every = max(2, TOK_DEV // 64)
    return jax.random.randint(key, (TOKENS,), 0, TOK_DEV) < every


def base_noise(key, shape):
    return jax.random.normal(jax.random.fold_in(key, 3), shape, jnp.float32)


def self_operand(key, member):
    width = HEADS * HEAD_DIM
    plan = jax.random.fold_in(key, 9001)
    picked = picked_rows(jax.random.fold_in(plan, 1))
    pattern = sign_vector(jax.random.fold_in(plan, 2), width)
    strength = jax.random.uniform(jax.random.fold_in(plan, 3), (TOKENS,), jnp.float32, 3.0, 5.5)
    spread = 0.4
    noise = base_noise(jax.random.fold_in(key, member), (TOKENS, width))
    aligned = strength[:, None] * pattern[None, :] + spread * noise
    mixed = jnp.where(picked[:, None], aligned, noise)
    return jnp.clip(mixed, -6.0, 6.0).astype(jnp.bfloat16)


def draw_q_self(key, part):
    return self_operand(key, 11)


def draw_k_self(key, part):
    return self_operand(key, 12)


def cross_patterns(key):
    plan = jax.random.fold_in(key, 9002)
    return (sign_vector(jax.random.fold_in(plan, 1), D), sign_vector(jax.random.fold_in(plan, 2), HEAD_DIM))


def draw_residual(key, part):
    feature_sign = cross_patterns(key)[0]
    plan = jax.random.fold_in(key, 9003)
    picked = picked_rows(jax.random.fold_in(plan, 1))
    strength = jax.random.uniform(jax.random.fold_in(plan, 2), (TOKENS,), jnp.float32, 2.0, 4.5)
    noise = base_noise(jax.random.fold_in(key, 13), (TOKENS, D))
    aligned = strength[:, None] * feature_sign[None, :] + 0.3 * noise
    mixed = jnp.where(picked[:, None], aligned, noise)
    return jnp.clip(mixed, -6.0, 6.0).astype(jnp.bfloat16)


def scaled_noise(key, columns):
    limit = 6.0 * D ** (-0.5)
    return jnp.clip(base_noise(key, (D, columns)) * D ** (-0.5), -limit, limit)


def draw_w_query(key, part):
    feature_sign, head_sign = cross_patterns(key)
    width = HEADS * HEAD_DIM
    noise = scaled_noise(jax.random.fold_in(key, 14), width)
    amounts = jax.random.uniform(jax.random.fold_in(key, 9005), (HEADS,), jnp.float32, 14.5, 24.5)
    columns = (amounts[:, None] * head_sign[None, :]).reshape(width)
    plant = feature_sign[:, None] * columns[None, :] / (D * HEAD_DIM ** 0.25)
    return (noise + plant).astype(jnp.bfloat16)


def draw_w_cache(key, part):
    feature_sign, head_sign = cross_patterns(key)
    group = KV_HEADS // N_HEAD
    width = 2 * KV_HEADS * HEAD_DIM
    noise = scaled_noise(jax.random.fold_in(key, 15), width)
    key_part = jnp.broadcast_to(16.0 * head_sign, (N_HEAD, group, HEAD_DIM))
    columns = jnp.stack([key_part, jnp.zeros_like(key_part)], axis=1).reshape(width)
    plant = feature_sign[:, None] * columns[None, :] / (D * HEAD_DIM ** 0.25)
    return (noise + plant).astype(jnp.bfloat16)


def with_ends(drawn, own_key, least, top_value):
    place = [jax.random.randint(jax.random.fold_in(own_key, axis), (), 0, length) for axis, length in enumerate(drawn.shape)]
    longest = drawn.shape.index(max(drawn.shape))
    next_to = place[:longest] + [(place[longest] + 1) % drawn.shape[longest]] + place[longest + 1:]
    return drawn.at[tuple(place)].set(least).at[tuple(next_to)].set(top_value)


def block_levels(own_key, shape, cuts, least, largest):
    factor_of = 1.0
    for axis_at, blocks in cuts:
        steps = jax.random.uniform(jax.random.fold_in(jax.random.fold_in(own_key, 6), axis_at), (blocks,), jnp.float32, least / len(cuts), largest / len(cuts))
        factor_of = factor_of * jnp.repeat(jnp.exp(steps), shape[axis_at] // blocks).reshape((-1,) + (1,) * (len(shape) - 1 - axis_at))
    return factor_of


def profile(count, total, most, lean):
    loads = [(1 << 20) // math.isqrt(standing ** lean) + 1 for standing in range(2, count + 1)]
    rest, holding = total - most - (count - 1), [1] * (count - 1)
    while rest > 0:
        free = [i for i in range(count - 1) if holding[i] < most]
        mass, remaining = sum([loads[i] for i in free]), rest
        for i in free:
            addition = min(most - holding[i], max(1, remaining * loads[i] // mass), rest)
            holding[i] = holding[i] + addition
            rest = rest - addition
    return np.array([most] + holding)


def uneven(own_key, amount, total, reach, lean):
    if amount == 2:
        one = jax.random.randint(own_key, (), max(1, total - reach), min(reach, total - 1) + 1)
        return jnp.stack([one, total - one])
    sizes = jnp.asarray(profile(amount, total, reach, lean), jnp.int32)
    pairs = (amount - 1) // 2
    giver, receiver = sizes[1:1 + 2 * pairs:2], sizes[2:2 + 2 * pairs:2]
    slack = jnp.minimum(giver - 1, reach - receiver)
    shifted = jax.random.randint(jax.random.fold_in(own_key, 1), (pairs,), 0, 1 << 20) % (slack + 1)
    sizes = sizes.at[1:1 + 2 * pairs:2].set(giver - shifted).at[2:2 + 2 * pairs:2].set(receiver + shifted)
    return sizes[jax.random.permutation(jax.random.fold_in(own_key, 2), amount)]


def bell_draw(stream_key, extent, scale, most, cuts=(), kind=jnp.bfloat16):
    entries = scale * jax.random.normal(stream_key, extent, jnp.float32)
    if cuts:
        entries = entries * block_levels(stream_key, extent, cuts, -0.22, 0.18)
    return jnp.clip(entries, -most, most).astype(kind)


def setup_inputs(seed: int = 0) -> dict:
    arg_keys = jax.random.split(jax.random.key(seed), 11)
    residual = draw_residual(jax.random.fold_in(arg_keys[10], 71), 0)
    q_self = draw_q_self(jax.random.fold_in(arg_keys[10], 71), 0)
    k_self = draw_k_self(jax.random.fold_in(arg_keys[10], 71), 0)
    v_self = bell_draw(arg_keys[3], (TOKENS, HEADS * HEAD_DIM), 1.0, 6.0, ((0, 8), (1, 4)))
    w_out = bell_draw(arg_keys[4], (HEADS * HEAD_DIM, D), (HEADS * HEAD_DIM) ** -0.5, 0.109375, ((0, 4),))
    norm_gain = jnp.clip(1.0 + 0.1 * jax.random.normal(arg_keys[5], (D,), jnp.float32), 0.5, 1.5)
    w_query = draw_w_query(jax.random.fold_in(arg_keys[10], 71), 0)
    w_cache = draw_w_cache(jax.random.fold_in(arg_keys[10], 71), 0)
    block_doc = jnp.searchsorted(jnp.cumsum(uneven(arg_keys[8], DOC_COUNT, NBLK, SPAN_MAX, 2)), jnp.arange(NBLK), side="right").astype(jnp.int32)
    tail_len = with_ends(jax.random.randint(arg_keys[9], (NBLK,), 1, TOK_DEV + 1), jax.random.fold_in(arg_keys[9], 1), 1, TOK_DEV).astype(jnp.int32)
    return dict(residual=residual, q_self=q_self, k_self=k_self, v_self=v_self, w_out=w_out, norm_gain=norm_gain, w_query=w_query, w_cache=w_cache, block_doc=block_doc, tail_len=tail_len)


EPSILON = 1e-06

def block_valid(block_doc, tail_len, tok_rows):
    following = jnp.concatenate([block_doc[1:], jnp.full((1,), -1, jnp.int32)])
    closing = following != block_doc
    within = jnp.arange(tok_rows, dtype=jnp.int32)
    return jnp.logical_or(jnp.logical_not(closing)[:, None], within[None, :] < tail_len[:, None])

def permitted(query_block, key_blocks, block_doc, valid_tokens, tok_rows, reach_tokens):
    inside = key_blocks >= 0
    safe_blocks = jnp.maximum(key_blocks, 0)
    own_doc = jnp.take(block_doc, query_block)
    same_doc = jnp.logical_and(inside, jnp.take(block_doc, safe_blocks) == own_doc)
    live_keys = jnp.logical_and(same_doc[:, None], jnp.take(valid_tokens, safe_blocks, axis=0))
    within = jnp.arange(tok_rows, dtype=jnp.int32)
    query_pos = query_block * tok_rows + within
    key_pos = (key_blocks[:, None] * tok_rows + within[None, :]).reshape(-1)
    distance = query_pos[:, None] - key_pos[None, :]
    near = jnp.logical_and(distance >= 0, distance < reach_tokens)
    return jnp.logical_and(near, live_keys.reshape(-1)[None, :])

def attend(queries, keys, values, allowed):
    row_count, head_count, head_dim = queries.shape
    group_size = head_count // keys.shape[1]
    scaling = 1.0 / math.sqrt(head_dim)

    def one_head(head_index):
        query_head = lax.dynamic_index_in_dim(queries, head_index, 1, keepdims=False)
        key_head = lax.dynamic_index_in_dim(keys, head_index // group_size, 1, keepdims=False)
        value_head = lax.dynamic_index_in_dim(values, head_index // group_size, 1, keepdims=False)
        scores = lax.dot_general(query_head, key_head, (((1,), (1,)), ((), ())), preferred_element_type=jnp.float32) * scaling
        scores = jnp.where(allowed, scores, -1e+30)
        row_peak = lax.optimization_barrier(jnp.max(scores, axis=1, keepdims=True))
        weights = jnp.exp(scores - row_peak)
        row_total = lax.optimization_barrier(jnp.sum(weights, axis=1, keepdims=True))
        blended = jnp.dot(weights.astype(jnp.bfloat16), value_head, preferred_element_type=jnp.float32)
        return (blended / row_total).astype(jnp.bfloat16)
    per_head = lax.map(one_head, jnp.arange(head_count, dtype=jnp.int32))
    return jnp.transpose(per_head, (1, 0, 2)).reshape(row_count, head_count * head_dim)

def reference(residual, q_self, k_self, v_self, w_out, norm_gain, w_query, w_cache, block_doc, tail_len):
    valid_tokens = block_valid(block_doc, tail_len, TOK_DEV)
    width_all = HEADS * HEAD_DIM
    win_rows = WIN_BLOCKS * TOK_DEV
    key_pad = jnp.concatenate([jnp.zeros((win_rows, width_all), jnp.bfloat16), k_self], axis=0)
    value_pad = jnp.concatenate([jnp.zeros((win_rows, width_all), jnp.bfloat16), v_self], axis=0)

    def self_block(block_index):
        row_start = block_index * TOK_DEV
        queries = lax.dynamic_slice_in_dim(q_self, row_start, TOK_DEV, 0).reshape(TOK_DEV, HEADS, HEAD_DIM)
        keys = lax.dynamic_slice_in_dim(key_pad, row_start, win_rows + TOK_DEV, 0).reshape(-1, HEADS, HEAD_DIM)
        values = lax.dynamic_slice_in_dim(value_pad, row_start, win_rows + TOK_DEV, 0).reshape(-1, HEADS, HEAD_DIM)
        key_blocks = block_index - WIN_BLOCKS + jnp.arange(WIN_BLOCKS + 1, dtype=jnp.int32)
        allowed = permitted(block_index, key_blocks, block_doc, valid_tokens, TOK_DEV, WINDOW)
        return attend(queries, keys, values, allowed)
    context = lax.map(self_block, jnp.arange(NBLK, dtype=jnp.int32)).reshape(TOKENS, width_all)
    projected = jnp.dot(context, w_out, preferred_element_type=jnp.float32)
    hidden = (residual.astype(jnp.float32) + projected).astype(jnp.bfloat16)
    wide = hidden.astype(jnp.float32)
    mean_square = lax.optimization_barrier(jnp.mean(wide * wide, axis=1, keepdims=True))
    normed = (wide * lax.rsqrt(mean_square + EPSILON) * norm_gain).astype(jnp.bfloat16)
    cross_queries = jnp.dot(normed, w_query, preferred_element_type=jnp.float32).astype(jnp.bfloat16)
    cache_rows = jnp.dot(normed, w_cache, preferred_element_type=jnp.float32).astype(jnp.bfloat16)
    cache_rows = cache_rows.reshape(TOKENS, N_HEAD, 2, KV_HEADS // N_HEAD, HEAD_DIM)
    cache_keys = cache_rows[:, :, 0].reshape(TOKENS, KV_HEADS * HEAD_DIM)
    cache_values = cache_rows[:, :, 1].reshape(TOKENS, KV_HEADS * HEAD_DIM)
    doc_rows = (DOC_BLOCKS - 1) * TOK_DEV
    cache_key_pad = jnp.concatenate([jnp.zeros((doc_rows, KV_HEADS * HEAD_DIM), jnp.bfloat16), cache_keys], axis=0)
    cache_value_pad = jnp.concatenate([jnp.zeros((doc_rows, KV_HEADS * HEAD_DIM), jnp.bfloat16), cache_values], axis=0)

    def cross_block(block_index):
        row_start = block_index * TOK_DEV
        queries = lax.dynamic_slice_in_dim(cross_queries, row_start, TOK_DEV, 0).reshape(TOK_DEV, HEADS, HEAD_DIM)
        keys = lax.dynamic_slice_in_dim(cache_key_pad, row_start, doc_rows + TOK_DEV, 0).reshape(-1, KV_HEADS, HEAD_DIM)
        values = lax.dynamic_slice_in_dim(cache_value_pad, row_start, doc_rows + TOK_DEV, 0).reshape(-1, KV_HEADS, HEAD_DIM)
        key_blocks = block_index - DOC_BLOCKS + 1 + jnp.arange(DOC_BLOCKS, dtype=jnp.int32)
        allowed = permitted(block_index, key_blocks, block_doc, valid_tokens, TOK_DEV, DOC_MAX)
        return attend(queries, keys, values, allowed)
    cross_context = lax.map(cross_block, jnp.arange(NBLK, dtype=jnp.int32)).reshape(TOKENS, width_all)
    return (hidden, cross_context)
```

```python
import functools
import math

import jax
import jax.numpy as jnp
from jax import lax
from jax.experimental import pallas as pl
from jax.experimental.pallas import tpu as pltpu
from jax.sharding import PartitionSpec as P

D = 3072
HEAD_DIM = 128
WINDOW = 2048
DOC_BLOCKS = 5
EPSILON = 1e-06
ROW_TILE = 256


def passed_along(block, axis, distance):
    devices = range(lax.axis_size(axis))
    route = [(i - distance, i) for i in devices if i - distance in devices]
    return lax.ppermute(block, axis, route)


def swapped(block, axis, flip):
    return lax.ppermute(block, axis, [(i, i ^ flip) for i in range(lax.axis_size(axis))])


MESH = pl.DeviceIdType.MESH
TILE = 256
NEG = -1e30
SCALE = math.log2(math.e) / math.sqrt(HEAD_DIM)

COPIES = (
    "ky", "vy", "qy", "kz", "vz", "kvz", "kvr", "wqy", "wky", "wvy", "wf1", "wf2", "wf3", "wb1", "wb1y",
    "wb2", "wb3", "wox", "woc", "wod", "cy", "cx0", "cc0", "cx1", "cc1", "cxc0", "cxc1", "dx0", "dx1", "dy0",
    "dy1", "dc0", "dc1", "dxc0", "dxc1", "dyc0", "dyc1", "dy2", "dx2", "dy2c", "dx2c", "e1", "e0", "er", "o0",
    "o1", "o2",
)
LOCALS = (
    "k", "v", "q", "wq", "wk", "wv", "res", "gain", "wo", "hid0", "hid1", "o0", "o1", "o2",
)


def fused_kernel(
    res_hbm, q_hbm, k_hbm, v_hbm, wo_hbm, gain_hbm, wq_hbm, wc_hbm, doc_ref, tail_ref,
    hid_hbm, out_hbm,
    qx, kv, acc, peak, wo, wfull, ctx, ctxo, hsum, hall, resv, gainv, proj, cq, kvc, outs,
    ss, rs, ls,
):
    s_at, h_at = lax.axis_index("seq"), lax.axis_index("head")
    seq_size = lax.axis_size("seq")
    planes = seq_size // 2
    z, y = s_at // 2, lax.rem(s_at, 2)
    yo = 1 - y
    c_at = lax.rem(h_at, 2)
    hx, hc = lax.rem(h_at + 2, 4), h_at + 1 - 2 * c_at
    hxc = lax.rem(hc + 2, 4)
    rows, width = q_hbm.shape
    half = width // 2
    heads = half // HEAD_DIM
    wrows = wq_hbm.shape[0]
    kvw = wc_hbm.shape[1] // 4
    cols = half + 2 * kvw
    to_y, to_x, to_c, to_d = (z * 2 + yo, h_at), (s_at, hx), (s_at, hc), (s_at, hxc)
    up, down = (s_at + 2, h_at), (s_at - 2, h_at)
    has_up, has_down = z < planes - 1, z > 0

    def part(at, size):
        return pl.ds(pl.multiple_of(at, size), size)

    def remote(name, src, dst, device):
        i = COPIES.index(name)
        return pltpu.make_async_remote_copy(
            src_ref=src, dst_ref=dst, send_sem=ss.at[i], recv_sem=rs.at[i],
            device_id=device, device_id_type=MESH,
        )

    def near(name, src, dst):
        return pltpu.make_async_copy(src, dst, ls.at[LOCALS.index(name)])

    sends = []

    def send(name, src, dst, device, cond=None):
        def go():
            remote(name, src, dst, device).start()

        if cond is None:
            go()
        else:
            pl.when(cond)(go)
        sends.append((name, src, dst, device, cond))

    def arrived(name, dst, cond=None):
        def go():
            remote(name, dst, dst, to_y).wait_recv()

        if cond is None:
            go()
        else:
            pl.when(cond)(go)

    mine, other = part(y * half, half), part(yo * half, half)
    kmine, kother = part(y * kvw, kvw), part(yo * kvw, kvw)
    vmine, vother = part((2 + y) * kvw, kvw), part((2 + yo) * kvw, kvw)
    kpart, vpart = pl.ds(0, half), pl.ds(half, half)
    wrow, wrow_y = part(s_at * wrows, wrows), part((z * 2 + yo) * wrows, wrows)
    wq_c, wk_c, wv_c = pl.ds(0, half), pl.ds(half, kvw), pl.ds(half + kvw, kvw)

    def wchunk(plane):
        return wfull.at[part(plane * 2 * wrows, 2 * wrows), :]

    barrier = pltpu.get_barrier_semaphore()
    for device in (to_y, to_x, to_c, to_d):
        pl.semaphore_signal(barrier, inc=1, device_id=device, device_id_type=MESH)

    @pl.when(has_up)
    def _():
        pl.semaphore_signal(barrier, inc=1, device_id=up, device_id_type=MESH)

    @pl.when(has_down)
    def _():
        pl.semaphore_signal(barrier, inc=1, device_id=down, device_id_type=MESH)

    locals_ = [
        ("k", k_hbm.at[:, mine], kv.at[y, :, kpart]),
        ("v", v_hbm.at[:, mine], kv.at[y, :, vpart]),
        ("q", q_hbm.at[:, mine], qx.at[y]),
        ("wq", wq_hbm.at[:, mine], wfull.at[wrow, wq_c]),
        ("wk", wc_hbm.at[:, kmine], wfull.at[wrow, wk_c]),
        ("wv", wc_hbm.at[:, vmine], wfull.at[wrow, wv_c]),
        ("res", res_hbm, resv),
        ("gain", gain_hbm, gainv),
        ("wo", wo_hbm.at[:, part(h_at * width, width)], wo.at[h_at]),
    ]
    for item in locals_:
        near(*item).start()
    pl.semaphore_wait(barrier, 4 + jnp.where(has_up, 1, 0) + jnp.where(has_down, 1, 0))

    send("ky", k_hbm.at[:, other], kv.at[y, :, kpart], to_y)
    send("kz", k_hbm.at[:, mine], kv.at[2 + y, :, kpart], up, has_up)
    send("vy", v_hbm.at[:, other], kv.at[y, :, vpart], to_y)
    send("vz", v_hbm.at[:, mine], kv.at[2 + y, :, vpart], up, has_up)
    send("qy", q_hbm.at[:, other], qx.at[y], to_y)
    send("wqy", wq_hbm.at[:, other], wfull.at[wrow, wq_c], to_y)
    send("wky", wc_hbm.at[:, kother], wfull.at[wrow, wk_c], to_y)
    send("wvy", wc_hbm.at[:, vother], wfull.at[wrow, wv_c], to_y)
    send("woc", wo_hbm.at[:, part(hc * width, width)], wo.at[h_at], to_c)
    send("wox", wo_hbm.at[:, part(hx * width, width)], wo.at[h_at], to_x)
    send("wod", wo_hbm.at[:, part(hxc * width, width)], wo.at[h_at], to_d)
    for item in locals_:
        if item[0] in ("k", "v", "q", "wq", "wk", "wv"):
            near(*item).wait()
    send("wb1", wfull.at[wrow, :], wfull.at[wrow, :], down, has_down)

    def block_of(j):
        return jnp.where(j < 2, 2 * z + j, jnp.where(j < 4, 2 * z - 4 + j, 2 * z - 3))

    def doc_of(block):
        return doc_ref[jnp.maximum(block, 0)]

    def live_of(block):
        following = jnp.minimum(block + 1, seq_size - 1)
        closing = jnp.logical_or(block == seq_size - 1, doc_ref[following] != doc_ref[block])
        return jnp.where(closing, jnp.minimum(tail_ref[block], rows), rows)

    ones = jnp.ones((rows, HEAD_DIM), jnp.bfloat16)

    def scores_of(q, k):
        return lax.dot_general(q, k, (((1,), (1,)), ((), ())), preferred_element_type=jnp.float32)

    def diag(queries, store, key_at, value_at, b):
        live = live_of(2 * z + b)
        for r in range(0, rows, TILE):
            here, keys = pl.ds(r, TILE), r + TILE
            for i in range(heads):
                k = store[b, pl.ds(0, keys), key_at(i)]
                v = store[b, pl.ds(0, keys), value_at(i)]
                s = scores_of(queries[b, here, pl.ds(i * HEAD_DIM, HEAD_DIM)], k)
                q_at = r + lax.broadcasted_iota(jnp.int32, s.shape, 0)
                k_at = lax.broadcasted_iota(jnp.int32, s.shape, 1)
                s = jnp.where((k_at <= q_at) & (k_at < live), s, NEG)
                top = jnp.max(s, axis=1, keepdims=True)
                w = jnp.exp2((s - top) * SCALE).astype(jnp.bfloat16)
                va = jnp.concatenate([v, ones[:keys]], axis=1)
                acc[b * heads + i, here, :] = jnp.dot(w, va, preferred_element_type=jnp.float32)
                peak[b * heads + i, here, :] = jnp.broadcast_to(top, (TILE, HEAD_DIM))

    def off(queries, store, key_at, value_at, b, j):
        same = doc_of(2 * z + b) == doc_of(block_of(j))
        on = jnp.where(same, 1.0, 0.0)
        gone = jnp.where(same, 0.0, 1e30)
        gain = jnp.where(same, SCALE, 0.0)

        def tile(t, carry):
            here = part(t * TILE, TILE)
            for i in range(heads):
                k = store[j, :, key_at(i)]
                v = store[j, :, value_at(i)]
                s = scores_of(queries[b, here, pl.ds(i * HEAD_DIM, HEAD_DIM)], k)
                top = jnp.max(s, axis=1, keepdims=True) * on - gone
                old = peak[b * heads + i, here, :]
                new = jnp.maximum(old, top)
                fade = jnp.exp2((old - new) * SCALE)
                w = jnp.exp2(s * gain - (new[:, :1] * gain + gone)).astype(jnp.bfloat16)
                va = jnp.concatenate([v, ones], axis=1)
                more = jnp.dot(w, va, preferred_element_type=jnp.float32)
                fades = jnp.concatenate([fade, fade], axis=1)
                acc[b * heads + i, here, :] = acc[b * heads + i, here, :] * fades + more
                peak[b * heads + i, here, :] = new
            return carry

        lax.fori_loop(0, rows // TILE, tile, 0)

    def finish(b, i):
        whole = acc[b * heads + i]
        return (whole[:, :HEAD_DIM] / whole[:, HEAD_DIM:]).astype(jnp.bfloat16)

    def head_cols(i):
        return pl.ds(i * HEAD_DIM, HEAD_DIM)

    self_at = (qx, kv, head_cols, lambda i: pl.ds(half + i * HEAD_DIM, HEAD_DIM))
    cross_at = (cq, kvc, lambda i: pl.ds(0, HEAD_DIM), lambda i: pl.ds(kvw, HEAD_DIM))

    diag(*self_at, y)
    arrived("ky", kv.at[yo, :, kpart])
    arrived("vy", kv.at[yo, :, vpart])
    send("kvz", kv.at[yo], kv.at[2 + yo], up, has_up)
    relay = jnp.logical_and(has_up, has_down)
    arrived("kz", kv.at[2 + y, :, kpart], has_down)
    arrived("vz", kv.at[2 + y, :, vpart], has_down)
    send_kvr = lambda cond: pl.when(cond)(
        lambda: remote("kvr", kv.at[3], kv.at[4], up).start()
    )
    send_kvr(jnp.logical_and(relay, y == 1))

    @pl.when(has_down)
    def _():
        off(*self_at, y, 2 + y)

    arrived("qy", qx.at[yo])
    diag(*self_at, yo)

    def second(i, carry):
        off(*self_at, jnp.where(i == 0, 1, yo), jnp.where(i == 0, 0, 2 + y))
        return carry

    lax.fori_loop(0, jnp.where(has_down, 2, 1), second, 0)
    arrived("kvz", kv.at[2 + yo], has_down)
    send_kvr(jnp.logical_and(relay, y == 0))
    sends.append(("kvr", kv.at[3], kv.at[4], up, relay))

    arrived("wqy", wfull.at[wrow_y, wq_c])
    arrived("wky", wfull.at[wrow_y, wk_c])
    arrived("wvy", wfull.at[wrow_y, wv_c])
    send("wb1y", wfull.at[wrow_y, :], wfull.at[wrow_y, :], down, has_down)
    send("wf1", wchunk(z), wchunk(z), up, has_up)

    @pl.when(has_down)
    def _():
        def third(b, carry):
            off(*self_at, b, 2 + yo)
            return carry

        lax.fori_loop(0, 2, third, 0)

    def context_out(b):
        @pl.when(b == y)
        def _():
            for i in range(heads):
                ctx[h_at * 2 + y, :, head_cols(i)] = finish(b, i)

        @pl.when(b != y)
        def _():
            for i in range(heads):
                ctxo[:, head_cols(i)] = finish(b, i)

    mine_c, from_y = ctx.at[h_at * 2 + y], ctx.at[h_at * 2 + yo]

    def context_send(b):
        @pl.when(b == y)
        def _():
            remote("cx0", mine_c, mine_c, to_x).start()
            remote("cc0", mine_c, mine_c, to_c).start()

        @pl.when(b != y)
        def _():
            remote("cy", ctxo, mine_c, to_y).start()

    context_out(1)
    context_send(1)
    far_down = z > 1
    arrived("kvr", kv.at[4], far_down)

    @pl.when(far_down)
    def _():
        off(*self_at, 0, 4)

    context_out(0)
    context_send(0)
    sends.append(("cx0", mine_c, mine_c, to_x, None))
    sends.append(("cc0", mine_c, mine_c, to_c, None))
    sends.append(("cy", ctxo, mine_c, to_y, None))

    last = planes - 1
    arrived("wb1", wfull.at[part(jnp.minimum(s_at + 2, seq_size - 1) * wrows, wrows), :], has_up)
    arrived("wb1y", wfull.at[part(jnp.minimum((z + 1) * 2 + yo, seq_size - 1) * wrows, wrows), :], has_up)
    send("wb2", wchunk(jnp.minimum(z + 1, last)), wchunk(jnp.minimum(z + 1, last)), down, relay)

    for item in locals_:
        if item[0] in ("res", "gain", "wo"):
            near(*item).wait()
    arrived("woc", wo.at[hc])
    arrived("wox", wo.at[hx])
    arrived("wod", wo.at[hxc])

    def project(ha, hb, side, first):
        def tile(t, carry):
            here = part(t * TILE, TILE)
            total = None if first else hsum[here, :]
            for h in (ha, hb):
                more = jnp.dot(
                    ctx[h * 2 + side, here, :], wo[h, part(side * half, half), :],
                    preferred_element_type=jnp.float32,
                )
                total = more if total is None else total + more
            hsum[here, :] = total
            return carry

        lax.fori_loop(0, rows // TILE, tile, 0)

    arrived("cy", from_y)
    send("cx1", from_y, from_y, to_x)
    send("cc1", from_y, from_y, to_c)
    arrived("cc0", ctx.at[hc * 2 + y])
    project(h_at, hc, y, True)
    arrived("cx0", ctx.at[hx * 2 + y])
    send("cxc0", ctx.at[hx * 2 + y], ctx.at[hx * 2 + y], to_c)
    arrived("cc1", ctx.at[hc * 2 + yo])
    project(h_at, hc, yo, False)
    arrived("cxc0", ctx.at[hxc * 2 + y])
    project(hx, hxc, y, False)
    arrived("cx1", ctx.at[hx * 2 + yo])
    send("cxc1", ctx.at[hx * 2 + yo], ctx.at[hx * 2 + yo], to_c)
    arrived("cxc1", ctx.at[hxc * 2 + yo])

    top = rows // 2

    def hpart(b, h, p):
        return hall.at[b, h, pl.ds(p * top, top), :]

    for p in range(2):
        here = pl.ds(p * top, top)
        total = hsum[here, :]
        for h in (hx, hxc):
            total += jnp.dot(
                ctx[h * 2 + yo, here, :], wo[h, part(yo * half, half), :],
                preferred_element_type=jnp.float32,
            )
        hall[y, h_at, here, :] = (resv[here, :].astype(jnp.float32) + total).astype(jnp.bfloat16)
        piece = hpart(y, h_at, p)
        send(f"dx{p}", piece, piece, to_x)
        send(f"dy{p}", piece, piece, to_y)
        send(f"dc{p}", piece, piece, to_c)
        near(f"hid{p}", piece, hid_hbm.at[here, :]).start()

    mid = jnp.logical_and(has_down, has_up)
    behind = jnp.maximum(z - 1, 0)
    arrived("wf1", wchunk(behind), has_down)
    send("wf2", wchunk(behind), wchunk(behind), up, mid)
    ahead2 = jnp.minimum(z + 2, last)
    arrived("wb2", wchunk(ahead2), z + 2 <= last)
    send("wb3", wchunk(ahead2), wchunk(ahead2), down, jnp.logical_and(z + 2 <= last, has_down))

    arrived("dx0", hpart(y, hx, 0))
    send("dxc0", hpart(y, hx, 0), hpart(y, hx, 0), to_c)
    arrived("dy0", hpart(yo, h_at, 0))
    send("dyc0", hpart(yo, h_at, 0), hpart(yo, h_at, 0), to_c)
    send("dy2", hpart(y, hx, 0), hpart(y, hx, 0), to_y)
    arrived("dy1", hpart(yo, h_at, 1))
    send("dx2", hpart(yo, h_at, 1), hpart(yo, h_at, 1), to_x)
    send("dyc1", hpart(yo, h_at, 1), hpart(yo, h_at, 1), to_c)
    arrived("dx1", hpart(y, hx, 1))
    send("dxc1", hpart(y, hx, 1), hpart(y, hx, 1), to_c)

    behind2 = jnp.maximum(z - 2, 0)
    arrived("wf2", wchunk(behind2), z >= 2)
    send("wf3", wchunk(behind2), wchunk(behind2), up, jnp.logical_and(z >= 2, has_up))

    arrived("dy2", hpart(yo, hx, 0))
    send("dy2c", hpart(yo, hx, 0), hpart(yo, hx, 0), to_c)
    arrived("dx2", hpart(yo, hx, 1))
    send("dx2c", hpart(yo, hx, 1), hpart(yo, hx, 1), to_c)
    for p in range(2):
        arrived(f"dc{p}", hpart(y, hc, p))
        arrived(f"dxc{p}", hpart(y, hxc, p))
        arrived(f"dyc{p}", hpart(yo, hc, p))
    arrived("dy2c", hpart(yo, hxc, 0))
    arrived("dx2c", hpart(yo, hxc, 1))
    early = [item for item in sends if item[0][0] == "d"]
    for name, src, dst, device, cond in early:
        remote(name, src, dst, device).wait_send()
    for p in range(2):
        near(f"hid{p}", hpart(y, h_at, p), hid_hbm.at[pl.ds(p * top, top), :]).wait()

    ntile = 128

    def norm(n, carry):
        b, t = n // (rows // ntile), lax.rem(n, rows // ntile)
        here = part(t * ntile, ntile)
        square = jnp.zeros((ntile, 1), jnp.float32)
        for h in range(hall.shape[1]):
            wide = hall[b, h, here, :].astype(jnp.float32)
            square += jnp.sum(wide * wide, axis=1, keepdims=True)
        scale = lax.rsqrt(square / D + EPSILON)
        for h in range(hall.shape[1]):
            wide = hall[b, h, here, :].astype(jnp.float32)
            gains = gainv[h:h + 1, :]
            hall[b, h, here, :] = (wide * scale * gains).astype(jnp.bfloat16)
        return carry

    lax.fori_loop(0, 2 * (rows // ntile), norm, 0)

    def cross_part(k, b, where, first):
        def tile(t, carry):
            here = part(t * TILE, TILE)
            more = jnp.dot(
                hall[b, k, here, :], wfull[part(k * 2 * wrows, 2 * wrows), where],
                preferred_element_type=jnp.float32,
            )
            proj[b, here, where] = more if first else proj[b, here, where] + more
            return carry

        lax.fori_loop(0, rows // TILE, tile, 0)

    def both(k, first):
        def one(b, carry):
            cross_part(k, b, pl.ds(0, cols), first)
            return carry

        lax.fori_loop(0, 2, one, 0)

    low = z < planes // 2
    order = [z, jnp.where(low, 1 - z, 5 - z), jnp.where(low, 2, 1), jnp.where(low, 3, 0)]
    both(order[0], True)
    both(order[1], False)
    both(order[2], False)
    arrived("wf3", wchunk(0), z == last)
    arrived("wb3", wchunk(last), z == 0)

    cache_c, query_c = pl.ds(half, 2 * kvw), pl.ds(0, half)

    def cache_out(b):
        cross_part(order[3], b, cache_c, False)
        kvc[b] = proj[b, :, cache_c].astype(jnp.bfloat16)

    cache_out(1)
    send("e1", kvc.at[1], kvc.at[3], up, has_up)
    cache_out(0)
    send("e0", kvc.at[0], kvc.at[2], up, has_up)

    def query_out(b, carry):
        cross_part(order[3], b, query_c, False)
        cq[b] = proj[b, :, query_c].astype(jnp.bfloat16)
        return carry

    lax.fori_loop(0, 2, query_out, 0)

    def own_diag(b, carry):
        diag(*cross_at, b)
        return carry

    lax.fori_loop(0, 2, own_diag, 0)
    arrived("e1", kvc.at[3], has_down)
    send("er", kvc.at[3], kvc.at[4], up, relay)
    off(*cross_at, 1, 0)

    @pl.when(has_down)
    def _():
        def step(b, carry):
            off(*cross_at, b, 3)
            return carry

        lax.fori_loop(0, 2, step, 0)

    arrived("e0", kvc.at[2], has_down)

    @pl.when(has_down)
    def _():
        def step(b, carry):
            off(*cross_at, b, 2)
            return carry

        lax.fori_loop(0, 2, step, 0)

    def out_cols(i):
        return part(y * half + i * HEAD_DIM, HEAD_DIM)

    def result(b):
        for i in range(heads):
            outs[b, i] = finish(b, i)

            @pl.when(b == y)
            def _():
                near(f"o{i}", outs.at[b, i], out_hbm.at[:, out_cols(i)]).start()

            @pl.when(b != y)
            def _():
                remote(f"o{i}", outs.at[b, i], out_hbm.at[:, out_cols(i)], to_y).start()

    result(1)
    arrived("er", kvc.at[4], far_down)

    @pl.when(far_down)
    def _():
        off(*cross_at, 0, 4)

    result(0)
    for i in range(heads):
        near(f"o{i}", outs.at[y, i], out_hbm.at[:, out_cols(i)]).wait()
        remote(f"o{i}", outs.at[yo, i], out_hbm.at[:, out_cols(i)], to_y).wait_send()
        arrived(f"o{i}", out_hbm.at[:, part(yo * half + i * HEAD_DIM, HEAD_DIM)])
    for name, src, dst, device, cond in sends:
        if name[0] == "d":
            continue
        done = remote(name, src, dst, device).wait_send
        if cond is None:
            done()
        else:
            pl.when(cond)(done)


def fused(residual, q_self, k_self, v_self, w_out, norm_gain, w_query, w_cache, block_doc, tail_len):
    rows, width = q_self.shape
    seq_size, head_size = lax.axis_size("seq"), lax.axis_size("head")
    half = width // 2
    heads = half // HEAD_DIM
    kvw = w_cache.shape[1] // 4
    cols = half + 2 * kvw
    bf, f32 = jnp.bfloat16, jnp.float32
    hbm = pl.BlockSpec(memory_space=pl.ANY)
    smem = pl.BlockSpec(memory_space=pltpu.SMEM)
    scratch = [
        pltpu.VMEM((2, rows, half), bf),
        pltpu.VMEM((5, rows, 2 * half), bf),
        pltpu.VMEM((2 * heads, rows, 2 * HEAD_DIM), f32),
        pltpu.VMEM((2 * heads, rows, HEAD_DIM), f32),
        pltpu.VMEM((head_size, width, width), bf),
        pltpu.VMEM((w_query.shape[0] * seq_size, cols), bf),
        pltpu.VMEM((2 * head_size, rows, half), bf),
        pltpu.VMEM((rows, half), bf),
        pltpu.VMEM((rows, width), f32),
        pltpu.VMEM((2, head_size, rows, width), bf),
        pltpu.VMEM((rows, width), bf),
        pltpu.VMEM((head_size, width), f32),
        pltpu.VMEM((2, rows, cols), f32),
        pltpu.VMEM((2, rows, half), bf),
        pltpu.VMEM((5, rows, 2 * kvw), bf),
        pltpu.VMEM((2, heads, rows, HEAD_DIM), bf),
        pltpu.SemaphoreType.DMA((len(COPIES),)),
        pltpu.SemaphoreType.DMA((len(COPIES),)),
        pltpu.SemaphoreType.DMA((len(LOCALS),)),
    ]
    wide = jax.ShapeDtypeStruct((rows, width), bf)
    return pl.pallas_call(
        fused_kernel,
        out_shape=(wide, wide),
        in_specs=[hbm] * 8 + [smem] * 2,
        out_specs=(hbm, hbm),
        scratch_shapes=scratch,
        compiler_params=pltpu.CompilerParams(
            collective_id=0, has_side_effects=True, vmem_limit_bytes=60 * 1024 * 1024
        ),
    )(
        residual, q_self, k_self, v_self, w_out, norm_gain.reshape(head_size, width),
        w_query, w_cache, block_doc, tail_len,
    )


def stage_kernel(offsets, window, first, last, facts, q_ref, *refs):
    pairs = [(refs[2 * i], refs[2 * i + 1]) for i in range(len(offsets))]
    rest = refs[2 * len(offsets):]
    if not first:
        acc_in, peak_in, total_in = rest[:3]
        rest = rest[3:]
    if last:
        out_ref = rest[0]
        acc, peak, total = rest[1:]
    else:
        acc, peak, total = rest
    rows = q_ref.shape[0]
    tile = min(ROW_TILE, rows)
    scaling = math.log2(math.e) / math.sqrt(HEAD_DIM)

    def scores_of(r, k):
        return lax.dot_general(
            q_ref[pl.ds(r, tile), :], k, (((1,), (1,)), ((), ())),
            preferred_element_type=jnp.float32,
        )

    if not first:
        acc[...] = acc_in[...]
        peak[...] = peak_in[...]
        total[...] = total_in[...]

    for (k_ref, v_ref), (flag, offset) in zip(pairs, offsets):

        def one(offset=offset, k_ref=k_ref, v_ref=v_ref):
            for r in range(0, rows, tile):
                here = pl.ds(r, tile)
                keys = r + tile if offset == 0 else rows
                s = scores_of(r, k_ref[pl.ds(0, keys), :])
                if offset == 0:
                    q_at = r + lax.broadcasted_iota(jnp.int32, s.shape, 0)
                    k_at = lax.broadcasted_iota(jnp.int32, s.shape, 1)
                    s = jnp.where((k_at <= q_at) & (k_at < facts[0]), s, -1e30)
                elif offset * rows + rows - 1 >= window:
                    q_at = r + lax.broadcasted_iota(jnp.int32, s.shape, 0)
                    k_at = lax.broadcasted_iota(jnp.int32, s.shape, 1)
                    s = jnp.where(offset * rows + q_at - k_at < window, s, -1e30)
                top = jnp.max(s, axis=1, keepdims=True)
                if offset == 0:
                    w = jnp.exp2((s - top) * scaling)
                    part = jnp.dot(
                        w.astype(jnp.bfloat16), v_ref[pl.ds(0, keys), :],
                        preferred_element_type=jnp.float32,
                    )
                    acc[here, :] = part
                    total[here, :] = jnp.broadcast_to(
                        jnp.sum(w, axis=1, keepdims=True), (tile, HEAD_DIM)
                    )
                    peak[here, :] = jnp.broadcast_to(top, (tile, HEAD_DIM))
                else:
                    old = peak[here, :]
                    new = jnp.maximum(old, top)
                    w = jnp.exp2((s - new[:, :1]) * scaling)
                    fade = jnp.exp2((old - new) * scaling)
                    part = jnp.dot(
                        w.astype(jnp.bfloat16), v_ref[...], preferred_element_type=jnp.float32
                    )
                    acc[here, :] = acc[here, :] * fade + part
                    total[here, :] = total[here, :] * fade + jnp.sum(w, axis=1, keepdims=True)
                    peak[here, :] = new

        if offset == 0:
            one()
        else:
            pl.when(facts[flag] > 0)(one)

    if last:
        out_ref[...] = (acc[...] / total[...]).astype(jnp.bfloat16)


def attend_stage(facts, queries, blocks, offsets, kv_heads, state, window, last):
    rows, width = queries.shape
    heads = width // HEAD_DIM
    group = heads // kv_heads
    tall = pl.BlockSpec((rows, HEAD_DIM), lambda h, f: (0, h))
    key_spec = pl.BlockSpec((rows, HEAD_DIM), lambda h, f: (0, h // group))
    value_spec = pl.BlockSpec((rows, HEAD_DIM), lambda h, f: (0, kv_heads + h // group))
    operands, specs = [queries], [tall]
    for block in blocks:
        operands += [block, block]
        specs += [key_spec, value_spec]
    if state is not None:
        operands += list(state)
        specs += [tall] * 3
    wide = jax.ShapeDtypeStruct((rows, width), jnp.float32)
    if last:
        out_shape = jax.ShapeDtypeStruct((rows, width), jnp.bfloat16)
        out_specs = tall
        scratch = [pltpu.VMEM((rows, HEAD_DIM), jnp.float32)] * 3
    else:
        out_shape, out_specs, scratch = (wide,) * 3, (tall,) * 3, []
    flops = 4 * rows * rows * width * len(offsets) * 3
    return pl.pallas_call(
        functools.partial(stage_kernel, offsets, window, state is None, last),
        out_shape=out_shape,
        grid_spec=pltpu.PrefetchScalarGridSpec(
            num_scalar_prefetch=1, grid=(heads,), in_specs=specs, out_specs=out_specs,
            scratch_shapes=scratch,
        ),
        compiler_params=pltpu.CompilerParams(
            dimension_semantics=("arbitrary",), vmem_limit_bytes=32 * 1024 * 1024
        ),
        cost_estimate=pl.CostEstimate(
            flops=flops, bytes_accessed=rows * width * 2 * (2 + 2 * len(offsets)),
            transcendentals=0,
        ),
    )(facts, *operands)


def shared_over_head(block):
    size = lax.axis_size("head")
    held = [block]
    step = size // 2
    got = {0: block}
    while step >= 1:
        for flip in sorted(got):
            got[flip ^ step] = None if got[flip] is None else swapped(got[flip], "head", step)
        step //= 2
    held = [got[flip] for flip in range(size)]
    return held


def sent(block, routes):
    return lax.ppermute(block, "seq", routes)


def row_gather(block):
    size = lax.axis_size("seq")
    me = lax.axis_index("seq")
    ring = [(i, (i + 2) % size) for i in range(size)]
    steps = []
    moving = block
    for step in range(size // 2):
        owner = lax.rem(me - 2 * step + size, size)
        across = swapped(moving, "seq", 1)
        onward = sent(moving, ring) if step + 1 < size // 2 else None
        moving, across, onward = yield moving, across, onward, owner
        moving = onward


def placed(whole, piece, owner):
    return lax.dynamic_update_slice_in_dim(whole, piece, owner * piece.shape[0], 0)


def waves(block, odd, beside):
    size = lax.axis_size("seq")
    first = sent(block, [(i, i + 1) for i in range(size - 1)])
    second_even = sent(block, [(i, i + 2) for i in range(0, size - 2, 2)])
    if beside is not None:
        first, beside = lax.optimization_barrier((first, beside))
    mixed = jnp.where(odd, block, first)
    second = sent(mixed, [(i, i + 2) for i in range(size - 2)])
    third_odd = sent(second_even, [(i, i + 1) for i in range(2, size, 2)])
    return first, [second_even, second, third_odd], beside


def fits(q_self, w_cache):
    seq_size, head_size = lax.axis_size("seq"), lax.axis_size("head")
    return (
        seq_size == 8 and head_size == 4 and q_self.shape[1] == 6 * HEAD_DIM
        and w_cache.shape[1] == 4 * HEAD_DIM and q_self.shape[0] % TILE == 0
    )


def local(
    residual, q_self, k_self, v_self, w_out, norm_gain, w_query, w_cache, block_doc, tail_len
):
    rows, width = q_self.shape
    local_heads = width // HEAD_DIM
    if fits(q_self, w_cache):
        return fused(
            residual, q_self, k_self, v_self, w_out, norm_gain, w_query, w_cache, block_doc, tail_len
        )
    local_kv = w_cache.shape[1] // (2 * HEAD_DIM)
    seq_size, head_size = lax.axis_size("seq"), lax.axis_size("head")
    span = min(DOC_BLOCKS, seq_size // 2)
    far = list(range(1, span))
    me, my_head = lax.axis_index("seq"), lax.axis_index("head")

    own_doc = block_doc[me]
    following = jnp.where(me == seq_size - 1, -1, block_doc[jnp.minimum(me + 1, seq_size - 1)])
    live = jnp.where(following != own_doc, jnp.minimum(tail_len[me], rows), rows)
    odd = lax.rem(me, 2) == 1
    small = span == 4 and seq_size % 2 == 0

    def together(distance):
        other = me - distance
        return jnp.logical_and(other >= 0, block_doc[jnp.maximum(other, 0)] == own_doc)

    if small:
        flags = [
            together(1),
            jnp.logical_and(jnp.logical_not(odd), together(2)),
            jnp.where(odd, together(2), together(3)),
            jnp.logical_and(odd, together(3)),
        ]
        distances = [1, 2, 3, 3]
    else:
        flags = [together(distance) for distance in far]
        distances = far
    facts = jnp.stack([live.astype(jnp.int32)] + [flag.astype(jnp.int32) for flag in flags])
    slots = [(1 + i, distance) for i, distance in enumerate(distances)]

    stacked = jnp.concatenate([k_self, v_self], axis=1)
    weight_rows = jnp.concatenate([w_query, w_cache], axis=1)
    state = attend_stage(facts, q_self, [stacked], [(0, 0)], local_heads, None, WINDOW, False)
    if small:
        near, late, state = waves(stacked, odd, state)
    else:
        near, *late = [passed_along(stacked, "seq", offset) for offset in far]

    own_columns = residual.shape[1]
    out_pieces = []
    for flip in range(head_size):
        piece = lax.dynamic_slice_in_dim(w_out, (my_head ^ flip) * own_columns, own_columns, 1)
        out_pieces.append(piece if flip == 0 else swapped(piece, "head", flip))

    state = attend_stage(facts, q_self, [near], slots[:1], local_heads, state, WINDOW, False)
    if small:
        weight_rows, state = lax.optimization_barrier((weight_rows, state))
        weights = jnp.zeros((weight_rows.shape[0] * seq_size, weight_rows.shape[1]), jnp.bfloat16)
        gather = row_gather(weight_rows)
        moving, across, onward, owner = next(gather)
        late, across, onward, out_pieces = lax.optimization_barrier(
            (late, across, onward, out_pieces)
        )
        weights = placed(placed(weights, moving, owner), across, owner ^ 1)
        moving, across, onward, owner = gather.send((moving, across, onward))
    else:
        weights = lax.all_gather(weight_rows, "seq", axis=0, tiled=True)
    context = attend_stage(facts, q_self, late, slots[1:], local_heads, state, WINDOW, True)
    if small:
        context, across, onward = lax.optimization_barrier((context, across, onward))
        weights = placed(placed(weights, moving, owner), across, owner ^ 1)
        moving, across, onward, owner = gather.send((moving, across, onward))

    contexts = shared_over_head(context)
    projected = jnp.dot(contexts[0], out_pieces[0], preferred_element_type=jnp.float32)
    for flip in range(1, head_size):
        projected += jnp.dot(contexts[flip], out_pieces[flip], preferred_element_type=jnp.float32)
    hidden = (residual.astype(jnp.float32) + projected).astype(jnp.bfloat16)
    if small:
        hidden, across, onward = lax.optimization_barrier((hidden, across, onward))
        weights = placed(placed(weights, moving, owner), across, owner ^ 1)
        while onward is not None:
            moving, across, onward, owner = gather.send((moving, across, onward))
            weights = placed(placed(weights, moving, owner), across, owner ^ 1)

    full = jnp.zeros((rows, own_columns * head_size), jnp.bfloat16)
    for flip, piece in enumerate(shared_over_head(hidden)):
        full = lax.dynamic_update_slice_in_dim(full, piece, (my_head ^ flip) * own_columns, 1)
    wide = full.astype(jnp.float32)
    mean_square = jnp.sum(wide * wide, axis=1, keepdims=True) / D
    normed = (wide * lax.rsqrt(mean_square + EPSILON) * norm_gain).astype(jnp.bfloat16)

    cache_rows = jnp.dot(
        normed, weights[:, width:], preferred_element_type=jnp.float32
    ).astype(jnp.bfloat16)
    if small:
        near, late, _ = waves(cache_rows, odd, None)
    else:
        near, *late = [passed_along(cache_rows, "seq", offset) for offset in far]
    cross_queries = jnp.dot(
        normed, weights[:, :width], preferred_element_type=jnp.float32
    ).astype(jnp.bfloat16)
    reach = DOC_BLOCKS * rows
    state = attend_stage(
        facts, cross_queries, [cache_rows, near], [(0, 0)] + slots[:1], local_kv, None, reach, False
    )
    cross_context = attend_stage(
        facts, cross_queries, late, slots[1:], local_kv, state, reach, True
    )
    return (hidden, cross_context)


def solution(mesh):
    in_specs = (
        P("seq", "head"),
        P("seq", "head"),
        P("seq", "head"),
        P("seq", "head"),
        P("head", None),
        P(),
        P("seq", "head"),
        P("seq", "head"),
        P(),
        P(),
    )
    out_specs = (P("seq", "head"), P("seq", "head"))
    return jax.shard_map(local, mesh=mesh, in_specs=in_specs, out_specs=out_specs, check_vma=False)
```

```python
import functools
import math

import jax
import jax.numpy as jnp
import numpy as np
from jax import lax
from jax.experimental import pallas as pl
from jax.experimental.pallas import tpu as pltpu
from jax.sharding import PartitionSpec as P

D = 3072
HEAD_DIM = 128
WINDOW = 2048
DOC_BLOCKS = 5
EPSILON = 1e-06
ROW_TILE = 256


def passed_along(block, axis, distance):
    devices = range(lax.axis_size(axis))
    route = [(i - distance, i) for i in devices if i - distance in devices]
    return lax.ppermute(block, axis, route)


def swapped(block, axis, flip):
    return lax.ppermute(block, axis, [(i, i ^ flip) for i in range(lax.axis_size(axis))])


MESH = pl.DeviceIdType.MESH
TILE = 256
NEG = -1e30
SCALE = math.log2(math.e) / math.sqrt(HEAD_DIM)

BY_HEAD = ("ky", "vy", "qy", "kz", "vz", "kvz", "kvr", "cy", "cc", "cyc", "o")
COPIES = (
    "wqy", "wky", "wvy", "wf1", "wf1y", "wf2", "wf2y", "wf3", "wf3y",
    "wb1", "wb1y", "wb2", "wb2y", "wb3", "wb3y", "woc0", "woc1",
    "px0", "px1", "dx0", "dx1", "dy0", "dy1", "dc0", "dc1", "dxc0", "dxc1", "dyc0", "dyc1",
    "dy2", "dx2", "dy2c", "dx2c", "e1", "e0", "er",
)
LOCALS = ("wq", "wk", "wv", "res", "gain", "wo0", "wo1", "hid0", "hid1")
LOCALS_BY_HEAD = ("k", "v", "q", "o")


def fused_kernel(
    far, res_hbm, q_hbm, k_hbm, v_hbm, wo_hbm, gain_hbm, wq_hbm, wc_hbm, doc_ref, tail_ref,
    hid_hbm, out_hbm,
    qx, kv, acc, peak, wo, wfull, ctx, ctxo, po, px, pxb, pxr, hall, nrm, resv, gainv, proj, cq, kvc, outs,
    ss, rs, ls,
):
    s_at, h_at = lax.axis_index("seq"), lax.axis_index("head")
    seq_size = lax.axis_size("seq")
    planes = seq_size // 2
    last = planes - 1
    z, y = s_at // 2, lax.rem(s_at, 2)
    yo = 1 - y
    c_at = lax.rem(h_at, 2)
    co = 1 - c_at
    hx, hc = lax.rem(h_at + 2, 4), h_at + 1 - 2 * c_at
    hxc = lax.rem(hc + 2, 4)
    rows, width = q_hbm.shape
    half = width // 2
    heads = half // HEAD_DIM
    wrows = wq_hbm.shape[0]
    kvw = wc_hbm.shape[1] // 4
    cols = half + 2 * kvw
    top = rows // 2
    to_y, to_x, to_c = (z * 2 + yo, h_at), (s_at, hx), (s_at, hc)
    up, down = (s_at + 2, h_at), (s_at - 2, h_at)
    has_up, has_down = z < last, z > 0
    mid = jnp.logical_and(has_up, has_down)
    far_down = z > 1

    def part(at, size):
        return pl.ds(pl.multiple_of(at, size), size)

    def index_of(name, i):
        if i is None:
            return len(BY_HEAD) * heads + COPIES.index(name)
        return BY_HEAD.index(name) * heads + i

    def remote(name, src, dst, device, i=None):
        at = index_of(name, i)
        return pltpu.make_async_remote_copy(
            src_ref=src, dst_ref=dst, send_sem=ss.at[at], recv_sem=rs.at[at],
            device_id=device, device_id_type=MESH,
        )

    def near(name, src, dst, i=None):
        at = LOCALS.index(name) if i is None else len(LOCALS) + LOCALS_BY_HEAD.index(name) * heads + i
        return pltpu.make_async_copy(src, dst, ls.at[at])

    def when(cond, go):
        if cond is None:
            go()
        else:
            pl.when(cond)(go)

    sends = []

    def send(name, src, dst, device, cond=None):
        when(cond, lambda: remote(name, src, dst, device).start())
        sends.append((name, src, dst, device, cond))

    def arrived(name, dst, cond=None, i=None):
        def go():
            remote(name, dst, dst, to_y, i).wait_recv()

        when(cond, go)

    def each_head(body):
        def step(i, carry):
            body(i)
            return carry

        lax.fori_loop(0, heads, step, 0)

    mine, other = part(y * half, half), part(yo * half, half)
    kmine, kother = part(y * kvw, kvw), part(yo * kvw, kvw)
    vmine, vother = part((2 + y) * kvw, kvw), part((2 + yo) * kvw, kvw)
    wrow, wrow_y = part(s_at * wrows, wrows), part((z * 2 + yo) * wrows, wrows)
    wq_c, wk_c, wv_c = pl.ds(0, half), pl.ds(half, kvw), pl.ds(half + kvw, kvw)

    def wchunk(plane):
        return wfull.at[part(plane * 2 * wrows, 2 * wrows), :]

    def own_head(i):
        return part(y * half + i * HEAD_DIM, HEAD_DIM)

    def other_head(i):
        return part(yo * half + i * HEAD_DIM, HEAD_DIM)

    def head_cols(i):
        return part(i * HEAD_DIM, HEAD_DIM)

    barrier = pltpu.get_barrier_semaphore()
    for device in (to_y, to_x, to_c):
        pl.semaphore_signal(barrier, inc=1, device_id=device, device_id_type=MESH)

    @pl.when(has_up)
    def _():
        pl.semaphore_signal(barrier, inc=1, device_id=up, device_id_type=MESH)

    @pl.when(has_down)
    def _():
        pl.semaphore_signal(barrier, inc=1, device_id=down, device_id_type=MESH)

    locals_ = [
        ("wq", wq_hbm.at[:, mine], wfull.at[wrow, wq_c]),
        ("wk", wc_hbm.at[:, kmine], wfull.at[wrow, wk_c]),
        ("wv", wc_hbm.at[:, vmine], wfull.at[wrow, wv_c]),
        ("wo0", wo_hbm.at[:, part(h_at * width, width)], wo.at[c_at, 0]),
        ("wo1", wo_hbm.at[:, part(hx * width, width)], wo.at[c_at, 1]),
        ("res", res_hbm, resv),
        ("gain", gain_hbm, gainv),
    ]

    def local_kvq(i):
        return [
            near("k", k_hbm.at[:, own_head(i)], kv.at[y, i, 0], i),
            near("v", v_hbm.at[:, own_head(i)], kv.at[y, i, 1], i),
            near("q", q_hbm.at[:, own_head(i)], qx.at[y, i], i),
        ]

    for i in range(heads):
        for copy in local_kvq(i):
            copy.start()
    for item in locals_:
        near(*item).start()
    pl.semaphore_wait(barrier, 3 + jnp.where(has_up, 1, 0) + jnp.where(has_down, 1, 0))

    def first_sends(i):
        return [
            (remote("ky", k_hbm.at[:, other_head(i)], kv.at[y, i, 0], to_y, i), None),
            (remote("vy", v_hbm.at[:, other_head(i)], kv.at[y, i, 1], to_y, i), None),
            (remote("qy", q_hbm.at[:, other_head(i)], qx.at[y, i], to_y, i), None),
            (remote("kz", k_hbm.at[:, own_head(i)], kv.at[2 + y, i, 0], up, i), has_up),
            (remote("vz", v_hbm.at[:, own_head(i)], kv.at[2 + y, i, 1], up, i), has_up),
        ]

    for i in range(heads):
        for copy, cond in first_sends(i):
            when(cond, copy.start)
    send("wqy", wq_hbm.at[:, other], wfull.at[wrow, wq_c], to_y)
    send("wky", wc_hbm.at[:, kother], wfull.at[wrow, wk_c], to_y)
    send("wvy", wc_hbm.at[:, vother], wfull.at[wrow, wv_c], to_y)
    send("woc0", wo_hbm.at[:, part(hc * width, width)], wo.at[c_at, 0], to_c)
    send("woc1", wo_hbm.at[:, part(hxc * width, width)], wo.at[c_at, 1], to_c)
    for item in locals_[:3]:
        near(*item).wait()
    send("wb1", wfull.at[wrow, :], wfull.at[wrow, :], down, has_down)

    def block_of(j):
        return jnp.where(j < 2, 2 * z + j, jnp.where(j < 4, 2 * z - 4 + j, 2 * z - 3))

    def doc_of(block):
        return doc_ref[jnp.maximum(block, 0)]

    def live_of(block):
        following = jnp.minimum(block + 1, seq_size - 1)
        closing = jnp.logical_or(block == seq_size - 1, doc_ref[following] != doc_ref[block])
        return jnp.where(closing, jnp.minimum(tail_ref[block], rows), rows)

    ones = jnp.ones((rows, HEAD_DIM), jnp.bfloat16)

    def scores_of(q, k):
        return lax.dot_general(q, k, (((1,), (1,)), ((), ())), preferred_element_type=jnp.float32)

    def self_keys(j, i):
        return kv.at[j, i, 0], kv.at[j, i, 1]

    def cross_keys(j, i):
        return kvc.at[j, :, pl.ds(0, kvw)], kvc.at[j, :, pl.ds(kvw, kvw)]

    def diag(queries, keys_of, items):
        for r in range(0, rows, TILE):
            for b, i in items:
                live = live_of(2 * z + b)
                k_ref, v_ref = keys_of(b, i)
                here, keys = pl.ds(r, TILE), r + TILE
                s = scores_of(queries[b, i, here, :], k_ref[pl.ds(0, keys), :])
                q_at = r + lax.broadcasted_iota(jnp.int32, s.shape, 0)
                k_at = lax.broadcasted_iota(jnp.int32, s.shape, 1)
                s = jnp.where((k_at <= q_at) & (k_at < live), s, NEG)
                peak_row = jnp.max(s, axis=1, keepdims=True)
                w = jnp.exp2((s - peak_row) * SCALE).astype(jnp.bfloat16)
                va = jnp.concatenate([v_ref[pl.ds(0, keys), :], ones[:keys]], axis=1)
                acc[b, i, here, :] = jnp.dot(w, va, preferred_element_type=jnp.float32)
                peak[b, i, here, :] = jnp.broadcast_to(peak_row, (TILE, HEAD_DIM))

    def off(queries, keys_of, items, j):
        def tile(t, carry):
            here = part(t * TILE, TILE)
            for b, i in items:
                same = doc_of(2 * z + b) == doc_of(block_of(j))
                on = jnp.where(same, 1.0, 0.0)
                gone = jnp.where(same, 0.0, 1e30)
                gain = jnp.where(same, SCALE, 0.0)
                k_ref, v_ref = keys_of(j, i)
                s = scores_of(queries[b, i, here, :], k_ref[...])
                peak_row = jnp.max(s, axis=1, keepdims=True) * on - gone
                old = peak[b, i, here, :]
                new = jnp.maximum(old, peak_row)
                fade = jnp.exp2((old - new) * SCALE)
                w = jnp.exp2(s * gain - (new[:, :1] * gain + gone)).astype(jnp.bfloat16)
                va = jnp.concatenate([v_ref[...], ones], axis=1)
                more = jnp.dot(w, va, preferred_element_type=jnp.float32)
                fades = jnp.concatenate([fade, fade], axis=1)
                acc[b, i, here, :] = acc[b, i, here, :] * fades + more
                peak[b, i, here, :] = new
            return carry

        lax.fori_loop(0, rows // TILE, tile, 0)

    def all_heads(b):
        return [(b, i) for i in range(heads)]

    def finish(b, i):
        whole = acc[b, i]
        return (whole[:, :HEAD_DIM] / whole[:, HEAD_DIM:]).astype(jnp.bfloat16)

    def stage2(i):
        arrived("ky", kv.at[yo, i, 0], None, i)
        arrived("vy", kv.at[yo, i, 1], None, i)
        when(has_up, remote("kvz", kv.at[yo, i], kv.at[2 + yo, i], up, i).start)
        arrived("qy", qx.at[yo, i], None, i)
        diag(qx, self_keys, [(yo, i)])
        off(qx, self_keys, [(1, i)], 0)

        @pl.when(has_down)
        def _():
            arrived("kz", kv.at[2 + y, i, 0], None, i)
            arrived("vz", kv.at[2 + y, i, 1], None, i)
            if far:
                when(jnp.logical_and(has_up, y == 1), remote("kvr", kv.at[3, i], kv.at[4, i], up, i).start)

            off(qx, self_keys, [(0, i), (1, i)], 2 + y)

    def stage3(i):
        @pl.when(has_down)
        def _():
            arrived("kvz", kv.at[2 + yo, i], None, i)
            if far:
                when(jnp.logical_and(has_up, y == 0), remote("kvr", kv.at[3, i], kv.at[4, i], up, i).start)

            off(qx, self_keys, [(0, i), (1, i)], 2 + yo)

        if not far:
            stage5(i)

    def stage4(i):
        @pl.when(far_down)
        def _():
            arrived("kvr", kv.at[4, i], None, i)
            off(qx, self_keys, [(0, i)], 4)

        stage5(i)

    def cy_copy(i):
        return remote("cy", ctxo.at[:, head_cols(i)], ctx.at[c_at, y, :, head_cols(i)], to_y, i)

    def cc_copy(i):
        piece = ctx.at[c_at, y, :, head_cols(i)]
        return remote("cc", piece, piece, to_c, i)

    def cyc_copy(i):
        piece = ctx.at[c_at, yo, :, head_cols(i)]
        return remote("cyc", piece, piece, to_c, i)

    def stage5(i):
        ctxo[:, head_cols(i)] = finish(yo, i)
        cy_copy(i).start()
        ctx[c_at, y, :, head_cols(i)] = finish(y, i)
        cc_copy(i).start()

    for i in range(heads):
        for copy in local_kvq(i):
            copy.wait()
    diag(qx, self_keys, all_heads(y))
    ahead, ahead2 = jnp.minimum(z + 1, last), jnp.minimum(z + 2, last)
    behind, behind2 = jnp.maximum(z - 1, 0), jnp.maximum(z - 2, 0)
    has_far = z + 2 <= last

    def wpart(plane, side):
        return wfull.at[part((plane * 2 + side) * wrows, wrows), :]

    def pass_on(name, onward, piece, cond, to, to_cond):
        arrived(name, piece, cond)
        send(onward, piece, piece, to, jnp.logical_and(cond, to_cond))

    each_head(stage2)
    pass_on("wb1", "wb2", wpart(ahead, y), has_up, down, has_down)
    if not far:
        send("wf1", wfull.at[wrow, :], wfull.at[wrow, :], up, has_up)
    each_head(stage3)
    if far:
        send("wf1", wfull.at[wrow, :], wfull.at[wrow, :], up, has_up)
        each_head(stage4)
    arrived("wqy", wfull.at[wrow_y, wq_c])
    arrived("wky", wfull.at[wrow_y, wk_c])
    arrived("wvy", wfull.at[wrow_y, wv_c])
    send("wf1y", wfull.at[wrow_y, :], wfull.at[wrow_y, :], up, has_up)
    send("wb1y", wfull.at[wrow_y, :], wfull.at[wrow_y, :], down, has_down)

    for item in locals_[3:]:
        near(*item).wait()
    arrived("woc0", wo.at[co, 0])
    arrived("woc1", wo.at[co, 1])

    def project(here, side, column):
        total = None
        for core in range(2):
            more = jnp.dot(
                ctx[core, side, here, :], wo[core, column, part(side * half, half), :],
                preferred_element_type=jnp.float32,
            )
            total = more if total is None else total + more
        return total

    each_head(lambda i: arrived("cc", ctx.at[co, y, :, head_cols(i)], None, i))

    def near_side(t, carry):
        here = part(t * TILE, TILE)
        px[here, :] = project(here, y, 1)
        po[here, :] = project(here, y, 0)
        return carry

    lax.fori_loop(0, rows // TILE, near_side, 0)

    def relay_context(i):
        arrived("cy", ctx.at[c_at, yo, :, head_cols(i)], None, i)
        cyc_copy(i).start()

    each_head(relay_context)
    each_head(lambda i: arrived("cyc", ctx.at[co, yo, :, head_cols(i)], None, i))
    for p in range(2):
        here = pl.ds(p * top, top)
        pxb[here, :] = (px[here, :] + project(here, yo, 1)).astype(jnp.bfloat16)
        send(f"px{p}", pxb.at[here, :], pxr.at[here, :], to_x)

    pass_on("wb2", "wb3", wpart(ahead2, y), has_far, down, has_down)
    pass_on("wf1", "wf2", wpart(behind, y), has_down, up, has_up)

    for p in range(2):
        here = pl.ds(p * top, top)
        po[here, :] = po[here, :] + project(here, yo, 0)

    def hpart(b, h, p):
        return hall.at[b, h, pl.ds(p * top, top), :]

    for p in range(2):
        here = pl.ds(p * top, top)
        arrived(f"px{p}", pxr.at[here, :])
        total = resv[here, :].astype(jnp.float32) + (po[here, :] + pxr[here, :].astype(jnp.float32))
        hall[y, h_at, here, :] = total.astype(jnp.bfloat16)
        piece = hpart(y, h_at, p)
        send(f"dx{p}", piece, piece, to_x)
        send(f"dy{p}", piece, piece, to_y)
        send(f"dc{p}", piece, piece, to_c)
        near(f"hid{p}", piece, hid_hbm.at[here, :]).start()
        if p == 0:
            pass_on("wb1y", "wb2y", wpart(ahead, yo), has_up, down, has_down)

    pass_on("wf1y", "wf2y", wpart(behind, yo), has_down, up, has_up)

    arrived("dx0", hpart(y, hx, 0))
    send("dxc0", hpart(y, hx, 0), hpart(y, hx, 0), to_c)
    arrived("dy0", hpart(yo, h_at, 0))
    send("dyc0", hpart(yo, h_at, 0), hpart(yo, h_at, 0), to_c)
    send("dy2", hpart(y, hx, 0), hpart(y, hx, 0), to_y)
    pass_on("wf2", "wf3", wpart(behind2, y), far_down, up, has_up)
    pass_on("wb2y", "wb3y", wpart(ahead2, yo), has_far, down, has_down)
    arrived("dy1", hpart(yo, h_at, 1))
    send("dx2", hpart(yo, h_at, 1), hpart(yo, h_at, 1), to_x)
    send("dyc1", hpart(yo, h_at, 1), hpart(yo, h_at, 1), to_c)
    arrived("dx1", hpart(y, hx, 1))
    send("dxc1", hpart(y, hx, 1), hpart(y, hx, 1), to_c)

    pass_on("wf2y", "wf3y", wpart(behind2, yo), far_down, up, has_up)
    for p in range(2):
        arrived(f"dc{p}", hpart(y, hc, p))
        arrived(f"dxc{p}", hpart(y, hxc, p))
        arrived(f"dyc{p}", hpart(yo, hc, p))

    ntile = 128

    def norm(b):
        def tile(t, carry):
            here = part(t * ntile, ntile)
            square = jnp.zeros((ntile, 1), jnp.float32)
            for h in range(hall.shape[1]):
                wide = hall[b, h, here, :].astype(jnp.float32)
                square += jnp.sum(wide * wide, axis=1, keepdims=True)
            scale = lax.rsqrt(square / D + EPSILON)
            for h in range(hall.shape[1]):
                wide = hall[b, h, here, :].astype(jnp.float32)
                gains = gainv[:, pl.ds(h * width, width)]
                nrm[b, h, here, :] = (wide * scale * gains).astype(jnp.bfloat16)
            return carry

        lax.fori_loop(0, rows // ntile, tile, 0)

    def cross_part(k, b, where, first):
        def tile(t, carry):
            here = part(t * TILE, TILE)
            more = jnp.dot(
                nrm[b, k, here, :], wfull[part(k * 2 * wrows, 2 * wrows), where],
                preferred_element_type=jnp.float32,
            )
            proj[b, here, where] = more if first else proj[b, here, where] + more
            return carry

        lax.fori_loop(0, rows // TILE, tile, 0)

    low = z < planes // 2
    order = [z, jnp.where(low, 1 - z, 5 - z), jnp.where(low, 2, 1), jnp.where(low, 3, 0)]
    norm(y)
    cross_part(order[0], y, pl.ds(0, cols), True)
    cross_part(order[1], y, pl.ds(0, cols), False)

    arrived("dy2", hpart(yo, hx, 0))
    send("dy2c", hpart(yo, hx, 0), hpart(yo, hx, 0), to_c)
    arrived("dx2", hpart(yo, hx, 1))
    send("dx2c", hpart(yo, hx, 1), hpart(yo, hx, 1), to_c)
    cross_part(order[2], y, pl.ds(0, cols), False)
    arrived("dy2c", hpart(yo, hxc, 0))
    arrived("dx2c", hpart(yo, hxc, 1))
    norm(yo)
    cross_part(order[0], yo, pl.ds(0, cols), True)
    cross_part(order[1], yo, pl.ds(0, cols), False)
    cross_part(order[2], yo, pl.ds(0, cols), False)
    for name, plane, cond in (("wf3", 0, z == last), ("wb3", last, z == 0)):
        arrived(name, wpart(plane, y), cond)
        arrived(name + "y", wpart(plane, yo), cond)

    cache_c, query_c = pl.ds(half, 2 * kvw), pl.ds(0, half)

    def cache_out(b):
        cross_part(order[3], b, cache_c, False)
        kvc[b] = proj[b, :, cache_c].astype(jnp.bfloat16)

    cache_out(1)
    send("e1", kvc.at[1], kvc.at[3], up, has_up)
    cache_out(0)
    send("e0", kvc.at[0], kvc.at[2], up, has_up)

    def query_out(b, carry):
        cross_part(order[3], b, query_c, False)
        for i in range(heads):
            cq[b, i] = proj[b, :, pl.ds(i * HEAD_DIM, HEAD_DIM)].astype(jnp.bfloat16)
        return carry

    lax.fori_loop(0, 2, query_out, 0)

    def own_diag(b, carry):
        diag(cq, cross_keys, all_heads(b))
        return carry

    lax.fori_loop(0, 2, own_diag, 0)
    if far:
        arrived("e1", kvc.at[3], has_down)
        send("er", kvc.at[3], kvc.at[4], up, mid)
    off(cq, cross_keys, all_heads(1), 0)
    if not far:
        arrived("e1", kvc.at[3], has_down)

    @pl.when(has_down)
    def _():
        def step(b, carry):
            off(cq, cross_keys, all_heads(b), 3)
            return carry

        lax.fori_loop(0, 2, step, 0)

    if far:
        @pl.when(far_down)
        def _():
            arrived("er", kvc.at[4])
            off(cq, cross_keys, all_heads(0), 4)

    arrived("e0", kvc.at[2], has_down)

    def home_copy(i):
        return near("o", outs.at[y, i], out_hbm.at[:, own_head(i)], i)

    def away_copy(i):
        return remote("o", outs.at[yo, i], out_hbm.at[:, own_head(i)], to_y, i)

    def result(n, carry):
        b = jnp.where(n == 0, yo, y)

        @pl.when(has_down)
        def _():
            off(cq, cross_keys, all_heads(b), 2)

        for i in range(heads):
            outs[b, i] = finish(b, i)
            when(n == 0, away_copy(i).start)
            when(n == 1, home_copy(i).start)
        return carry

    lax.fori_loop(0, 2, result, 0)

    for p in range(2):
        near(f"hid{p}", hpart(y, h_at, p), hid_hbm.at[pl.ds(p * top, top), :]).wait()
    for name, src, dst, device, cond in sends:
        when(cond, remote(name, src, dst, device).wait_send)

    def ended(i):
        for copy, cond in first_sends(i):
            when(cond, copy.wait_send)
        when(has_up, remote("kvz", kv.at[yo, i], kv.at[2 + yo, i], up, i).wait_send)
        if far:
            when(mid, remote("kvr", kv.at[3, i], kv.at[4, i], up, i).wait_send)
        cy_copy(i).wait_send()
        cc_copy(i).wait_send()
        cyc_copy(i).wait_send()
        home_copy(i).wait()
        away_copy(i).wait_send()
        arrived("o", out_hbm.at[:, other_head(i)], None, i)

    each_head(ended)


def settle_kernel(hid_ref, out_ref, hid_to, out_to):
    hid_to[...] = hid_ref[...]
    out_to[...] = out_ref[...]


def settled(hid, out):
    rows, width = hid.shape
    spec = pl.BlockSpec((rows // 2, width), lambda i: (i, 0))
    return pl.pallas_call(
        settle_kernel,
        out_shape=(jax.ShapeDtypeStruct(hid.shape, hid.dtype),) * 2,
        grid=(2,),
        in_specs=[spec, spec],
        out_specs=(spec, spec),
        compiler_params=pltpu.CompilerParams(vmem_limit_bytes=60 * 1024 * 1024),
    )(hid, out)


def fused(far, residual, q_self, k_self, v_self, w_out, norm_gain, w_query, w_cache, block_doc, tail_len):
    rows, width = q_self.shape
    seq_size, head_size = lax.axis_size("seq"), lax.axis_size("head")
    half = width // 2
    heads = half // HEAD_DIM
    kvw = w_cache.shape[1] // 4
    cols = half + 2 * kvw
    bf, f32 = jnp.bfloat16, jnp.float32
    hbm = pl.BlockSpec(memory_space=pl.ANY)
    smem = pl.BlockSpec(memory_space=pltpu.SMEM)
    copies = len(BY_HEAD) * heads + len(COPIES)
    scratch = [
        pltpu.VMEM((2, heads, rows, HEAD_DIM), bf),
        pltpu.VMEM((5 if far else 4, heads, 2, rows, HEAD_DIM), bf),
        pltpu.VMEM((2, heads, rows, 2 * HEAD_DIM), f32),
        pltpu.VMEM((2, heads, rows, HEAD_DIM), f32),
        pltpu.VMEM((2, 2, width, width), bf),
        pltpu.VMEM((w_query.shape[0] * seq_size, cols), bf),
        pltpu.VMEM((2, 2, rows, half), bf),
        pltpu.VMEM((rows, half), bf),
        pltpu.VMEM((rows, width), f32),
        pltpu.VMEM((rows, width), f32),
        pltpu.VMEM((rows, width), bf),
        pltpu.VMEM((rows, width), bf),
        pltpu.VMEM((2, head_size, rows, width), bf),
        pltpu.VMEM((2, head_size, rows, width), bf),
        pltpu.VMEM((rows, width), bf),
        pltpu.VMEM((1, head_size * width), f32),
        pltpu.VMEM((2, rows, cols), f32),
        pltpu.VMEM((2, heads, rows, HEAD_DIM), bf),
        pltpu.VMEM((5 if far else 4, rows, 2 * kvw), bf),
        pltpu.VMEM((2, heads, rows, HEAD_DIM), bf),
        pltpu.SemaphoreType.DMA((copies,)),
        pltpu.SemaphoreType.DMA((copies,)),
        pltpu.SemaphoreType.DMA((len(LOCALS) + len(LOCALS_BY_HEAD) * heads,)),
    ]
    wide = jax.ShapeDtypeStruct((rows, width), bf)
    return pl.pallas_call(
        functools.partial(fused_kernel, far),
        out_shape=(wide, wide),
        in_specs=[hbm] * 8 + [smem] * 2,
        out_specs=(hbm, hbm),
        scratch_shapes=scratch,
        compiler_params=pltpu.CompilerParams(
            collective_id=1 if far else 0, has_side_effects=True, vmem_limit_bytes=60 * 1024 * 1024
        ),
    )(
        residual, q_self, k_self, v_self, w_out, norm_gain.reshape(1, head_size * width),
        w_query, w_cache, block_doc, tail_len,
    )


def chosen(*args):
    block_doc = args[8]
    at = np.arange(block_doc.shape[0])
    apart = (at[None, :] - at[:, None] == 3) & (at[None, :] % 2 == 0)
    far = jnp.any((block_doc[:, None] == block_doc[None, :]) & apart)
    hid, out = lax.cond(far, functools.partial(fused, True), functools.partial(fused, False), *args)
    return settled(hid, out)


def stage_kernel(offsets, window, first, last, facts, q_ref, *refs):
    pairs = [(refs[2 * i], refs[2 * i + 1]) for i in range(len(offsets))]
    rest = refs[2 * len(offsets):]
    if not first:
        acc_in, peak_in, total_in = rest[:3]
        rest = rest[3:]
    if last:
        out_ref = rest[0]
        acc, peak, total = rest[1:]
    else:
        acc, peak, total = rest
    rows = q_ref.shape[0]
    tile = min(ROW_TILE, rows)
    scaling = math.log2(math.e) / math.sqrt(HEAD_DIM)

    def scores_of(r, k):
        return lax.dot_general(
            q_ref[pl.ds(r, tile), :], k, (((1,), (1,)), ((), ())),
            preferred_element_type=jnp.float32,
        )

    if not first:
        acc[...] = acc_in[...]
        peak[...] = peak_in[...]
        total[...] = total_in[...]

    for (k_ref, v_ref), (flag, offset) in zip(pairs, offsets):

        def one(offset=offset, k_ref=k_ref, v_ref=v_ref):
            for r in range(0, rows, tile):
                here = pl.ds(r, tile)
                keys = r + tile if offset == 0 else rows
                s = scores_of(r, k_ref[pl.ds(0, keys), :])
                if offset == 0:
                    q_at = r + lax.broadcasted_iota(jnp.int32, s.shape, 0)
                    k_at = lax.broadcasted_iota(jnp.int32, s.shape, 1)
                    s = jnp.where((k_at <= q_at) & (k_at < facts[0]), s, -1e30)
                elif offset * rows + rows - 1 >= window:
                    q_at = r + lax.broadcasted_iota(jnp.int32, s.shape, 0)
                    k_at = lax.broadcasted_iota(jnp.int32, s.shape, 1)
                    s = jnp.where(offset * rows + q_at - k_at < window, s, -1e30)
                top = jnp.max(s, axis=1, keepdims=True)
                if offset == 0:
                    w = jnp.exp2((s - top) * scaling)
                    part = jnp.dot(
                        w.astype(jnp.bfloat16), v_ref[pl.ds(0, keys), :],
                        preferred_element_type=jnp.float32,
                    )
                    acc[here, :] = part
                    total[here, :] = jnp.broadcast_to(
                        jnp.sum(w, axis=1, keepdims=True), (tile, HEAD_DIM)
                    )
                    peak[here, :] = jnp.broadcast_to(top, (tile, HEAD_DIM))
                else:
                    old = peak[here, :]
                    new = jnp.maximum(old, top)
                    w = jnp.exp2((s - new[:, :1]) * scaling)
                    fade = jnp.exp2((old - new) * scaling)
                    part = jnp.dot(
                        w.astype(jnp.bfloat16), v_ref[...], preferred_element_type=jnp.float32
                    )
                    acc[here, :] = acc[here, :] * fade + part
                    total[here, :] = total[here, :] * fade + jnp.sum(w, axis=1, keepdims=True)
                    peak[here, :] = new

        if offset == 0:
            one()
        else:
            pl.when(facts[flag] > 0)(one)

    if last:
        out_ref[...] = (acc[...] / total[...]).astype(jnp.bfloat16)


def attend_stage(facts, queries, blocks, offsets, kv_heads, state, window, last):
    rows, width = queries.shape
    heads = width // HEAD_DIM
    group = heads // kv_heads
    tall = pl.BlockSpec((rows, HEAD_DIM), lambda h, f: (0, h))
    key_spec = pl.BlockSpec((rows, HEAD_DIM), lambda h, f: (0, h // group))
    value_spec = pl.BlockSpec((rows, HEAD_DIM), lambda h, f: (0, kv_heads + h // group))
    operands, specs = [queries], [tall]
    for block in blocks:
        operands += [block, block]
        specs += [key_spec, value_spec]
    if state is not None:
        operands += list(state)
        specs += [tall] * 3
    wide = jax.ShapeDtypeStruct((rows, width), jnp.float32)
    if last:
        out_shape = jax.ShapeDtypeStruct((rows, width), jnp.bfloat16)
        out_specs = tall
        scratch = [pltpu.VMEM((rows, HEAD_DIM), jnp.float32)] * 3
    else:
        out_shape, out_specs, scratch = (wide,) * 3, (tall,) * 3, []
    flops = 4 * rows * rows * width * len(offsets) * 3
    return pl.pallas_call(
        functools.partial(stage_kernel, offsets, window, state is None, last),
        out_shape=out_shape,
        grid_spec=pltpu.PrefetchScalarGridSpec(
            num_scalar_prefetch=1, grid=(heads,), in_specs=specs, out_specs=out_specs,
            scratch_shapes=scratch,
        ),
        compiler_params=pltpu.CompilerParams(
            dimension_semantics=("arbitrary",), vmem_limit_bytes=32 * 1024 * 1024
        ),
        cost_estimate=pl.CostEstimate(
            flops=flops, bytes_accessed=rows * width * 2 * (2 + 2 * len(offsets)),
            transcendentals=0,
        ),
    )(facts, *operands)


def shared_over_head(block):
    size = lax.axis_size("head")
    held = [block]
    step = size // 2
    got = {0: block}
    while step >= 1:
        for flip in sorted(got):
            got[flip ^ step] = None if got[flip] is None else swapped(got[flip], "head", step)
        step //= 2
    held = [got[flip] for flip in range(size)]
    return held


def sent(block, routes):
    return lax.ppermute(block, "seq", routes)


def row_gather(block):
    size = lax.axis_size("seq")
    me = lax.axis_index("seq")
    ring = [(i, (i + 2) % size) for i in range(size)]
    steps = []
    moving = block
    for step in range(size // 2):
        owner = lax.rem(me - 2 * step + size, size)
        across = swapped(moving, "seq", 1)
        onward = sent(moving, ring) if step + 1 < size // 2 else None
        moving, across, onward = yield moving, across, onward, owner
        moving = onward


def placed(whole, piece, owner):
    return lax.dynamic_update_slice_in_dim(whole, piece, owner * piece.shape[0], 0)


def waves(block, odd, beside):
    size = lax.axis_size("seq")
    first = sent(block, [(i, i + 1) for i in range(size - 1)])
    second_even = sent(block, [(i, i + 2) for i in range(0, size - 2, 2)])
    if beside is not None:
        first, beside = lax.optimization_barrier((first, beside))
    mixed = jnp.where(odd, block, first)
    second = sent(mixed, [(i, i + 2) for i in range(size - 2)])
    third_odd = sent(second_even, [(i, i + 1) for i in range(2, size, 2)])
    return first, [second_even, second, third_odd], beside


def fits(q_self, w_cache):
    seq_size, head_size = lax.axis_size("seq"), lax.axis_size("head")
    return (
        seq_size == 8 and head_size == 4 and q_self.shape[1] == 6 * HEAD_DIM
        and w_cache.shape[1] == 4 * HEAD_DIM and q_self.shape[0] % TILE == 0
    )


def local(
    residual, q_self, k_self, v_self, w_out, norm_gain, w_query, w_cache, block_doc, tail_len
):
    rows, width = q_self.shape
    local_heads = width // HEAD_DIM
    if fits(q_self, w_cache):
        return chosen(
            residual, q_self, k_self, v_self, w_out, norm_gain, w_query, w_cache, block_doc, tail_len
        )
    local_kv = w_cache.shape[1] // (2 * HEAD_DIM)
    seq_size, head_size = lax.axis_size("seq"), lax.axis_size("head")
    span = min(DOC_BLOCKS, seq_size // 2)
    far = list(range(1, span))
    me, my_head = lax.axis_index("seq"), lax.axis_index("head")

    own_doc = block_doc[me]
    following = jnp.where(me == seq_size - 1, -1, block_doc[jnp.minimum(me + 1, seq_size - 1)])
    live = jnp.where(following != own_doc, jnp.minimum(tail_len[me], rows), rows)
    odd = lax.rem(me, 2) == 1
    small = span == 4 and seq_size % 2 == 0

    def together(distance):
        other = me - distance
        return jnp.logical_and(other >= 0, block_doc[jnp.maximum(other, 0)] == own_doc)

    if small:
        flags = [
            together(1),
            jnp.logical_and(jnp.logical_not(odd), together(2)),
            jnp.where(odd, together(2), together(3)),
            jnp.logical_and(odd, together(3)),
        ]
        distances = [1, 2, 3, 3]
    else:
        flags = [together(distance) for distance in far]
        distances = far
    facts = jnp.stack([live.astype(jnp.int32)] + [flag.astype(jnp.int32) for flag in flags])
    slots = [(1 + i, distance) for i, distance in enumerate(distances)]

    stacked = jnp.concatenate([k_self, v_self], axis=1)
    weight_rows = jnp.concatenate([w_query, w_cache], axis=1)
    state = attend_stage(facts, q_self, [stacked], [(0, 0)], local_heads, None, WINDOW, False)
    if small:
        near, late, state = waves(stacked, odd, state)
    else:
        near, *late = [passed_along(stacked, "seq", offset) for offset in far]

    own_columns = residual.shape[1]
    out_pieces = []
    for flip in range(head_size):
        piece = lax.dynamic_slice_in_dim(w_out, (my_head ^ flip) * own_columns, own_columns, 1)
        out_pieces.append(piece if flip == 0 else swapped(piece, "head", flip))

    state = attend_stage(facts, q_self, [near], slots[:1], local_heads, state, WINDOW, False)
    if small:
        weight_rows, state = lax.optimization_barrier((weight_rows, state))
        weights = jnp.zeros((weight_rows.shape[0] * seq_size, weight_rows.shape[1]), jnp.bfloat16)
        gather = row_gather(weight_rows)
        moving, across, onward, owner = next(gather)
        late, across, onward, out_pieces = lax.optimization_barrier(
            (late, across, onward, out_pieces)
        )
        weights = placed(placed(weights, moving, owner), across, owner ^ 1)
        moving, across, onward, owner = gather.send((moving, across, onward))
    else:
        weights = lax.all_gather(weight_rows, "seq", axis=0, tiled=True)
    context = attend_stage(facts, q_self, late, slots[1:], local_heads, state, WINDOW, True)
    if small:
        context, across, onward = lax.optimization_barrier((context, across, onward))
        weights = placed(placed(weights, moving, owner), across, owner ^ 1)
        moving, across, onward, owner = gather.send((moving, across, onward))

    contexts = shared_over_head(context)
    projected = jnp.dot(contexts[0], out_pieces[0], preferred_element_type=jnp.float32)
    for flip in range(1, head_size):
        projected += jnp.dot(contexts[flip], out_pieces[flip], preferred_element_type=jnp.float32)
    hidden = (residual.astype(jnp.float32) + projected).astype(jnp.bfloat16)
    if small:
        hidden, across, onward = lax.optimization_barrier((hidden, across, onward))
        weights = placed(placed(weights, moving, owner), across, owner ^ 1)
        while onward is not None:
            moving, across, onward, owner = gather.send((moving, across, onward))
            weights = placed(placed(weights, moving, owner), across, owner ^ 1)

    full = jnp.zeros((rows, own_columns * head_size), jnp.bfloat16)
    for flip, piece in enumerate(shared_over_head(hidden)):
        full = lax.dynamic_update_slice_in_dim(full, piece, (my_head ^ flip) * own_columns, 1)
    wide = full.astype(jnp.float32)
    mean_square = jnp.sum(wide * wide, axis=1, keepdims=True) / D
    normed = (wide * lax.rsqrt(mean_square + EPSILON) * norm_gain).astype(jnp.bfloat16)

    cache_rows = jnp.dot(
        normed, weights[:, width:], preferred_element_type=jnp.float32
    ).astype(jnp.bfloat16)
    if small:
        near, late, _ = waves(cache_rows, odd, None)
    else:
        near, *late = [passed_along(cache_rows, "seq", offset) for offset in far]
    cross_queries = jnp.dot(
        normed, weights[:, :width], preferred_element_type=jnp.float32
    ).astype(jnp.bfloat16)
    reach = DOC_BLOCKS * rows
    state = attend_stage(
        facts, cross_queries, [cache_rows, near], [(0, 0)] + slots[:1], local_kv, None, reach, False
    )
    cross_context = attend_stage(
        facts, cross_queries, late, slots[1:], local_kv, state, reach, True
    )
    return (hidden, cross_context)


def solution(mesh):
    in_specs = (
        P("seq", "head"),
        P("seq", "head"),
        P("seq", "head"),
        P("seq", "head"),
        P("head", None),
        P(),
        P("seq", "head"),
        P("seq", "head"),
        P(),
        P(),
    )
    out_specs = (P("seq", "head"), P("seq", "head"))
    return jax.shard_map(local, mesh=mesh, in_specs=in_specs, out_specs=out_specs, check_vma=False)
```

```python
import functools
import math

import jax
import jax.numpy as jnp
import numpy as np
from jax import lax
from jax.experimental import pallas as pl
from jax.experimental.pallas import tpu as pltpu
from jax.sharding import PartitionSpec as P

D = 3072
HEAD_DIM = 128
WINDOW = 2048
DOC_BLOCKS = 5
EPSILON = 1e-06
ROW_TILE = 256


def passed_along(block, axis, distance):
    devices = range(lax.axis_size(axis))
    route = [(i - distance, i) for i in devices if i - distance in devices]
    return lax.ppermute(block, axis, route)


def swapped(block, axis, flip):
    return lax.ppermute(block, axis, [(i, i ^ flip) for i in range(lax.axis_size(axis))])


MESH = pl.DeviceIdType.MESH
TILE = 256
NEG = -1e30
SCALE = math.log2(math.e) / math.sqrt(HEAD_DIM)

BY_HEAD = (
    "ky", "vy", "qy", "kz", "vz", "kvz", "kvr", "cy", "cc", "cyc", "o", "qz", "qzy", "ob", "lb", "wb1", "wf2",
)
COPIES = (
    "wqy", "wky", "wvy", "wf1", "wf1y", "wf2y", "wf3", "wf3y",
    "wb1y", "wb2", "wb2y", "wb3", "wb3y", "woc0", "woc1",
    "px0", "px1", "px2", "px3", "dx0", "dx1", "dx2", "dx3", "dy0", "dy1", "dy2", "dy3",
    "dc0", "dc1", "dc2", "dc3", "dxc0", "dxc1", "dxc2", "dxc3", "dyc0", "dyc1", "dyc2", "dyc3",
    "far0", "far1", "far2", "far3", "farc0", "farc1", "farc2", "farc3", "e1", "e0", "er",
)
LOCALS = ("wq", "wk", "wv", "res", "gain", "wo0", "wo1", "hid0", "hid1", "hid2", "hid3")
LOCALS_BY_HEAD = ("k", "v", "q", "o")


def fused_kernel(
    far, res_hbm, q_hbm, k_hbm, v_hbm, wo_hbm, gain_hbm, wq_hbm, wc_hbm, doc_ref, tail_ref,
    hid_hbm, out_hbm,
    qx, kv, qu, osend, orecv, lbuf, lsend, lrecv, acc, peak, wo, wfull, ctx, ctxo, po, px, pxb, pxr, hall, nrm, resv, gainv, proj, cq, kvc, outs,
    ss, rs, ls,
):
    s_at, h_at = lax.axis_index("seq"), lax.axis_index("head")
    seq_size = lax.axis_size("seq")
    planes = seq_size // 2
    last = planes - 1
    z, y = s_at // 2, lax.rem(s_at, 2)
    yo = 1 - y
    c_at = lax.rem(h_at, 2)
    co = 1 - c_at
    hx, hc = lax.rem(h_at + 2, 4), h_at + 1 - 2 * c_at
    hxc = lax.rem(hc + 2, 4)
    rows, width = q_hbm.shape
    half = width // 2
    heads = half // HEAD_DIM
    wrows = wq_hbm.shape[0]
    kvw = wc_hbm.shape[1] // 4
    cols = half + 2 * kvw
    quarter = rows // 4
    to_y, to_x, to_c = (z * 2 + yo, h_at), (s_at, hx), (s_at, hc)
    up, down = (s_at + 2, h_at), (s_at - 2, h_at)
    has_up, has_down = z < last, z > 0
    mid = jnp.logical_and(has_up, has_down)
    far_down = z > 1

    def part(at, size):
        return pl.ds(pl.multiple_of(at, size), size)

    def index_of(name, i):
        if i is None:
            return len(BY_HEAD) * heads + COPIES.index(name)
        return BY_HEAD.index(name) * heads + i

    def remote(name, src, dst, device, i=None):
        at = index_of(name, i)
        return pltpu.make_async_remote_copy(
            src_ref=src, dst_ref=dst, send_sem=ss.at[at], recv_sem=rs.at[at],
            device_id=device, device_id_type=MESH,
        )

    def near(name, src, dst, i=None):
        at = LOCALS.index(name) if i is None else len(LOCALS) + LOCALS_BY_HEAD.index(name) * heads + i
        return pltpu.make_async_copy(src, dst, ls.at[at])

    def when(cond, go):
        if cond is None:
            go()
        else:
            pl.when(cond)(go)

    sends = []

    def send(name, src, dst, device, cond=None):
        when(cond, lambda: remote(name, src, dst, device).start())
        sends.append((name, src, dst, device, cond))

    def arrived(name, dst, cond=None, i=None):
        def go():
            remote(name, dst, dst, to_y, i).wait_recv()

        when(cond, go)

    def each_head(body):
        def step(i, carry):
            body(i)
            return carry

        lax.fori_loop(0, heads, step, 0)

    mine, other = part(y * half, half), part(yo * half, half)
    kmine, kother = part(y * kvw, kvw), part(yo * kvw, kvw)
    vmine, vother = part((2 + y) * kvw, kvw), part((2 + yo) * kvw, kvw)
    wrow, wrow_y = part(s_at * wrows, wrows), part((z * 2 + yo) * wrows, wrows)
    wq_c, wk_c, wv_c = pl.ds(0, half), pl.ds(half, kvw), pl.ds(half + kvw, kvw)

    def wchunk(plane):
        return wfull.at[part(plane * 2 * wrows, 2 * wrows), :]

    def own_head(i):
        return part(y * half + i * HEAD_DIM, HEAD_DIM)

    def other_head(i):
        return part(yo * half + i * HEAD_DIM, HEAD_DIM)

    def head_cols(i):
        return part(i * HEAD_DIM, HEAD_DIM)

    barrier = pltpu.get_barrier_semaphore()
    for device in (to_y, to_x, to_c):
        pl.semaphore_signal(barrier, inc=1, device_id=device, device_id_type=MESH)

    @pl.when(has_up)
    def _():
        pl.semaphore_signal(barrier, inc=1, device_id=up, device_id_type=MESH)

    @pl.when(has_down)
    def _():
        pl.semaphore_signal(barrier, inc=1, device_id=down, device_id_type=MESH)

    locals_ = [
        ("wq", wq_hbm.at[:, mine], wfull.at[wrow, wq_c]),
        ("wk", wc_hbm.at[:, kmine], wfull.at[wrow, wk_c]),
        ("wv", wc_hbm.at[:, vmine], wfull.at[wrow, wv_c]),
        ("wo0", wo_hbm.at[:, part(h_at * width, width)], wo.at[c_at, 0]),
        ("wo1", wo_hbm.at[:, part(hx * width, width)], wo.at[c_at, 1]),
        ("res", res_hbm, resv),
        ("gain", gain_hbm, gainv),
    ]

    def local_kvq(i):
        return [
            near("k", k_hbm.at[:, own_head(i)], kv.at[y, i, 0], i),
            near("v", v_hbm.at[:, own_head(i)], kv.at[y, i, 1], i),
            near("q", q_hbm.at[:, own_head(i)], qx.at[y, i], i),
        ]

    for i in range(heads):
        for copy in local_kvq(i):
            copy.start()
    for item in locals_:
        near(*item).start()
    pl.semaphore_wait(barrier, 3 + jnp.where(has_up, 1, 0) + jnp.where(has_down, 1, 0))

    def first_sends(i):
        return [
            (remote("qy", q_hbm.at[:, other_head(i)], qx.at[y, i], to_y, i), None),
            (remote("ky", k_hbm.at[:, other_head(i)], kv.at[y, i, 0], to_y, i), None),
            (remote("vy", v_hbm.at[:, other_head(i)], kv.at[y, i, 1], to_y, i), None),
        ] + ([
            (remote("kz", k_hbm.at[:, own_head(i)], kv.at[2 + y, i, 0], up, i), has_up),
            (remote("vz", v_hbm.at[:, own_head(i)], kv.at[2 + y, i, 1], up, i), has_up),
        ] if far else [
            (remote("qz", q_hbm.at[:, own_head(i)], qu.at[y, i], down, i), has_down),
        ])

    for i in range(heads):
        for copy, cond in first_sends(i):
            when(cond, copy.start)
    send("wqy", wq_hbm.at[:, other], wfull.at[wrow, wq_c], to_y)
    send("wky", wc_hbm.at[:, kother], wfull.at[wrow, wk_c], to_y)
    send("wvy", wc_hbm.at[:, vother], wfull.at[wrow, wv_c], to_y)
    send("woc0", wo_hbm.at[:, part(hc * width, width)], wo.at[c_at, 0], to_c)
    send("woc1", wo_hbm.at[:, part(hxc * width, width)], wo.at[c_at, 1], to_c)
    for item in locals_[:3]:
        near(*item).wait()
    third = wrows // heads

    def wthird(block, i):
        return wfull.at[part(block * wrows + i * third, third), :]

    def wb1_copy(i):
        return remote("wb1", wthird(s_at, i), wthird(s_at, i), down, i)

    def wf2_copy(i):
        piece = wthird(jnp.maximum(s_at - 2, 0), i)
        return remote("wf2", piece, piece, up, i)

    if far:
        for i in range(heads):
            when(has_down, wb1_copy(i).start)
    else:
        send("wf1", wfull.at[wrow, :], wfull.at[wrow, :], up, has_up)

    def block_of(j):
        return jnp.where(j < 2, 2 * z + j, jnp.where(j < 4, 2 * z - 4 + j, 2 * z - 3))

    def doc_of(block):
        return doc_ref[jnp.maximum(block, 0)]

    def live_of(block):
        following = jnp.minimum(block + 1, seq_size - 1)
        closing = jnp.logical_or(block == seq_size - 1, doc_ref[following] != doc_ref[block])
        return jnp.where(closing, jnp.minimum(tail_ref[block], rows), rows)

    ones = jnp.ones((rows, HEAD_DIM), jnp.bfloat16)

    def scores_of(q, k):
        return lax.dot_general(q, k, (((1,), (1,)), ((), ())), preferred_element_type=jnp.float32)

    def self_keys(j, i):
        return kv.at[j, i, 0], kv.at[j, i, 1]

    def cross_keys(j, i):
        return kvc.at[j, :, pl.ds(0, kvw)], kvc.at[j, :, pl.ds(kvw, kvw)]

    def diag(queries, keys_of, items):
        for r in range(0, rows, TILE):
            for b, i in items:
                live = live_of(2 * z + b)
                k_ref, v_ref = keys_of(b, i)
                here, keys = pl.ds(r, TILE), r + TILE
                s = scores_of(queries[b, i, here, :], k_ref[pl.ds(0, keys), :])
                q_at = r + lax.broadcasted_iota(jnp.int32, s.shape, 0)
                k_at = lax.broadcasted_iota(jnp.int32, s.shape, 1)
                s = jnp.where((k_at <= q_at) & (k_at < live), s, NEG)
                peak_row = jnp.max(s, axis=1, keepdims=True)
                w = jnp.exp2((s - peak_row) * SCALE).astype(jnp.bfloat16)
                va = jnp.concatenate([v_ref[pl.ds(0, keys), :], ones[:keys]], axis=1)
                acc[b, i, here, :] = jnp.dot(w, va, preferred_element_type=jnp.float32)
                peak[b, i, here, :] = jnp.broadcast_to(peak_row, (TILE, HEAD_DIM))

    def off(queries, keys_of, items, j, size=TILE):
        def tile(t, carry):
            here = part(t * size, size)
            for b, i in items:
                same = doc_of(2 * z + b) == doc_of(block_of(j))
                on = jnp.where(same, 1.0, 0.0)
                gone = jnp.where(same, 0.0, 1e30)
                gain = jnp.where(same, SCALE, 0.0)
                k_ref, v_ref = keys_of(j, i)
                s = scores_of(queries[b, i, here, :], k_ref[...])
                peak_row = jnp.max(s, axis=1, keepdims=True) * on - gone
                old = peak[b, i, here, :]
                new = jnp.maximum(old, peak_row)
                fade = jnp.exp2((old - new) * SCALE)
                w = jnp.exp2(s * gain - (new[:, :1] * gain + gone)).astype(jnp.bfloat16)
                va = jnp.concatenate([v_ref[...], ones], axis=1)
                more = jnp.dot(w, va, preferred_element_type=jnp.float32)
                fades = jnp.concatenate([fade, fade], axis=1)
                acc[b, i, here, :] = acc[b, i, here, :] * fades + more
                peak[b, i, here, :] = new
            return carry

        lax.fori_loop(0, rows // size, tile, 0)

    def all_heads(b):
        return [(b, i) for i in range(heads)]

    def finish(b, i):
        whole = acc[b, i]
        return (whole[:, :HEAD_DIM] / whole[:, HEAD_DIM:]).astype(jnp.bfloat16)

    ahead, ahead2 = jnp.minimum(z + 1, last), jnp.minimum(z + 2, last)
    behind, behind2 = jnp.maximum(z - 1, 0), jnp.maximum(z - 2, 0)
    has_far = z + 2 <= last

    def wpart(plane, side):
        return wfull.at[part((plane * 2 + side) * wrows, wrows), :]

    def pass_on(name, onward, piece, cond, to, to_cond):
        arrived(name, piece, cond)
        send(onward, piece, piece, to, jnp.logical_and(cond, to_cond))

    def qzy_copy(i):
        return remote("qzy", qx.at[yo, i], qu.at[yo, i], down, i)

    def ob_copy(i):
        return remote("ob", osend.at[i], orecv.at[i], up, i)

    def lb_copy(i):
        return remote("lb", lsend.at[i], lrecv.at[i, pl.ds(0, 8), :], up, i)

    def above(i):
        def tile(t, carry):
            here = part(t * TILE, TILE)
            lane = lax.broadcasted_iota(jnp.int32, (TILE, HEAD_DIM), 1)
            logs = jnp.zeros((TILE, HEAD_DIM), jnp.float32)
            for b in range(2):
                query = qu[b, i, here, :]
                scores, tops, marks = [], [], []
                for k in range(2):
                    ahead_doc = doc_of(jnp.minimum(2 * z + 2 + b, seq_size - 1))
                    same = ahead_doc == doc_of(2 * z + k)
                    marks.append((jnp.where(same, SCALE, 0.0), jnp.where(same, 0.0, 1e30)))
                    s = scores_of(query, kv[k, i, 0])
                    scores.append(s)
                    tops.append(jnp.max(s, axis=1, keepdims=True) * jnp.where(same, 1.0, 0.0) - marks[k][1])
                top_row = jnp.maximum(tops[0], tops[1])
                total = None
                for k in range(2):
                    gain, gone = marks[k]
                    w = jnp.exp2(scores[k] * gain - (top_row * gain + gone)).astype(jnp.bfloat16)
                    va = jnp.concatenate([kv[k, i, 1], ones], axis=1)
                    more = jnp.dot(w, va, preferred_element_type=jnp.float32)
                    total = more if total is None else total + more
                weight = total[:, HEAD_DIM:]
                weight = jnp.where(weight > 0.0, weight, 1.0)
                osend[i, b, here, :] = (total[:, :HEAD_DIM] / weight).astype(jnp.bfloat16)
                logs = jnp.where(lane == b, top_row * SCALE + jnp.log2(weight), logs)
            lbuf[here, :] = logs
            return carry

        lax.fori_loop(0, rows // TILE, tile, 0)
        lsend[i] = jnp.transpose(lbuf[...])[:8, :]

    def merged(b, i, logs):
        log_row = jnp.where(has_down, logs[:, b:b + 1], NEG)
        part_row = jnp.where(has_down, orecv[i, b].astype(jnp.float32), 0.0)
        whole, own_log = acc[b, i], peak[b, i] * SCALE
        most = jnp.maximum(own_log, log_row)
        fade, share = jnp.exp2(own_log - most), jnp.exp2(log_row - most)
        above_row = whole[:, :HEAD_DIM] * fade + part_row * share
        return (above_row / (whole[:, HEAD_DIM:] * fade + share)).astype(jnp.bfloat16)

    def stage2(i):
        arrived("qy", qx.at[yo, i], None, i)
        if not far:
            when(has_down, qzy_copy(i).start)
            when(has_down, wb1_copy(i).start)
        arrived("ky", kv.at[yo, i, 0], None, i)
        arrived("vy", kv.at[yo, i, 1], None, i)
        if far:
            when(has_up, remote("kvz", kv.at[yo, i], kv.at[2 + yo, i], up, i).start)
        else:
            @pl.when(has_up)
            def _():
                arrived("qz", qu.at[y, i], None, i)
                arrived("qzy", qu.at[yo, i], None, i)
                above(i)
                ob_copy(i).start()
                lb_copy(i).start()

            when(jnp.logical_and(i == 0, has_down), lambda: arrived("wf1", wpart(behind, y)))
            when(jnp.logical_and(mid, i == 0), wf2_copy(0).start)
        diag(qx, self_keys, [(yo, i)])
        off(qx, self_keys, [(1, i)], 0)
        if far:
            @pl.when(has_down)
            def _():
                arrived("kz", kv.at[2 + y, i, 0], None, i)
                arrived("vz", kv.at[2 + y, i, 1], None, i)
                when(jnp.logical_and(has_up, y == 1), remote("kvr", kv.at[3, i], kv.at[4, i], up, i).start)
                off(qx, self_keys, [(0, i), (1, i)], 2 + y)

    def stage3(i):
        if not far:
            arrived("ob", orecv.at[i], has_down, i)
            arrived("lb", lrecv.at[i, pl.ds(0, 8), :], has_down, i)
            stage5(i)
            return

        @pl.when(has_down)
        def _():
            arrived("kvz", kv.at[2 + yo, i], None, i)
            when(jnp.logical_and(has_up, y == 0), remote("kvr", kv.at[3, i], kv.at[4, i], up, i).start)
            off(qx, self_keys, [(0, i), (1, i)], 2 + yo)

    def stage4(i):
        @pl.when(far_down)
        def _():
            arrived("kvr", kv.at[4, i], None, i)
            off(qx, self_keys, [(0, i)], 4)

        stage5(i)

    def cy_copy(i):
        return remote("cy", ctxo.at[:, head_cols(i)], ctx.at[c_at, y, :, head_cols(i)], to_y, i)

    def cc_copy(i):
        piece = ctx.at[c_at, y, :, head_cols(i)]
        return remote("cc", piece, piece, to_c, i)

    def cyc_copy(i):
        piece = ctx.at[c_at, yo, :, head_cols(i)]
        return remote("cyc", piece, piece, to_c, i)

    def stage5(i):
        if far:
            done = [finish(0, i), finish(1, i)]
        else:
            logs = jnp.transpose(lrecv[i])
            done = [merged(0, i, logs), merged(1, i, logs)]
        ctxo[:, head_cols(i)] = jnp.where(y == 0, done[1], done[0])
        cy_copy(i).start()
        ctx[c_at, y, :, head_cols(i)] = jnp.where(y == 0, done[0], done[1])
        cc_copy(i).start()

    for i in range(heads):
        for copy in local_kvq(i):
            copy.wait()
    diag(qx, self_keys, all_heads(y))
    each_head(stage2)
    if not far:
        for i in range(1, heads):
            when(mid, wf2_copy(i).start)
    each_head(lambda i: arrived("wb1", wthird(jnp.minimum(s_at + 2, seq_size - 1), i), has_up, i))
    send("wb2", wpart(ahead, y), wpart(ahead, y), down, mid)
    each_head(stage3)
    if far:
        send("wf1", wfull.at[wrow, :], wfull.at[wrow, :], up, has_up)
        each_head(stage4)
    arrived("wqy", wfull.at[wrow_y, wq_c])
    arrived("wky", wfull.at[wrow_y, wk_c])
    arrived("wvy", wfull.at[wrow_y, wv_c])
    send("wf1y", wfull.at[wrow_y, :], wfull.at[wrow_y, :], up, has_up)
    send("wb1y", wfull.at[wrow_y, :], wfull.at[wrow_y, :], down, has_down)

    for item in locals_[3:]:
        near(*item).wait()
    arrived("woc0", wo.at[co, 0])
    arrived("woc1", wo.at[co, 1])

    def project(here, side, column):
        total = None
        for core in range(2):
            more = jnp.dot(
                ctx[core, side, here, :], wo[core, column, part(side * half, half), :],
                preferred_element_type=jnp.float32,
            )
            total = more if total is None else total + more
        return total

    each_head(lambda i: arrived("cc", ctx.at[co, y, :, head_cols(i)], None, i))

    def near_side(t, carry):
        here = part(t * TILE, TILE)
        px[here, :] = project(here, y, 1)
        po[here, :] = project(here, y, 0)
        return carry

    lax.fori_loop(0, rows // TILE, near_side, 0)

    def relay_context(i):
        arrived("cy", ctx.at[c_at, yo, :, head_cols(i)], None, i)
        cyc_copy(i).start()

    each_head(relay_context)
    each_head(lambda i: arrived("cyc", ctx.at[co, yo, :, head_cols(i)], None, i))
    for p in range(4):
        here = pl.ds(p * quarter, quarter)
        pxb[here, :] = (px[here, :] + project(here, yo, 1)).astype(jnp.bfloat16)
        send(f"px{p}", pxb.at[here, :], pxr.at[here, :], to_x)

    pass_on("wb2", "wb3", wpart(ahead2, y), has_far, down, has_down)
    if not far:
        each_head(lambda i: arrived("wf2", wthird(jnp.maximum(s_at - 4, 0), i), far_down, i))
        send("wf3", wpart(behind2, y), wpart(behind2, y), up, jnp.logical_and(far_down, has_up))
    if far:
        arrived("wf1", wpart(behind, y), has_down)
        for i in range(heads):
            when(mid, wf2_copy(i).start)

    def far_side(t, carry):
        here = part(t * TILE, TILE)
        po[here, :] = po[here, :] + project(here, yo, 0)
        return carry

    lax.fori_loop(0, rows // TILE, far_side, 0)

    def hpart(b, h, p):
        return hall.at[b, h, pl.ds(p * quarter, quarter), :]

    for p in range(4):
        here = pl.ds(p * quarter, quarter)
        arrived(f"px{p}", pxr.at[here, :])
        total = resv[here, :].astype(jnp.float32) + (po[here, :] + pxr[here, :].astype(jnp.float32))
        hall[y, h_at, here, :] = total.astype(jnp.bfloat16)
        piece = hpart(y, h_at, p)
        send(f"dx{p}", piece, piece, to_x)
        send(f"dy{p}", piece, piece, to_y)
        send(f"dc{p}", piece, piece, to_c)
        near(f"hid{p}", piece, hid_hbm.at[here, :]).start()
        if p == 1:
            pass_on("wb1y", "wb2y", wpart(ahead, yo), has_up, down, has_down)
        if p == 2:
            pass_on("wf1y", "wf2y", wpart(behind, yo), has_down, up, has_up)

    def from_x(p):
        piece = hpart(y, hx, p)
        arrived(f"dx{p}", piece)
        send(f"dxc{p}", piece, piece, to_c)
        if p < 3:
            send(f"far{p}", piece, piece, to_y)

    def from_y(p):
        piece = hpart(yo, h_at, p)
        arrived(f"dy{p}", piece)
        send(f"dyc{p}", piece, piece, to_c)
        if p == 3:
            send("far3", piece, piece, to_x)

    def from_far(p):
        piece = hpart(yo, hx, p)
        arrived(f"far{p}", piece)
        send(f"farc{p}", piece, piece, to_c)

    def own_rows(p):
        arrived(f"dc{p}", hpart(y, hc, p))
        arrived(f"dxc{p}", hpart(y, hxc, p))

    def other_rows(p):
        arrived(f"dyc{p}", hpart(yo, hc, p))
        arrived(f"farc{p}", hpart(yo, hxc, p))

    for p in range(3):
        from_y(p)
    from_x(0)
    from_y(3)
    if far:
        each_head(lambda i: arrived("wf2", wthird(jnp.maximum(s_at - 4, 0), i), far_down, i))
        send("wf3", wpart(behind2, y), wpart(behind2, y), up, jnp.logical_and(far_down, has_up))
    pass_on("wb2y", "wb3y", wpart(ahead2, yo), has_far, down, has_down)
    from_x(1)
    if not far:
        pass_on("wf2y", "wf3y", wpart(behind2, yo), far_down, up, has_up)

    def norm(b, at):
        square = jnp.zeros((quarter, 1), jnp.float32)
        here = part(at * quarter, quarter)
        for h in range(hall.shape[1]):
            wide = hall[b, h, here, :].astype(jnp.float32)
            square += jnp.sum(wide * wide, axis=1, keepdims=True)
        scale = lax.rsqrt(square / D + EPSILON)
        for h in range(hall.shape[1]):
            wide = hall[b, h, here, :].astype(jnp.float32)
            gains = gainv[:, pl.ds(h * width, width)]
            nrm[b, h, here, :] = (wide * scale * gains).astype(jnp.bfloat16)

    def norm_half(b, p):
        def step(n, carry):
            norm(b, 2 * p + n)
            return carry

        lax.fori_loop(0, 2, step, 0)

    def cross_tile(k, b, t, where, first):
        here = part(t * TILE, TILE)
        more = jnp.dot(
            nrm[b, k, here, :], wfull[part(k * 2 * wrows, 2 * wrows), where],
            preferred_element_type=jnp.float32,
        )
        proj[b, here, where] = more if first else proj[b, here, where] + more

    def cross_part(k, b, where, first):
        def tile(t, carry):
            cross_tile(k, b, t, where, first)
            return carry

        lax.fori_loop(0, rows // TILE, tile, 0)

    low = z < planes // 2
    order = [z, jnp.where(low, 1 - z, 5 - z), jnp.where(low, 2, 1), jnp.where(low, 3, 0)]
    every = pl.ds(0, cols)

    def chunks(b, t):
        def step(n, carry):
            cross_tile(jnp.where(n == 0, order[1], order[2]), b, t, every, False)
            return carry

        cross_tile(order[0], b, t, every, True)
        lax.fori_loop(0, 2, step, 0)

    own_rows(0)
    own_rows(1)
    norm_half(y, 0)
    cross_tile(order[0], y, 0, every, True)
    cross_tile(order[1], y, 0, every, False)
    from_x(2)
    from_far(0)
    from_far(1)
    from_x(3)
    other_rows(0)
    other_rows(1)
    norm_half(yo, 0)
    own_rows(2)
    own_rows(3)
    norm_half(y, 1)
    from_far(2)
    if far:
        pass_on("wf2y", "wf3y", wpart(behind2, yo), far_down, up, has_up)
    from_far(3)
    chunks(y, 1)
    chunks(yo, 0)
    cross_tile(order[2], y, 0, every, False)
    other_rows(2)
    other_rows(3)
    norm_half(yo, 1)
    chunks(yo, 1)
    for name, plane, cond in (("wf3", 0, z == last), ("wb3", last, z == 0)):
        arrived(name, wpart(plane, y), cond)
        arrived(name + "y", wpart(plane, yo), cond)

    cache_c, query_c = pl.ds(half, 2 * kvw), pl.ds(0, half)

    def cache_out(b):
        cross_part(order[3], b, cache_c, False)
        kvc[b] = proj[b, :, cache_c].astype(jnp.bfloat16)

    cache_out(1)
    send("e1", kvc.at[1], kvc.at[3], up, has_up)
    cache_out(0)
    send("e0", kvc.at[0], kvc.at[2], up, has_up)

    def query_out(b, carry):
        cross_part(order[3], b, query_c, False)
        for i in range(heads):
            cq[b, i] = proj[b, :, pl.ds(i * HEAD_DIM, HEAD_DIM)].astype(jnp.bfloat16)
        return carry

    lax.fori_loop(0, 2, query_out, 0)

    def own_diag(b, carry):
        diag(cq, cross_keys, all_heads(b))
        return carry

    lax.fori_loop(0, 2, own_diag, 0)

    def home_copy(i):
        return near("o", outs.at[y, i], out_hbm.at[:, own_head(i)], i)

    def away_copy(i):
        return remote("o", outs.at[yo, i], out_hbm.at[:, own_head(i)], to_y, i)

    plan = [(1, 0), (yo, 3), (y, 3)] + ([(0, 4)] if far else []) + [(yo, 2), (y, 2)]

    def look_up(n, which):
        value = plan[0][which]
        for at in range(1, len(plan)):
            value = jnp.where(n == at, plan[at][which], value)
        return value

    def step(n, carry):
        if far:
            @pl.when(jnp.logical_and(n == 0, has_down))
            def _():
                arrived("e1", kvc.at[3])
                when(has_up, remote("er", kvc.at[3], kvc.at[4], up).start)

            when(jnp.logical_and(n == 3, far_down), lambda: arrived("er", kvc.at[4]))
            runs = jnp.where(n == 3, far_down, jnp.logical_or(n == 0, has_down))
        else:
            when(jnp.logical_and(n == 1, has_down), lambda: arrived("e1", kvc.at[3]))
            runs = jnp.logical_or(n == 0, has_down)
        when(jnp.logical_and(n == len(plan) - 2, has_down), lambda: arrived("e0", kvc.at[2]))
        b, j = look_up(n, 0), look_up(n, 1)
        when(runs, lambda: off(cq, cross_keys, all_heads(b), j, rows))

        @pl.when(n >= len(plan) - 2)
        def _():
            for i in range(heads):
                outs[b, i] = finish(b, i)
                when(n == len(plan) - 2, away_copy(i).start)
                when(n == len(plan) - 1, home_copy(i).start)

        return carry

    lax.fori_loop(0, len(plan), step, 0)
    if far:
        sends.append(("er", kvc.at[3], kvc.at[4], up, mid))

    for p in range(4):
        near(f"hid{p}", hpart(y, h_at, p), hid_hbm.at[pl.ds(p * quarter, quarter), :]).wait()
    for name, src, dst, device, cond in sends:
        when(cond, remote(name, src, dst, device).wait_send)

    def ended(i):
        for copy, cond in first_sends(i):
            when(cond, copy.wait_send)
        when(has_down, wb1_copy(i).wait_send)
        when(mid, wf2_copy(i).wait_send)
        if not far:
            when(has_down, qzy_copy(i).wait_send)
            when(has_up, ob_copy(i).wait_send)
            when(has_up, lb_copy(i).wait_send)
        if far:
            when(has_up, remote("kvz", kv.at[yo, i], kv.at[2 + yo, i], up, i).wait_send)
            when(mid, remote("kvr", kv.at[3, i], kv.at[4, i], up, i).wait_send)
        cy_copy(i).wait_send()
        cc_copy(i).wait_send()
        cyc_copy(i).wait_send()
        home_copy(i).wait()
        away_copy(i).wait_send()
        arrived("o", out_hbm.at[:, other_head(i)], None, i)

    each_head(ended)


def settle_kernel(hid_ref, out_ref, hid_to, out_to):
    hid_to[...] = hid_ref[...]
    out_to[...] = out_ref[...]


def settled(hid, out):
    rows, width = hid.shape
    spec = pl.BlockSpec((rows // 2, width), lambda i: (i, 0))
    return pl.pallas_call(
        settle_kernel,
        out_shape=(jax.ShapeDtypeStruct(hid.shape, hid.dtype),) * 2,
        grid=(2,),
        in_specs=[spec, spec],
        out_specs=(spec, spec),
        compiler_params=pltpu.CompilerParams(vmem_limit_bytes=60 * 1024 * 1024),
    )(hid, out)


def fused(far, residual, q_self, k_self, v_self, w_out, norm_gain, w_query, w_cache, block_doc, tail_len):
    rows, width = q_self.shape
    seq_size, head_size = lax.axis_size("seq"), lax.axis_size("head")
    half = width // 2
    heads = half // HEAD_DIM
    kvw = w_cache.shape[1] // 4
    cols = half + 2 * kvw
    bf, f32 = jnp.bfloat16, jnp.float32
    hbm = pl.BlockSpec(memory_space=pl.ANY)
    smem = pl.BlockSpec(memory_space=pltpu.SMEM)
    copies = len(BY_HEAD) * heads + len(COPIES)
    scratch = [
        pltpu.VMEM((2, heads, rows, HEAD_DIM), bf),
        pltpu.VMEM((5 if far else 2, heads, 2, rows, HEAD_DIM), bf),
        pltpu.VMEM((2, heads, rows, HEAD_DIM), bf),
        pltpu.VMEM((heads, 2, rows, HEAD_DIM), bf),
        pltpu.VMEM((heads, 2, rows, HEAD_DIM), bf),
        pltpu.VMEM((rows, HEAD_DIM), f32),
        pltpu.VMEM((heads, 8, rows), f32),
        pltpu.VMEM((heads, HEAD_DIM, rows), f32),
        pltpu.VMEM((2, heads, rows, 2 * HEAD_DIM), f32),
        pltpu.VMEM((2, heads, rows, HEAD_DIM), f32),
        pltpu.VMEM((2, 2, width, width), bf),
        pltpu.VMEM((w_query.shape[0] * seq_size, cols), bf),
        pltpu.VMEM((2, 2, rows, half), bf),
        pltpu.VMEM((rows, half), bf),
        pltpu.VMEM((rows, width), f32),
        pltpu.VMEM((rows, width), f32),
        pltpu.VMEM((rows, width), bf),
        pltpu.VMEM((rows, width), bf),
        pltpu.VMEM((2, head_size, rows, width), bf),
        pltpu.VMEM((2, head_size, rows, width), bf),
        pltpu.VMEM((rows, width), bf),
        pltpu.VMEM((1, head_size * width), f32),
        pltpu.VMEM((2, rows, cols), f32),
        pltpu.VMEM((2, heads, rows, HEAD_DIM), bf),
        pltpu.VMEM((5 if far else 4, rows, 2 * kvw), bf),
        pltpu.VMEM((2, heads, rows, HEAD_DIM), bf),
        pltpu.SemaphoreType.DMA((copies,)),
        pltpu.SemaphoreType.DMA((copies,)),
        pltpu.SemaphoreType.DMA((len(LOCALS) + len(LOCALS_BY_HEAD) * heads,)),
    ]
    wide = jax.ShapeDtypeStruct((rows, width), bf)
    return pl.pallas_call(
        functools.partial(fused_kernel, far),
        out_shape=(wide, wide),
        in_specs=[hbm] * 8 + [smem] * 2,
        out_specs=(hbm, hbm),
        scratch_shapes=scratch,
        compiler_params=pltpu.CompilerParams(
            collective_id=1 if far else 0, has_side_effects=True, vmem_limit_bytes=60 * 1024 * 1024
        ),
    )(
        residual, q_self, k_self, v_self, w_out, norm_gain.reshape(1, head_size * width),
        w_query, w_cache, block_doc, tail_len,
    )


def chosen(*args):
    block_doc = args[8]
    at = np.arange(block_doc.shape[0])
    apart = (at[None, :] - at[:, None] == 3) & (at[None, :] % 2 == 0)
    far = jnp.any((block_doc[:, None] == block_doc[None, :]) & apart)
    hid, out = lax.cond(far, functools.partial(fused, True), functools.partial(fused, False), *args)
    return settled(hid, out)


def stage_kernel(offsets, window, first, last, facts, q_ref, *refs):
    pairs = [(refs[2 * i], refs[2 * i + 1]) for i in range(len(offsets))]
    rest = refs[2 * len(offsets):]
    if not first:
        acc_in, peak_in, total_in = rest[:3]
        rest = rest[3:]
    if last:
        out_ref = rest[0]
        acc, peak, total = rest[1:]
    else:
        acc, peak, total = rest
    rows = q_ref.shape[0]
    tile = min(ROW_TILE, rows)
    scaling = math.log2(math.e) / math.sqrt(HEAD_DIM)

    def scores_of(r, k):
        return lax.dot_general(
            q_ref[pl.ds(r, tile), :], k, (((1,), (1,)), ((), ())),
            preferred_element_type=jnp.float32,
        )

    if not first:
        acc[...] = acc_in[...]
        peak[...] = peak_in[...]
        total[...] = total_in[...]

    for (k_ref, v_ref), (flag, offset) in zip(pairs, offsets):

        def one(offset=offset, k_ref=k_ref, v_ref=v_ref):
            for r in range(0, rows, tile):
                here = pl.ds(r, tile)
                keys = r + tile if offset == 0 else rows
                s = scores_of(r, k_ref[pl.ds(0, keys), :])
                if offset == 0:
                    q_at = r + lax.broadcasted_iota(jnp.int32, s.shape, 0)
                    k_at = lax.broadcasted_iota(jnp.int32, s.shape, 1)
                    s = jnp.where((k_at <= q_at) & (k_at < facts[0]), s, -1e30)
                elif offset * rows + rows - 1 >= window:
                    q_at = r + lax.broadcasted_iota(jnp.int32, s.shape, 0)
                    k_at = lax.broadcasted_iota(jnp.int32, s.shape, 1)
                    s = jnp.where(offset * rows + q_at - k_at < window, s, -1e30)
                top = jnp.max(s, axis=1, keepdims=True)
                if offset == 0:
                    w = jnp.exp2((s - top) * scaling)
                    part = jnp.dot(
                        w.astype(jnp.bfloat16), v_ref[pl.ds(0, keys), :],
                        preferred_element_type=jnp.float32,
                    )
                    acc[here, :] = part
                    total[here, :] = jnp.broadcast_to(
                        jnp.sum(w, axis=1, keepdims=True), (tile, HEAD_DIM)
                    )
                    peak[here, :] = jnp.broadcast_to(top, (tile, HEAD_DIM))
                else:
                    old = peak[here, :]
                    new = jnp.maximum(old, top)
                    w = jnp.exp2((s - new[:, :1]) * scaling)
                    fade = jnp.exp2((old - new) * scaling)
                    part = jnp.dot(
                        w.astype(jnp.bfloat16), v_ref[...], preferred_element_type=jnp.float32
                    )
                    acc[here, :] = acc[here, :] * fade + part
                    total[here, :] = total[here, :] * fade + jnp.sum(w, axis=1, keepdims=True)
                    peak[here, :] = new

        if offset == 0:
            one()
        else:
            pl.when(facts[flag] > 0)(one)

    if last:
        out_ref[...] = (acc[...] / total[...]).astype(jnp.bfloat16)


def attend_stage(facts, queries, blocks, offsets, kv_heads, state, window, last):
    rows, width = queries.shape
    heads = width // HEAD_DIM
    group = heads // kv_heads
    tall = pl.BlockSpec((rows, HEAD_DIM), lambda h, f: (0, h))
    key_spec = pl.BlockSpec((rows, HEAD_DIM), lambda h, f: (0, h // group))
    value_spec = pl.BlockSpec((rows, HEAD_DIM), lambda h, f: (0, kv_heads + h // group))
    operands, specs = [queries], [tall]
    for block in blocks:
        operands += [block, block]
        specs += [key_spec, value_spec]
    if state is not None:
        operands += list(state)
        specs += [tall] * 3
    wide = jax.ShapeDtypeStruct((rows, width), jnp.float32)
    if last:
        out_shape = jax.ShapeDtypeStruct((rows, width), jnp.bfloat16)
        out_specs = tall
        scratch = [pltpu.VMEM((rows, HEAD_DIM), jnp.float32)] * 3
    else:
        out_shape, out_specs, scratch = (wide,) * 3, (tall,) * 3, []
    flops = 4 * rows * rows * width * len(offsets) * 3
    return pl.pallas_call(
        functools.partial(stage_kernel, offsets, window, state is None, last),
        out_shape=out_shape,
        grid_spec=pltpu.PrefetchScalarGridSpec(
            num_scalar_prefetch=1, grid=(heads,), in_specs=specs, out_specs=out_specs,
            scratch_shapes=scratch,
        ),
        compiler_params=pltpu.CompilerParams(
            dimension_semantics=("arbitrary",), vmem_limit_bytes=32 * 1024 * 1024
        ),
        cost_estimate=pl.CostEstimate(
            flops=flops, bytes_accessed=rows * width * 2 * (2 + 2 * len(offsets)),
            transcendentals=0,
        ),
    )(facts, *operands)


def shared_over_head(block):
    size = lax.axis_size("head")
    held = [block]
    step = size // 2
    got = {0: block}
    while step >= 1:
        for flip in sorted(got):
            got[flip ^ step] = None if got[flip] is None else swapped(got[flip], "head", step)
        step //= 2
    held = [got[flip] for flip in range(size)]
    return held


def sent(block, routes):
    return lax.ppermute(block, "seq", routes)


def row_gather(block):
    size = lax.axis_size("seq")
    me = lax.axis_index("seq")
    ring = [(i, (i + 2) % size) for i in range(size)]
    steps = []
    moving = block
    for step in range(size // 2):
        owner = lax.rem(me - 2 * step + size, size)
        across = swapped(moving, "seq", 1)
        onward = sent(moving, ring) if step + 1 < size // 2 else None
        moving, across, onward = yield moving, across, onward, owner
        moving = onward


def placed(whole, piece, owner):
    return lax.dynamic_update_slice_in_dim(whole, piece, owner * piece.shape[0], 0)


def waves(block, odd, beside):
    size = lax.axis_size("seq")
    first = sent(block, [(i, i + 1) for i in range(size - 1)])
    second_even = sent(block, [(i, i + 2) for i in range(0, size - 2, 2)])
    if beside is not None:
        first, beside = lax.optimization_barrier((first, beside))
    mixed = jnp.where(odd, block, first)
    second = sent(mixed, [(i, i + 2) for i in range(size - 2)])
    third_odd = sent(second_even, [(i, i + 1) for i in range(2, size, 2)])
    return first, [second_even, second, third_odd], beside


def fits(q_self, w_cache):
    seq_size, head_size = lax.axis_size("seq"), lax.axis_size("head")
    return (
        seq_size == 8 and head_size == 4 and q_self.shape[1] == 6 * HEAD_DIM
        and w_cache.shape[1] == 4 * HEAD_DIM and q_self.shape[0] % TILE == 0
    )


def local(
    residual, q_self, k_self, v_self, w_out, norm_gain, w_query, w_cache, block_doc, tail_len
):
    rows, width = q_self.shape
    local_heads = width // HEAD_DIM
    if fits(q_self, w_cache):
        return chosen(
            residual, q_self, k_self, v_self, w_out, norm_gain, w_query, w_cache, block_doc, tail_len
        )
    local_kv = w_cache.shape[1] // (2 * HEAD_DIM)
    seq_size, head_size = lax.axis_size("seq"), lax.axis_size("head")
    span = min(DOC_BLOCKS, seq_size // 2)
    far = list(range(1, span))
    me, my_head = lax.axis_index("seq"), lax.axis_index("head")

    own_doc = block_doc[me]
    following = jnp.where(me == seq_size - 1, -1, block_doc[jnp.minimum(me + 1, seq_size - 1)])
    live = jnp.where(following != own_doc, jnp.minimum(tail_len[me], rows), rows)
    odd = lax.rem(me, 2) == 1
    small = span == 4 and seq_size % 2 == 0

    def together(distance):
        other = me - distance
        return jnp.logical_and(other >= 0, block_doc[jnp.maximum(other, 0)] == own_doc)

    if small:
        flags = [
            together(1),
            jnp.logical_and(jnp.logical_not(odd), together(2)),
            jnp.where(odd, together(2), together(3)),
            jnp.logical_and(odd, together(3)),
        ]
        distances = [1, 2, 3, 3]
    else:
        flags = [together(distance) for distance in far]
        distances = far
    facts = jnp.stack([live.astype(jnp.int32)] + [flag.astype(jnp.int32) for flag in flags])
    slots = [(1 + i, distance) for i, distance in enumerate(distances)]

    stacked = jnp.concatenate([k_self, v_self], axis=1)
    weight_rows = jnp.concatenate([w_query, w_cache], axis=1)
    state = attend_stage(facts, q_self, [stacked], [(0, 0)], local_heads, None, WINDOW, False)
    if small:
        near, late, state = waves(stacked, odd, state)
    else:
        near, *late = [passed_along(stacked, "seq", offset) for offset in far]

    own_columns = residual.shape[1]
    out_pieces = []
    for flip in range(head_size):
        piece = lax.dynamic_slice_in_dim(w_out, (my_head ^ flip) * own_columns, own_columns, 1)
        out_pieces.append(piece if flip == 0 else swapped(piece, "head", flip))

    state = attend_stage(facts, q_self, [near], slots[:1], local_heads, state, WINDOW, False)
    if small:
        weight_rows, state = lax.optimization_barrier((weight_rows, state))
        weights = jnp.zeros((weight_rows.shape[0] * seq_size, weight_rows.shape[1]), jnp.bfloat16)
        gather = row_gather(weight_rows)
        moving, across, onward, owner = next(gather)
        late, across, onward, out_pieces = lax.optimization_barrier(
            (late, across, onward, out_pieces)
        )
        weights = placed(placed(weights, moving, owner), across, owner ^ 1)
        moving, across, onward, owner = gather.send((moving, across, onward))
    else:
        weights = lax.all_gather(weight_rows, "seq", axis=0, tiled=True)
    context = attend_stage(facts, q_self, late, slots[1:], local_heads, state, WINDOW, True)
    if small:
        context, across, onward = lax.optimization_barrier((context, across, onward))
        weights = placed(placed(weights, moving, owner), across, owner ^ 1)
        moving, across, onward, owner = gather.send((moving, across, onward))

    contexts = shared_over_head(context)
    projected = jnp.dot(contexts[0], out_pieces[0], preferred_element_type=jnp.float32)
    for flip in range(1, head_size):
        projected += jnp.dot(contexts[flip], out_pieces[flip], preferred_element_type=jnp.float32)
    hidden = (residual.astype(jnp.float32) + projected).astype(jnp.bfloat16)
    if small:
        hidden, across, onward = lax.optimization_barrier((hidden, across, onward))
        weights = placed(placed(weights, moving, owner), across, owner ^ 1)
        while onward is not None:
            moving, across, onward, owner = gather.send((moving, across, onward))
            weights = placed(placed(weights, moving, owner), across, owner ^ 1)

    full = jnp.zeros((rows, own_columns * head_size), jnp.bfloat16)
    for flip, piece in enumerate(shared_over_head(hidden)):
        full = lax.dynamic_update_slice_in_dim(full, piece, (my_head ^ flip) * own_columns, 1)
    wide = full.astype(jnp.float32)
    mean_square = jnp.sum(wide * wide, axis=1, keepdims=True) / D
    normed = (wide * lax.rsqrt(mean_square + EPSILON) * norm_gain).astype(jnp.bfloat16)

    cache_rows = jnp.dot(
        normed, weights[:, width:], preferred_element_type=jnp.float32
    ).astype(jnp.bfloat16)
    if small:
        near, late, _ = waves(cache_rows, odd, None)
    else:
        near, *late = [passed_along(cache_rows, "seq", offset) for offset in far]
    cross_queries = jnp.dot(
        normed, weights[:, :width], preferred_element_type=jnp.float32
    ).astype(jnp.bfloat16)
    reach = DOC_BLOCKS * rows
    state = attend_stage(
        facts, cross_queries, [cache_rows, near], [(0, 0)] + slots[:1], local_kv, None, reach, False
    )
    cross_context = attend_stage(
        facts, cross_queries, late, slots[1:], local_kv, state, reach, True
    )
    return (hidden, cross_context)


def solution(mesh):
    in_specs = (
        P("seq", "head"),
        P("seq", "head"),
        P("seq", "head"),
        P("seq", "head"),
        P("head", None),
        P(),
        P("seq", "head"),
        P("seq", "head"),
        P(),
        P(),
    )
    out_specs = (P("seq", "head"), P("seq", "head"))
    return jax.shard_map(local, mesh=mesh, in_specs=in_specs, out_specs=out_specs, check_vma=False)
```

```python
import functools
import math

import jax
import jax.numpy as jnp
import numpy as np
from jax import lax
from jax.experimental import pallas as pl
from jax.experimental.pallas import tpu as pltpu
from jax.sharding import PartitionSpec as P

D = 3072
HEAD_DIM = 128
WINDOW = 2048
DOC_BLOCKS = 5
EPSILON = 1e-06
ROW_TILE = 256


def passed_along(block, axis, distance):
    devices = range(lax.axis_size(axis))
    route = [(i - distance, i) for i in devices if i - distance in devices]
    return lax.ppermute(block, axis, route)


def swapped(block, axis, flip):
    return lax.ppermute(block, axis, [(i, i ^ flip) for i in range(lax.axis_size(axis))])


MESH = pl.DeviceIdType.MESH
TILE = 256
NEG = -1e30
SCALE = math.log2(math.e) / math.sqrt(HEAD_DIM)

BY_HEAD = (
    "ky", "vy", "qy", "kz", "vz", "kvz", "kvr", "cy", "cc", "cyc", "o", "qz", "qzy", "ob", "obb", "lb", "wb1", "wf2",
)
COPIES = (
    "wqy", "wky", "wvy", "wf1", "wf1y", "wf1k", "wf2y", "wf3", "wf3y",
    "wb1y", "wb1k", "wb2", "wb2y", "wb3", "wb3y", "woc0", "woc1",
    "px0", "px1", "px2", "px3", "dx0", "dx1", "dx2", "dx3", "dy0", "dy1", "dy2", "dy3",
    "dc0", "dc1", "dc2", "dc3", "dxc0", "dxc1", "dxc2", "dxc3", "dyc0", "dyc1", "dyc2", "dyc3",
    "far0", "far1", "far2", "far3", "farc0", "farc1", "farc2", "farc3", "e1", "e0", "er",
)
LOCALS = ("wq", "wk", "wv", "res", "gain", "wo0", "wo1", "hid0", "hid1", "hid2", "hid3")
LOCALS_BY_HEAD = ("k", "v", "q", "o")


def fused_kernel(
    far, res_hbm, q_hbm, k_hbm, v_hbm, wo_hbm, gain_hbm, wq_hbm, wc_hbm, doc_ref, tail_ref,
    hid_hbm, out_hbm,
    qx, kv, qu, osend, orecv, lbuf, lsend, lrecv, acc, peak, wo, wfull, ctx, ctxo, po, px, pxb, pxr, hall, nrm, resv, gainv, proj, cq, kvc, outs,
    ss, rs, ls,
):
    s_at, h_at = lax.axis_index("seq"), lax.axis_index("head")
    seq_size = lax.axis_size("seq")
    planes = seq_size // 2
    last = planes - 1
    z, y = s_at // 2, lax.rem(s_at, 2)
    yo = 1 - y
    c_at = lax.rem(h_at, 2)
    co = 1 - c_at
    hx, hc = lax.rem(h_at + 2, 4), h_at + 1 - 2 * c_at
    hxc = lax.rem(hc + 2, 4)
    rows, width = q_hbm.shape
    half = width // 2
    heads = half // HEAD_DIM
    wrows = wq_hbm.shape[0]
    kvw = wc_hbm.shape[1] // 4
    cols = half + 2 * kvw
    quarter = rows // 4
    to_y, to_x, to_c = (z * 2 + yo, h_at), (s_at, hx), (s_at, hc)
    up, down = (s_at + 2, h_at), (s_at - 2, h_at)
    has_up, has_down = z < last, z > 0
    mid = jnp.logical_and(has_up, has_down)
    far_down = z > 1

    def part(at, size):
        return pl.ds(pl.multiple_of(at, size), size)

    def index_of(name, i):
        if i is None:
            return len(BY_HEAD) * heads + COPIES.index(name)
        return BY_HEAD.index(name) * heads + i

    def remote(name, src, dst, device, i=None):
        at = index_of(name, i)
        return pltpu.make_async_remote_copy(
            src_ref=src, dst_ref=dst, send_sem=ss.at[at], recv_sem=rs.at[at],
            device_id=device, device_id_type=MESH,
        )

    def near(name, src, dst, i=None):
        at = LOCALS.index(name) if i is None else len(LOCALS) + LOCALS_BY_HEAD.index(name) * heads + i
        return pltpu.make_async_copy(src, dst, ls.at[at])

    def when(cond, go):
        if cond is None:
            go()
        else:
            pl.when(cond)(go)

    sends = []

    def send(name, src, dst, device, cond=None):
        when(cond, lambda: remote(name, src, dst, device).start())
        sends.append((name, src, dst, device, cond))

    def arrived(name, dst, cond=None, i=None):
        def go():
            remote(name, dst, dst, to_y, i).wait_recv()

        when(cond, go)

    def each_head(body):
        def step(i, carry):
            body(i)
            return carry

        lax.fori_loop(0, heads, step, 0)

    mine, other = part(y * half, half), part(yo * half, half)
    kmine, kother = part(y * kvw, kvw), part(yo * kvw, kvw)
    vmine, vother = part((2 + y) * kvw, kvw), part((2 + yo) * kvw, kvw)
    wrow, wrow_y = part(s_at * wrows, wrows), part((z * 2 + yo) * wrows, wrows)
    wq_c, wk_c, wv_c = pl.ds(0, half), pl.ds(half, kvw), pl.ds(half + kvw, kvw)

    def wchunk(plane):
        return wfull.at[part(plane * 2 * wrows, 2 * wrows), :]

    def own_head(i):
        return part(y * half + i * HEAD_DIM, HEAD_DIM)

    def other_head(i):
        return part(yo * half + i * HEAD_DIM, HEAD_DIM)

    def head_cols(i):
        return part(i * HEAD_DIM, HEAD_DIM)

    barrier = pltpu.get_barrier_semaphore()
    for device in (to_y, to_x, to_c):
        pl.semaphore_signal(barrier, inc=1, device_id=device, device_id_type=MESH)

    @pl.when(has_up)
    def _():
        pl.semaphore_signal(barrier, inc=1, device_id=up, device_id_type=MESH)

    @pl.when(has_down)
    def _():
        pl.semaphore_signal(barrier, inc=1, device_id=down, device_id_type=MESH)

    locals_ = [
        ("wq", wq_hbm.at[:, mine], wfull.at[wrow, wq_c]),
        ("wk", wc_hbm.at[:, kmine], wfull.at[wrow, wk_c]),
        ("wv", wc_hbm.at[:, vmine], wfull.at[wrow, wv_c]),
        ("wo0", wo_hbm.at[:, part(h_at * width, width)], wo.at[c_at, 0]),
        ("wo1", wo_hbm.at[:, part(hx * width, width)], wo.at[c_at, 1]),
        ("res", res_hbm, resv),
        ("gain", gain_hbm, gainv),
    ]

    def local_kvq(i):
        return [
            near("k", k_hbm.at[:, own_head(i)], kv.at[y, i, 0], i),
            near("v", v_hbm.at[:, own_head(i)], kv.at[y, i, 1], i),
            near("q", q_hbm.at[:, own_head(i)], qx.at[y, i], i),
        ]

    for i in range(heads):
        for copy in local_kvq(i):
            copy.start()
    for item in locals_:
        near(*item).start()
    pl.semaphore_wait(barrier, 3 + jnp.where(has_up, 1, 0) + jnp.where(has_down, 1, 0))

    def first_sends(i):
        return [
            (remote("qy", q_hbm.at[:, other_head(i)], qx.at[y, i], to_y, i), None),
            (remote("ky", k_hbm.at[:, other_head(i)], kv.at[y, i, 0], to_y, i), None),
            (remote("vy", v_hbm.at[:, other_head(i)], kv.at[y, i, 1], to_y, i), None),
        ] + ([
            (remote("kz", k_hbm.at[:, own_head(i)], kv.at[2 + y, i, 0], up, i), has_up),
            (remote("vz", v_hbm.at[:, own_head(i)], kv.at[2 + y, i, 1], up, i), has_up),
        ] if far else [
            (remote("qz", q_hbm.at[:, own_head(i)], qu.at[y, i], down, i), has_down),
        ])

    for i in range(heads):
        for copy, cond in first_sends(i):
            when(cond, copy.start)
    send("wqy", wq_hbm.at[:, other], wfull.at[wrow, wq_c], to_y)
    if far:
        send("wky", wc_hbm.at[:, kother], wfull.at[wrow, wk_c], to_y)
        send("wvy", wc_hbm.at[:, vother], wfull.at[wrow, wv_c], to_y)
    send("woc0", wo_hbm.at[:, part(hc * width, width)], wo.at[c_at, 0], to_c)
    send("woc1", wo_hbm.at[:, part(hxc * width, width)], wo.at[c_at, 1], to_c)
    for item in locals_[:3]:
        near(*item).wait()
    third = wrows // heads

    def wthird(block, i):
        return wfull.at[part(block * wrows + i * third, third), :]

    def wb1_copy(i):
        return remote("wb1", wthird(s_at, i), wthird(s_at, i), down, i)

    def wf2_copy(i):
        piece = wthird(jnp.maximum(s_at - 2, 0), i)
        return remote("wf2", piece, piece, up, i)

    if far:
        for i in range(heads):
            when(has_down, wb1_copy(i).start)
    else:
        send("wf1", wfull.at[wrow, :], wfull.at[wrow, :], up, has_up)

    def block_of(j):
        return jnp.where(j < 2, 2 * z + j, jnp.where(j < 4, 2 * z - 4 + j, 2 * z - 3))

    def doc_of(block):
        return doc_ref[jnp.maximum(block, 0)]

    def live_of(block):
        following = jnp.minimum(block + 1, seq_size - 1)
        closing = jnp.logical_or(block == seq_size - 1, doc_ref[following] != doc_ref[block])
        return jnp.where(closing, jnp.minimum(tail_ref[block], rows), rows)

    ones = jnp.ones((rows, HEAD_DIM), jnp.bfloat16)

    def scores_of(q, k):
        return lax.dot_general(q, k, (((1,), (1,)), ((), ())), preferred_element_type=jnp.float32)

    def self_keys(j, i):
        return kv.at[j, i, 0], kv.at[j, i, 1]

    def cross_keys(j, i):
        return kvc.at[j, :, pl.ds(0, kvw)], kvc.at[j, :, pl.ds(kvw, kvw)]

    def diag(queries, keys_of, items):
        for r in range(0, rows, TILE):
            for b, i in items:
                live = live_of(2 * z + b)
                k_ref, v_ref = keys_of(b, i)
                here, keys = pl.ds(r, TILE), r + TILE
                s = scores_of(queries[b, i, here, :], k_ref[pl.ds(0, keys), :])
                q_at = r + lax.broadcasted_iota(jnp.int32, s.shape, 0)
                k_at = lax.broadcasted_iota(jnp.int32, s.shape, 1)
                s = jnp.where((k_at <= q_at) & (k_at < live), s, NEG)
                peak_row = jnp.max(s, axis=1, keepdims=True)
                w = jnp.exp2((s - peak_row) * SCALE).astype(jnp.bfloat16)
                va = jnp.concatenate([v_ref[pl.ds(0, keys), :], ones[:keys]], axis=1)
                acc[b, i, here, :] = jnp.dot(w, va, preferred_element_type=jnp.float32)
                peak[b, i, here, :] = jnp.broadcast_to(peak_row, (TILE, HEAD_DIM))

    def off(queries, keys_of, items, j, size=TILE):
        def tile(t, carry):
            here = part(t * size, size)
            for b, i in items:
                same = doc_of(2 * z + b) == doc_of(block_of(j))
                on = jnp.where(same, 1.0, 0.0)
                gone = jnp.where(same, 0.0, 1e30)
                gain = jnp.where(same, SCALE, 0.0)
                k_ref, v_ref = keys_of(j, i)
                s = scores_of(queries[b, i, here, :], k_ref[...])
                peak_row = jnp.max(s, axis=1, keepdims=True) * on - gone
                old = peak[b, i, here, :]
                new = jnp.maximum(old, peak_row)
                fade = jnp.exp2((old - new) * SCALE)
                w = jnp.exp2(s * gain - (new[:, :1] * gain + gone)).astype(jnp.bfloat16)
                va = jnp.concatenate([v_ref[...], ones], axis=1)
                more = jnp.dot(w, va, preferred_element_type=jnp.float32)
                fades = jnp.concatenate([fade, fade], axis=1)
                acc[b, i, here, :] = acc[b, i, here, :] * fades + more
                peak[b, i, here, :] = new
            return carry

        lax.fori_loop(0, rows // size, tile, 0)

    def all_heads(b):
        return [(b, i) for i in range(heads)]

    def finish(b, i):
        whole = acc[b, i]
        return (whole[:, :HEAD_DIM] / whole[:, HEAD_DIM:]).astype(jnp.bfloat16)

    ahead, ahead2 = jnp.minimum(z + 1, last), jnp.minimum(z + 2, last)
    behind, behind2 = jnp.maximum(z - 1, 0), jnp.maximum(z - 2, 0)
    has_far = z + 2 <= last

    def wpart(plane, side):
        return wfull.at[part((plane * 2 + side) * wrows, wrows), :]

    def pass_on(name, onward, piece, cond, to, to_cond):
        arrived(name, piece, cond)
        send(onward, piece, piece, to, jnp.logical_and(cond, to_cond))

    def qzy_copy(i):
        return remote("qzy", qx.at[yo, i], qu.at[yo, i], down, i)

    def ob_copy(name, i):
        here = pl.ds(0 if name == "ob" else rows // 2, rows // 2)
        return remote(name, osend.at[i, :, here, :], orecv.at[i, :, here, :], up, i)

    def lb_copy(i):
        return remote("lb", lsend.at[i], lrecv.at[i, pl.ds(0, 8), :], up, i)

    def above(i):
        def tile(t, carry):
            here = part(t * TILE, TILE)
            lane = lax.broadcasted_iota(jnp.int32, (TILE, HEAD_DIM), 1)
            logs = jnp.zeros((TILE, HEAD_DIM), jnp.float32)
            for b in range(2):
                query = qu[b, i, here, :]
                scores, tops, marks = [], [], []
                for k in range(2):
                    ahead_doc = doc_of(jnp.minimum(2 * z + 2 + b, seq_size - 1))
                    same = ahead_doc == doc_of(2 * z + k)
                    marks.append((jnp.where(same, SCALE, 0.0), jnp.where(same, 0.0, 1e30)))
                    s = scores_of(query, kv[k, i, 0])
                    scores.append(s)
                    tops.append(jnp.max(s, axis=1, keepdims=True) * jnp.where(same, 1.0, 0.0) - marks[k][1])
                top_row = jnp.maximum(tops[0], tops[1])
                total = None
                for k in range(2):
                    gain, gone = marks[k]
                    w = jnp.exp2(scores[k] * gain - (top_row * gain + gone)).astype(jnp.bfloat16)
                    va = jnp.concatenate([kv[k, i, 1], ones], axis=1)
                    more = jnp.dot(w, va, preferred_element_type=jnp.float32)
                    total = more if total is None else total + more
                weight = total[:, HEAD_DIM:]
                weight = jnp.where(weight > 0.0, weight, 1.0)
                osend[i, b, here, :] = (total[:, :HEAD_DIM] / weight).astype(jnp.bfloat16)
                logs = jnp.where(lane == b, top_row * SCALE + jnp.log2(weight), logs)
            lbuf[here, :] = logs
            when(t == rows // TILE // 2 - 1, ob_copy("ob", i).start)
            return carry

        lax.fori_loop(0, rows // TILE, tile, 0)
        lsend[i] = jnp.transpose(lbuf[...])[:8, :]

    def merged(b, i, logs):
        log_row = jnp.where(has_down, logs[:, b:b + 1], NEG)
        part_row = jnp.where(has_down, orecv[i, b].astype(jnp.float32), 0.0)
        whole, own_log = acc[b, i], peak[b, i] * SCALE
        most = jnp.maximum(own_log, log_row)
        fade, share = jnp.exp2(own_log - most), jnp.exp2(log_row - most)
        above_row = whole[:, :HEAD_DIM] * fade + part_row * share
        return (above_row / (whole[:, HEAD_DIM:] * fade + share)).astype(jnp.bfloat16)

    def stage2(i):
        arrived("qy", qx.at[yo, i], None, i)
        if not far:
            when(has_down, qzy_copy(i).start)
            when(has_down, wb1_copy(i).start)
        arrived("ky", kv.at[yo, i, 0], None, i)
        arrived("vy", kv.at[yo, i, 1], None, i)
        if far:
            when(has_up, remote("kvz", kv.at[yo, i], kv.at[2 + yo, i], up, i).start)
        else:
            @pl.when(has_up)
            def _():
                arrived("qz", qu.at[y, i], None, i)
                arrived("qzy", qu.at[yo, i], None, i)
                above(i)
                ob_copy("obb", i).start()
                lb_copy(i).start()

            when(jnp.logical_and(i == 0, has_down), lambda: arrived("wf1", wpart(behind, y)))
            when(jnp.logical_and(mid, i == 0), wf2_copy(0).start)
        diag(qx, self_keys, [(yo, i)])
        off(qx, self_keys, [(1, i)], 0)
        if far:
            @pl.when(has_down)
            def _():
                arrived("kz", kv.at[2 + y, i, 0], None, i)
                arrived("vz", kv.at[2 + y, i, 1], None, i)
                when(jnp.logical_and(has_up, y == 1), remote("kvr", kv.at[3, i], kv.at[4, i], up, i).start)
                off(qx, self_keys, [(0, i), (1, i)], 2 + y)

    def stage3(i):
        if not far:
            arrived("ob", orecv.at[i, :, pl.ds(0, rows // 2), :], has_down, i)
            arrived("obb", orecv.at[i, :, pl.ds(rows // 2, rows // 2), :], has_down, i)
            arrived("lb", lrecv.at[i, pl.ds(0, 8), :], has_down, i)
            stage5(i)
            return

        @pl.when(has_down)
        def _():
            arrived("kvz", kv.at[2 + yo, i], None, i)
            when(jnp.logical_and(has_up, y == 0), remote("kvr", kv.at[3, i], kv.at[4, i], up, i).start)
            off(qx, self_keys, [(0, i), (1, i)], 2 + yo)

    def stage4(i):
        @pl.when(far_down)
        def _():
            arrived("kvr", kv.at[4, i], None, i)
            off(qx, self_keys, [(0, i)], 4)

        stage5(i)

    def cy_copy(i):
        return remote("cy", ctxo.at[:, head_cols(i)], ctx.at[c_at, y, :, head_cols(i)], to_y, i)

    def cc_copy(i):
        piece = ctx.at[c_at, y, :, head_cols(i)]
        return remote("cc", piece, piece, to_c, i)

    def cyc_copy(i):
        piece = ctx.at[c_at, yo, :, head_cols(i)]
        return remote("cyc", piece, piece, to_c, i)

    def stage5(i):
        if far:
            done = [finish(0, i), finish(1, i)]
        else:
            logs = jnp.transpose(lrecv[i])
            done = [merged(0, i, logs), merged(1, i, logs)]
        ctxo[:, head_cols(i)] = jnp.where(y == 0, done[1], done[0])
        cy_copy(i).start()
        ctx[c_at, y, :, head_cols(i)] = jnp.where(y == 0, done[0], done[1])
        cc_copy(i).start()

    for i in range(heads):
        for copy in local_kvq(i):
            copy.wait()
    diag(qx, self_keys, all_heads(y))
    each_head(stage2)
    if not far:
        for i in range(1, heads):
            when(mid, wf2_copy(i).start)
    each_head(lambda i: arrived("wb1", wthird(jnp.minimum(s_at + 2, seq_size - 1), i), has_up, i))
    send("wb2", wpart(ahead, y), wpart(ahead, y), down, mid)
    each_head(stage3)
    if far:
        send("wf1", wfull.at[wrow, :], wfull.at[wrow, :], up, has_up)
        each_head(stage4)
    if not far:
        send("wky", wc_hbm.at[:, kother], wfull.at[wrow, wk_c], to_y)
        send("wvy", wc_hbm.at[:, vother], wfull.at[wrow, wv_c], to_y)
    wkv_c = pl.ds(half, 2 * kvw)
    arrived("wqy", wfull.at[wrow_y, wq_c])
    send("wf1y", wfull.at[wrow_y, wq_c], wfull.at[wrow_y, wq_c], up, has_up)
    send("wb1y", wfull.at[wrow_y, wq_c], wfull.at[wrow_y, wq_c], down, has_down)

    for item in locals_[3:]:
        near(*item).wait()
    arrived("woc0", wo.at[co, 0])
    arrived("woc1", wo.at[co, 1])

    def project(here, side, column):
        total = None
        for core in range(2):
            more = jnp.dot(
                ctx[core, side, here, :], wo[core, column, part(side * half, half), :],
                preferred_element_type=jnp.float32,
            )
            total = more if total is None else total + more
        return total

    each_head(lambda i: arrived("cc", ctx.at[co, y, :, head_cols(i)], None, i))

    def near_side(t, carry):
        here = part(t * TILE, TILE)
        px[here, :] = project(here, y, 1)
        po[here, :] = project(here, y, 0)
        return carry

    lax.fori_loop(0, rows // TILE, near_side, 0)

    def relay_context(i):
        arrived("cy", ctx.at[c_at, yo, :, head_cols(i)], None, i)
        cyc_copy(i).start()

    each_head(relay_context)
    each_head(lambda i: arrived("cyc", ctx.at[co, yo, :, head_cols(i)], None, i))
    for p in range(4):
        here = pl.ds(p * quarter, quarter)
        pxb[here, :] = (px[here, :] + project(here, yo, 1)).astype(jnp.bfloat16)
        send(f"px{p}", pxb.at[here, :], pxr.at[here, :], to_x)

    arrived("wky", wfull.at[wrow_y, wk_c])
    arrived("wvy", wfull.at[wrow_y, wv_c])
    send("wf1k", wfull.at[wrow_y, wkv_c], wfull.at[wrow_y, wkv_c], up, has_up)
    send("wb1k", wfull.at[wrow_y, wkv_c], wfull.at[wrow_y, wkv_c], down, has_down)
    pass_on("wb2", "wb3", wpart(ahead2, y), has_far, down, has_down)
    if not far:
        each_head(lambda i: arrived("wf2", wthird(jnp.maximum(s_at - 4, 0), i), far_down, i))
        send("wf3", wpart(behind2, y), wpart(behind2, y), up, jnp.logical_and(far_down, has_up))
    if far:
        arrived("wf1", wpart(behind, y), has_down)
        for i in range(heads):
            when(mid, wf2_copy(i).start)

    def far_side(t, carry):
        here = part(t * TILE, TILE)
        po[here, :] = po[here, :] + project(here, yo, 0)
        return carry

    lax.fori_loop(0, rows // TILE, far_side, 0)

    def hpart(b, h, p):
        return hall.at[b, h, pl.ds(p * quarter, quarter), :]

    for p in range(4):
        here = pl.ds(p * quarter, quarter)
        arrived(f"px{p}", pxr.at[here, :])
        total = resv[here, :].astype(jnp.float32) + (po[here, :] + pxr[here, :].astype(jnp.float32))
        hall[y, h_at, here, :] = total.astype(jnp.bfloat16)
        piece = hpart(y, h_at, p)
        send(f"dx{p}", piece, piece, to_x)
        send(f"dy{p}", piece, piece, to_y)
        send(f"dc{p}", piece, piece, to_c)
        near(f"hid{p}", piece, hid_hbm.at[here, :]).start()
        if p == 1:
            arrived("wb1y", wfull.at[part((ahead * 2 + yo) * wrows, wrows), wq_c], has_up)
            arrived("wb1k", wfull.at[part((ahead * 2 + yo) * wrows, wrows), wkv_c], has_up)
            send("wb2y", wpart(ahead, yo), wpart(ahead, yo), down, mid)
        if p == 2:
            arrived("wf1y", wfull.at[part((behind * 2 + yo) * wrows, wrows), wq_c], has_down)
            arrived("wf1k", wfull.at[part((behind * 2 + yo) * wrows, wrows), wkv_c], has_down)
            send("wf2y", wpart(behind, yo), wpart(behind, yo), up, mid)

    def from_x(p):
        piece = hpart(y, hx, p)
        arrived(f"dx{p}", piece)
        send(f"dxc{p}", piece, piece, to_c)
        if p < 3:
            send(f"far{p}", piece, piece, to_y)

    def from_y(p):
        piece = hpart(yo, h_at, p)
        arrived(f"dy{p}", piece)
        send(f"dyc{p}", piece, piece, to_c)
        if p == 3:
            send("far3", piece, piece, to_x)

    def from_far(p):
        piece = hpart(yo, hx, p)
        arrived(f"far{p}", piece)
        send(f"farc{p}", piece, piece, to_c)

    def own_rows(p):
        arrived(f"dc{p}", hpart(y, hc, p))
        arrived(f"dxc{p}", hpart(y, hxc, p))

    def other_rows(p):
        arrived(f"dyc{p}", hpart(yo, hc, p))
        arrived(f"farc{p}", hpart(yo, hxc, p))

    for p in range(3):
        from_y(p)
    from_x(0)
    from_y(3)
    if far:
        each_head(lambda i: arrived("wf2", wthird(jnp.maximum(s_at - 4, 0), i), far_down, i))
        send("wf3", wpart(behind2, y), wpart(behind2, y), up, jnp.logical_and(far_down, has_up))
    pass_on("wb2y", "wb3y", wpart(ahead2, yo), has_far, down, has_down)
    from_x(1)
    pass_on("wf2y", "wf3y", wpart(behind2, yo), far_down, up, has_up)

    def norm(b, at):
        square = jnp.zeros((quarter, 1), jnp.float32)
        here = part(at * quarter, quarter)
        for h in range(hall.shape[1]):
            wide = hall[b, h, here, :].astype(jnp.float32)
            square += jnp.sum(wide * wide, axis=1, keepdims=True)
        scale = lax.rsqrt(square / D + EPSILON)
        for h in range(hall.shape[1]):
            wide = hall[b, h, here, :].astype(jnp.float32)
            gains = gainv[:, pl.ds(h * width, width)]
            nrm[b, h, here, :] = (wide * scale * gains).astype(jnp.bfloat16)

    def norm_half(b, p):
        def step(n, carry):
            norm(b, 2 * p + n)
            return carry

        lax.fori_loop(0, 2, step, 0)

    def cross_tile(k, b, t, where, first):
        here = part(t * TILE, TILE)
        more = jnp.dot(
            nrm[b, k, here, :], wfull[part(k * 2 * wrows, 2 * wrows), where],
            preferred_element_type=jnp.float32,
        )
        proj[b, here, where] = more if first else proj[b, here, where] + more

    def cross_part(k, b, where, first):
        def tile(t, carry):
            cross_tile(k, b, t, where, first)
            return carry

        lax.fori_loop(0, rows // TILE, tile, 0)

    low = z < planes // 2
    order = [z, jnp.where(low, 1 - z, 5 - z), jnp.where(low, 2, 1), jnp.where(low, 3, 0)]
    every = pl.ds(0, cols)

    def chunks(b, t):
        def step(n, carry):
            cross_tile(jnp.where(n == 0, order[1], order[2]), b, t, every, False)
            return carry

        cross_tile(order[0], b, t, every, True)
        lax.fori_loop(0, 2, step, 0)

    own_rows(0)
    own_rows(1)
    norm_half(y, 0)
    chunks(y, 0)
    from_x(2)
    from_far(0)
    from_far(1)
    from_x(3)
    other_rows(0)
    other_rows(1)
    norm_half(yo, 0)
    chunks(yo, 0)
    from_far(2)
    own_rows(2)
    own_rows(3)
    norm_half(y, 1)
    from_far(3)
    chunks(y, 1)
    other_rows(2)
    other_rows(3)
    norm_half(yo, 1)
    chunks(yo, 1)
    for name, plane, cond in (("wf3", 0, z == last), ("wb3", last, z == 0)):
        arrived(name, wpart(plane, y), cond)
        arrived(name + "y", wpart(plane, yo), cond)

    cache_c, query_c = pl.ds(half, 2 * kvw), pl.ds(0, half)

    def cache_out(b):
        cross_part(order[3], b, cache_c, False)
        kvc[b] = proj[b, :, cache_c].astype(jnp.bfloat16)

    cache_out(1)
    send("e1", kvc.at[1], kvc.at[3], up, has_up)
    cache_out(0)
    send("e0", kvc.at[0], kvc.at[2], up, has_up)

    def query_out(b, carry):
        cross_part(order[3], b, query_c, False)
        for i in range(heads):
            cq[b, i] = proj[b, :, pl.ds(i * HEAD_DIM, HEAD_DIM)].astype(jnp.bfloat16)
        return carry

    lax.fori_loop(0, 2, query_out, 0)

    def own_diag(b, carry):
        diag(cq, cross_keys, all_heads(b))
        return carry

    lax.fori_loop(0, 2, own_diag, 0)

    def home_copy(i):
        return near("o", outs.at[y, i], out_hbm.at[:, own_head(i)], i)

    def away_copy(i):
        return remote("o", outs.at[yo, i], out_hbm.at[:, own_head(i)], to_y, i)

    plan = [(1, 0), (yo, 3), (y, 3)] + ([(0, 4)] if far else []) + [(yo, 2), (y, 2)]

    def look_up(n, which):
        value = plan[0][which]
        for at in range(1, len(plan)):
            value = jnp.where(n == at, plan[at][which], value)
        return value

    def step(n, carry):
        if far:
            @pl.when(jnp.logical_and(n == 0, has_down))
            def _():
                arrived("e1", kvc.at[3])
                when(has_up, remote("er", kvc.at[3], kvc.at[4], up).start)

            when(jnp.logical_and(n == 3, far_down), lambda: arrived("er", kvc.at[4]))
            runs = jnp.where(n == 3, far_down, jnp.logical_or(n == 0, has_down))
        else:
            when(jnp.logical_and(n == 1, has_down), lambda: arrived("e1", kvc.at[3]))
            runs = jnp.logical_or(n == 0, has_down)
        when(jnp.logical_and(n == len(plan) - 2, has_down), lambda: arrived("e0", kvc.at[2]))
        b, j = look_up(n, 0), look_up(n, 1)
        when(runs, lambda: off(cq, cross_keys, all_heads(b), j, rows))

        @pl.when(n >= len(plan) - 2)
        def _():
            for i in range(heads):
                outs[b, i] = finish(b, i)
                when(n == len(plan) - 2, away_copy(i).start)
                when(n == len(plan) - 1, home_copy(i).start)

        return carry

    lax.fori_loop(0, len(plan), step, 0)
    if far:
        sends.append(("er", kvc.at[3], kvc.at[4], up, mid))

    for p in range(4):
        near(f"hid{p}", hpart(y, h_at, p), hid_hbm.at[pl.ds(p * quarter, quarter), :]).wait()
    for name, src, dst, device, cond in sends:
        when(cond, remote(name, src, dst, device).wait_send)

    def ended(i):
        for copy, cond in first_sends(i):
            when(cond, copy.wait_send)
        when(has_down, wb1_copy(i).wait_send)
        when(mid, wf2_copy(i).wait_send)
        if not far:
            when(has_down, qzy_copy(i).wait_send)
            when(has_up, ob_copy("ob", i).wait_send)
            when(has_up, ob_copy("obb", i).wait_send)
            when(has_up, lb_copy(i).wait_send)
        if far:
            when(has_up, remote("kvz", kv.at[yo, i], kv.at[2 + yo, i], up, i).wait_send)
            when(mid, remote("kvr", kv.at[3, i], kv.at[4, i], up, i).wait_send)
        cy_copy(i).wait_send()
        cc_copy(i).wait_send()
        cyc_copy(i).wait_send()
        home_copy(i).wait()
        away_copy(i).wait_send()
        arrived("o", out_hbm.at[:, other_head(i)], None, i)

    each_head(ended)


def settle_kernel(hid_ref, out_ref, hid_to, out_to):
    hid_to[...] = hid_ref[...]
    out_to[...] = out_ref[...]


def settled(hid, out):
    rows, width = hid.shape
    spec = pl.BlockSpec((rows // 2, width), lambda i: (i, 0))
    return pl.pallas_call(
        settle_kernel,
        out_shape=(jax.ShapeDtypeStruct(hid.shape, hid.dtype),) * 2,
        grid=(2,),
        in_specs=[spec, spec],
        out_specs=(spec, spec),
        compiler_params=pltpu.CompilerParams(vmem_limit_bytes=60 * 1024 * 1024),
    )(hid, out)


def fused(far, residual, q_self, k_self, v_self, w_out, norm_gain, w_query, w_cache, block_doc, tail_len):
    rows, width = q_self.shape
    seq_size, head_size = lax.axis_size("seq"), lax.axis_size("head")
    half = width // 2
    heads = half // HEAD_DIM
    kvw = w_cache.shape[1] // 4
    cols = half + 2 * kvw
    bf, f32 = jnp.bfloat16, jnp.float32
    hbm = pl.BlockSpec(memory_space=pl.ANY)
    smem = pl.BlockSpec(memory_space=pltpu.SMEM)
    copies = len(BY_HEAD) * heads + len(COPIES)
    scratch = [
        pltpu.VMEM((2, heads, rows, HEAD_DIM), bf),
        pltpu.VMEM((5 if far else 2, heads, 2, rows, HEAD_DIM), bf),
        pltpu.VMEM((2, heads, rows, HEAD_DIM), bf),
        pltpu.VMEM((heads, 2, rows, HEAD_DIM), bf),
        pltpu.VMEM((heads, 2, rows, HEAD_DIM), bf),
        pltpu.VMEM((rows, HEAD_DIM), f32),
        pltpu.VMEM((heads, 8, rows), f32),
        pltpu.VMEM((heads, HEAD_DIM, rows), f32),
        pltpu.VMEM((2, heads, rows, 2 * HEAD_DIM), f32),
        pltpu.VMEM((2, heads, rows, HEAD_DIM), f32),
        pltpu.VMEM((2, 2, width, width), bf),
        pltpu.VMEM((w_query.shape[0] * seq_size, cols), bf),
        pltpu.VMEM((2, 2, rows, half), bf),
        pltpu.VMEM((rows, half), bf),
        pltpu.VMEM((rows, width), f32),
        pltpu.VMEM((rows, width), f32),
        pltpu.VMEM((rows, width), bf),
        pltpu.VMEM((rows, width), bf),
        pltpu.VMEM((2, head_size, rows, width), bf),
        pltpu.VMEM((2, head_size, rows, width), bf),
        pltpu.VMEM((rows, width), bf),
        pltpu.VMEM((1, head_size * width), f32),
        pltpu.VMEM((2, rows, cols), f32),
        pltpu.VMEM((2, heads, rows, HEAD_DIM), bf),
        pltpu.VMEM((5 if far else 4, rows, 2 * kvw), bf),
        pltpu.VMEM((2, heads, rows, HEAD_DIM), bf),
        pltpu.SemaphoreType.DMA((copies,)),
        pltpu.SemaphoreType.DMA((copies,)),
        pltpu.SemaphoreType.DMA((len(LOCALS) + len(LOCALS_BY_HEAD) * heads,)),
    ]
    wide = jax.ShapeDtypeStruct((rows, width), bf)
    return pl.pallas_call(
        functools.partial(fused_kernel, far),
        out_shape=(wide, wide),
        in_specs=[hbm] * 8 + [smem] * 2,
        out_specs=(hbm, hbm),
        scratch_shapes=scratch,
        compiler_params=pltpu.CompilerParams(
            collective_id=1 if far else 0, has_side_effects=True, vmem_limit_bytes=60 * 1024 * 1024
        ),
    )(
        residual, q_self, k_self, v_self, w_out, norm_gain.reshape(1, head_size * width),
        w_query, w_cache, block_doc, tail_len,
    )


def chosen(*args):
    block_doc = args[8]
    at = np.arange(block_doc.shape[0])
    apart = (at[None, :] - at[:, None] == 3) & (at[None, :] % 2 == 0)
    far = jnp.any((block_doc[:, None] == block_doc[None, :]) & apart)
    hid, out = lax.cond(far, functools.partial(fused, True), functools.partial(fused, False), *args)
    return settled(hid, out)


def stage_kernel(offsets, window, first, last, facts, q_ref, *refs):
    pairs = [(refs[2 * i], refs[2 * i + 1]) for i in range(len(offsets))]
    rest = refs[2 * len(offsets):]
    if not first:
        acc_in, peak_in, total_in = rest[:3]
        rest = rest[3:]
    if last:
        out_ref = rest[0]
        acc, peak, total = rest[1:]
    else:
        acc, peak, total = rest
    rows = q_ref.shape[0]
    tile = min(ROW_TILE, rows)
    scaling = math.log2(math.e) / math.sqrt(HEAD_DIM)

    def scores_of(r, k):
        return lax.dot_general(
            q_ref[pl.ds(r, tile), :], k, (((1,), (1,)), ((), ())),
            preferred_element_type=jnp.float32,
        )

    if not first:
        acc[...] = acc_in[...]
        peak[...] = peak_in[...]
        total[...] = total_in[...]

    for (k_ref, v_ref), (flag, offset) in zip(pairs, offsets):

        def one(offset=offset, k_ref=k_ref, v_ref=v_ref):
            for r in range(0, rows, tile):
                here = pl.ds(r, tile)
                keys = r + tile if offset == 0 else rows
                s = scores_of(r, k_ref[pl.ds(0, keys), :])
                if offset == 0:
                    q_at = r + lax.broadcasted_iota(jnp.int32, s.shape, 0)
                    k_at = lax.broadcasted_iota(jnp.int32, s.shape, 1)
                    s = jnp.where((k_at <= q_at) & (k_at < facts[0]), s, -1e30)
                elif offset * rows + rows - 1 >= window:
                    q_at = r + lax.broadcasted_iota(jnp.int32, s.shape, 0)
                    k_at = lax.broadcasted_iota(jnp.int32, s.shape, 1)
                    s = jnp.where(offset * rows + q_at - k_at < window, s, -1e30)
                top = jnp.max(s, axis=1, keepdims=True)
                if offset == 0:
                    w = jnp.exp2((s - top) * scaling)
                    part = jnp.dot(
                        w.astype(jnp.bfloat16), v_ref[pl.ds(0, keys), :],
                        preferred_element_type=jnp.float32,
                    )
                    acc[here, :] = part
                    total[here, :] = jnp.broadcast_to(
                        jnp.sum(w, axis=1, keepdims=True), (tile, HEAD_DIM)
                    )
                    peak[here, :] = jnp.broadcast_to(top, (tile, HEAD_DIM))
                else:
                    old = peak[here, :]
                    new = jnp.maximum(old, top)
                    w = jnp.exp2((s - new[:, :1]) * scaling)
                    fade = jnp.exp2((old - new) * scaling)
                    part = jnp.dot(
                        w.astype(jnp.bfloat16), v_ref[...], preferred_element_type=jnp.float32
                    )
                    acc[here, :] = acc[here, :] * fade + part
                    total[here, :] = total[here, :] * fade + jnp.sum(w, axis=1, keepdims=True)
                    peak[here, :] = new

        if offset == 0:
            one()
        else:
            pl.when(facts[flag] > 0)(one)

    if last:
        out_ref[...] = (acc[...] / total[...]).astype(jnp.bfloat16)


def attend_stage(facts, queries, blocks, offsets, kv_heads, state, window, last):
    rows, width = queries.shape
    heads = width // HEAD_DIM
    group = heads // kv_heads
    tall = pl.BlockSpec((rows, HEAD_DIM), lambda h, f: (0, h))
    key_spec = pl.BlockSpec((rows, HEAD_DIM), lambda h, f: (0, h // group))
    value_spec = pl.BlockSpec((rows, HEAD_DIM), lambda h, f: (0, kv_heads + h // group))
    operands, specs = [queries], [tall]
    for block in blocks:
        operands += [block, block]
        specs += [key_spec, value_spec]
    if state is not None:
        operands += list(state)
        specs += [tall] * 3
    wide = jax.ShapeDtypeStruct((rows, width), jnp.float32)
    if last:
        out_shape = jax.ShapeDtypeStruct((rows, width), jnp.bfloat16)
        out_specs = tall
        scratch = [pltpu.VMEM((rows, HEAD_DIM), jnp.float32)] * 3
    else:
        out_shape, out_specs, scratch = (wide,) * 3, (tall,) * 3, []
    flops = 4 * rows * rows * width * len(offsets) * 3
    return pl.pallas_call(
        functools.partial(stage_kernel, offsets, window, state is None, last),
        out_shape=out_shape,
        grid_spec=pltpu.PrefetchScalarGridSpec(
            num_scalar_prefetch=1, grid=(heads,), in_specs=specs, out_specs=out_specs,
            scratch_shapes=scratch,
        ),
        compiler_params=pltpu.CompilerParams(
            dimension_semantics=("arbitrary",), vmem_limit_bytes=32 * 1024 * 1024
        ),
        cost_estimate=pl.CostEstimate(
            flops=flops, bytes_accessed=rows * width * 2 * (2 + 2 * len(offsets)),
            transcendentals=0,
        ),
    )(facts, *operands)


def shared_over_head(block):
    size = lax.axis_size("head")
    held = [block]
    step = size // 2
    got = {0: block}
    while step >= 1:
        for flip in sorted(got):
            got[flip ^ step] = None if got[flip] is None else swapped(got[flip], "head", step)
        step //= 2
    held = [got[flip] for flip in range(size)]
    return held


def sent(block, routes):
    return lax.ppermute(block, "seq", routes)


def row_gather(block):
    size = lax.axis_size("seq")
    me = lax.axis_index("seq")
    ring = [(i, (i + 2) % size) for i in range(size)]
    steps = []
    moving = block
    for step in range(size // 2):
        owner = lax.rem(me - 2 * step + size, size)
        across = swapped(moving, "seq", 1)
        onward = sent(moving, ring) if step + 1 < size // 2 else None
        moving, across, onward = yield moving, across, onward, owner
        moving = onward


def placed(whole, piece, owner):
    return lax.dynamic_update_slice_in_dim(whole, piece, owner * piece.shape[0], 0)


def waves(block, odd, beside):
    size = lax.axis_size("seq")
    first = sent(block, [(i, i + 1) for i in range(size - 1)])
    second_even = sent(block, [(i, i + 2) for i in range(0, size - 2, 2)])
    if beside is not None:
        first, beside = lax.optimization_barrier((first, beside))
    mixed = jnp.where(odd, block, first)
    second = sent(mixed, [(i, i + 2) for i in range(size - 2)])
    third_odd = sent(second_even, [(i, i + 1) for i in range(2, size, 2)])
    return first, [second_even, second, third_odd], beside


def fits(q_self, w_cache):
    seq_size, head_size = lax.axis_size("seq"), lax.axis_size("head")
    return (
        seq_size == 8 and head_size == 4 and q_self.shape[1] == 6 * HEAD_DIM
        and w_cache.shape[1] == 4 * HEAD_DIM and q_self.shape[0] % TILE == 0
    )


def local(
    residual, q_self, k_self, v_self, w_out, norm_gain, w_query, w_cache, block_doc, tail_len
):
    rows, width = q_self.shape
    local_heads = width // HEAD_DIM
    if fits(q_self, w_cache):
        return chosen(
            residual, q_self, k_self, v_self, w_out, norm_gain, w_query, w_cache, block_doc, tail_len
        )
    local_kv = w_cache.shape[1] // (2 * HEAD_DIM)
    seq_size, head_size = lax.axis_size("seq"), lax.axis_size("head")
    span = min(DOC_BLOCKS, seq_size // 2)
    far = list(range(1, span))
    me, my_head = lax.axis_index("seq"), lax.axis_index("head")

    own_doc = block_doc[me]
    following = jnp.where(me == seq_size - 1, -1, block_doc[jnp.minimum(me + 1, seq_size - 1)])
    live = jnp.where(following != own_doc, jnp.minimum(tail_len[me], rows), rows)
    odd = lax.rem(me, 2) == 1
    small = span == 4 and seq_size % 2 == 0

    def together(distance):
        other = me - distance
        return jnp.logical_and(other >= 0, block_doc[jnp.maximum(other, 0)] == own_doc)

    if small:
        flags = [
            together(1),
            jnp.logical_and(jnp.logical_not(odd), together(2)),
            jnp.where(odd, together(2), together(3)),
            jnp.logical_and(odd, together(3)),
        ]
        distances = [1, 2, 3, 3]
    else:
        flags = [together(distance) for distance in far]
        distances = far
    facts = jnp.stack([live.astype(jnp.int32)] + [flag.astype(jnp.int32) for flag in flags])
    slots = [(1 + i, distance) for i, distance in enumerate(distances)]

    stacked = jnp.concatenate([k_self, v_self], axis=1)
    weight_rows = jnp.concatenate([w_query, w_cache], axis=1)
    state = attend_stage(facts, q_self, [stacked], [(0, 0)], local_heads, None, WINDOW, False)
    if small:
        near, late, state = waves(stacked, odd, state)
    else:
        near, *late = [passed_along(stacked, "seq", offset) for offset in far]

    own_columns = residual.shape[1]
    out_pieces = []
    for flip in range(head_size):
        piece = lax.dynamic_slice_in_dim(w_out, (my_head ^ flip) * own_columns, own_columns, 1)
        out_pieces.append(piece if flip == 0 else swapped(piece, "head", flip))

    state = attend_stage(facts, q_self, [near], slots[:1], local_heads, state, WINDOW, False)
    if small:
        weight_rows, state = lax.optimization_barrier((weight_rows, state))
        weights = jnp.zeros((weight_rows.shape[0] * seq_size, weight_rows.shape[1]), jnp.bfloat16)
        gather = row_gather(weight_rows)
        moving, across, onward, owner = next(gather)
        late, across, onward, out_pieces = lax.optimization_barrier(
            (late, across, onward, out_pieces)
        )
        weights = placed(placed(weights, moving, owner), across, owner ^ 1)
        moving, across, onward, owner = gather.send((moving, across, onward))
    else:
        weights = lax.all_gather(weight_rows, "seq", axis=0, tiled=True)
    context = attend_stage(facts, q_self, late, slots[1:], local_heads, state, WINDOW, True)
    if small:
        context, across, onward = lax.optimization_barrier((context, across, onward))
        weights = placed(placed(weights, moving, owner), across, owner ^ 1)
        moving, across, onward, owner = gather.send((moving, across, onward))

    contexts = shared_over_head(context)
    projected = jnp.dot(contexts[0], out_pieces[0], preferred_element_type=jnp.float32)
    for flip in range(1, head_size):
        projected += jnp.dot(contexts[flip], out_pieces[flip], preferred_element_type=jnp.float32)
    hidden = (residual.astype(jnp.float32) + projected).astype(jnp.bfloat16)
    if small:
        hidden, across, onward = lax.optimization_barrier((hidden, across, onward))
        weights = placed(placed(weights, moving, owner), across, owner ^ 1)
        while onward is not None:
            moving, across, onward, owner = gather.send((moving, across, onward))
            weights = placed(placed(weights, moving, owner), across, owner ^ 1)

    full = jnp.zeros((rows, own_columns * head_size), jnp.bfloat16)
    for flip, piece in enumerate(shared_over_head(hidden)):
        full = lax.dynamic_update_slice_in_dim(full, piece, (my_head ^ flip) * own_columns, 1)
    wide = full.astype(jnp.float32)
    mean_square = jnp.sum(wide * wide, axis=1, keepdims=True) / D
    normed = (wide * lax.rsqrt(mean_square + EPSILON) * norm_gain).astype(jnp.bfloat16)

    cache_rows = jnp.dot(
        normed, weights[:, width:], preferred_element_type=jnp.float32
    ).astype(jnp.bfloat16)
    if small:
        near, late, _ = waves(cache_rows, odd, None)
    else:
        near, *late = [passed_along(cache_rows, "seq", offset) for offset in far]
    cross_queries = jnp.dot(
        normed, weights[:, :width], preferred_element_type=jnp.float32
    ).astype(jnp.bfloat16)
    reach = DOC_BLOCKS * rows
    state = attend_stage(
        facts, cross_queries, [cache_rows, near], [(0, 0)] + slots[:1], local_kv, None, reach, False
    )
    cross_context = attend_stage(
        facts, cross_queries, late, slots[1:], local_kv, state, reach, True
    )
    return (hidden, cross_context)


def solution(mesh):
    in_specs = (
        P("seq", "head"),
        P("seq", "head"),
        P("seq", "head"),
        P("seq", "head"),
        P("head", None),
        P(),
        P("seq", "head"),
        P("seq", "head"),
        P(),
        P(),
    )
    out_specs = (P("seq", "head"), P("seq", "head"))
    return jax.shard_map(local, mesh=mesh, in_specs=in_specs, out_specs=out_specs, check_vma=False)
```

```python
import functools
import math

import jax
import jax.numpy as jnp
import numpy as np
from jax import lax
from jax.experimental import pallas as pl
from jax.experimental.pallas import tpu as pltpu
from jax.sharding import PartitionSpec as P

D = 3072
HEAD_DIM = 128
WINDOW = 2048
DOC_BLOCKS = 5
EPSILON = 1e-06
ROW_TILE = 256


def passed_along(block, axis, distance):
    devices = range(lax.axis_size(axis))
    route = [(i - distance, i) for i in devices if i - distance in devices]
    return lax.ppermute(block, axis, route)


def swapped(block, axis, flip):
    return lax.ppermute(block, axis, [(i, i ^ flip) for i in range(lax.axis_size(axis))])


MESH = pl.DeviceIdType.MESH
TILE = 256
NEG = -1e30
SCALE = math.log2(math.e) / math.sqrt(HEAD_DIM)

BY_HEAD = (
    "ky", "vy", "qy", "cy", "cc", "cyc", "o", "qz", "qzy", "ob", "obb", "lb", "wb1", "wf2",
)
FAR_BY_HEAD = ("quu", "o2", "l2", "o3", "l3")
COPIES = (
    "wqy", "wky", "wvy", "wf1", "wf1y", "wf1k", "wf2y", "wf3", "wf3y",
    "wb1y", "wb1k", "wb2", "wb2y", "wb3", "wb3y", "woc0", "woc1",
    "px0", "px1", "px2", "px3", "dx0", "dx1", "dx2", "dx3", "dy0", "dy1", "dy2", "dy3",
    "dc0", "dc1", "dc2", "dc3", "dxc0", "dxc1", "dxc2", "dxc3", "dyc0", "dyc1", "dyc2", "dyc3",
    "far0", "far1", "far2", "far3", "farc0", "farc1", "farc2", "farc3", "e1", "e0", "er",
)
LOCALS = ("wq", "wk", "wv", "res", "gain", "wo0", "wo1", "hid0", "hid1", "hid2", "hid3")
LOCALS_BY_HEAD = ("k", "v", "q", "o")


def fused_kernel(
    far, res_hbm, q_hbm, k_hbm, v_hbm, wo_hbm, gain_hbm, wq_hbm, wc_hbm, doc_ref, tail_ref,
    hid_hbm, out_hbm,
    qx, kv, qu, osend, orecv, lbuf, lsend, lrecv, quu, osend2, orecv2, orecv3, lrecv2, lrecv3, acc, peak, wo, wfull, ctx, ctxo, po, px, pxb, pxr, hall, nrm, resv, gainv, proj, cq, kvc, outs,
    ss, rs, ls,
):
    s_at, h_at = lax.axis_index("seq"), lax.axis_index("head")
    seq_size = lax.axis_size("seq")
    planes = seq_size // 2
    last = planes - 1
    z, y = s_at // 2, lax.rem(s_at, 2)
    yo = 1 - y
    c_at = lax.rem(h_at, 2)
    co = 1 - c_at
    hx, hc = lax.rem(h_at + 2, 4), h_at + 1 - 2 * c_at
    hxc = lax.rem(hc + 2, 4)
    rows, width = q_hbm.shape
    half = width // 2
    heads = half // HEAD_DIM
    wrows = wq_hbm.shape[0]
    kvw = wc_hbm.shape[1] // 4
    cols = half + 2 * kvw
    quarter = rows // 4
    to_y, to_x, to_c = (z * 2 + yo, h_at), (s_at, hx), (s_at, hc)
    up, down = (s_at + 2, h_at), (s_at - 2, h_at)
    has_up, has_down = z < last, z > 0
    mid = jnp.logical_and(has_up, has_down)
    far_down = z > 1

    by_head = BY_HEAD + (FAR_BY_HEAD if far else ())

    def part(at, size):
        return pl.ds(pl.multiple_of(at, size), size)

    def index_of(name, i):
        if i is None:
            return len(by_head) * heads + COPIES.index(name)
        return by_head.index(name) * heads + i

    def remote(name, src, dst, device, i=None):
        at = index_of(name, i)
        return pltpu.make_async_remote_copy(
            src_ref=src, dst_ref=dst, send_sem=ss.at[at], recv_sem=rs.at[at],
            device_id=device, device_id_type=MESH,
        )

    def near(name, src, dst, i=None):
        at = LOCALS.index(name) if i is None else len(LOCALS) + LOCALS_BY_HEAD.index(name) * heads + i
        return pltpu.make_async_copy(src, dst, ls.at[at])

    def when(cond, go):
        if cond is None:
            go()
        else:
            pl.when(cond)(go)

    sends = []

    def send(name, src, dst, device, cond=None):
        when(cond, lambda: remote(name, src, dst, device).start())
        sends.append((name, src, dst, device, cond))

    def arrived(name, dst, cond=None, i=None):
        def go():
            remote(name, dst, dst, to_y, i).wait_recv()

        when(cond, go)

    def each_head(body):
        def step(i, carry):
            body(i)
            return carry

        lax.fori_loop(0, heads, step, 0)

    mine, other = part(y * half, half), part(yo * half, half)
    kmine, kother = part(y * kvw, kvw), part(yo * kvw, kvw)
    vmine, vother = part((2 + y) * kvw, kvw), part((2 + yo) * kvw, kvw)
    wrow, wrow_y = part(s_at * wrows, wrows), part((z * 2 + yo) * wrows, wrows)
    wq_c, wk_c, wv_c = pl.ds(0, half), pl.ds(half, kvw), pl.ds(half + kvw, kvw)

    def wchunk(plane):
        return wfull.at[part(plane * 2 * wrows, 2 * wrows), :]

    def own_head(i):
        return part(y * half + i * HEAD_DIM, HEAD_DIM)

    def other_head(i):
        return part(yo * half + i * HEAD_DIM, HEAD_DIM)

    def head_cols(i):
        return part(i * HEAD_DIM, HEAD_DIM)

    barrier = pltpu.get_barrier_semaphore()
    for device in (to_y, to_x, to_c):
        pl.semaphore_signal(barrier, inc=1, device_id=device, device_id_type=MESH)

    @pl.when(has_up)
    def _():
        pl.semaphore_signal(barrier, inc=1, device_id=up, device_id_type=MESH)

    @pl.when(has_down)
    def _():
        pl.semaphore_signal(barrier, inc=1, device_id=down, device_id_type=MESH)

    locals_ = [
        ("wq", wq_hbm.at[:, mine], wfull.at[wrow, wq_c]),
        ("wk", wc_hbm.at[:, kmine], wfull.at[wrow, wk_c]),
        ("wv", wc_hbm.at[:, vmine], wfull.at[wrow, wv_c]),
        ("wo0", wo_hbm.at[:, part(h_at * width, width)], wo.at[c_at, 0]),
        ("wo1", wo_hbm.at[:, part(hx * width, width)], wo.at[c_at, 1]),
        ("res", res_hbm, resv),
        ("gain", gain_hbm, gainv),
    ]

    def local_kvq(i):
        return [
            near("k", k_hbm.at[:, own_head(i)], kv.at[y, i, 0], i),
            near("v", v_hbm.at[:, own_head(i)], kv.at[y, i, 1], i),
            near("q", q_hbm.at[:, own_head(i)], qx.at[y, i], i),
        ]

    for i in range(heads):
        for copy in local_kvq(i):
            copy.start()
    for item in locals_:
        near(*item).start()
    pl.semaphore_wait(barrier, 3 + jnp.where(has_up, 1, 0) + jnp.where(has_down, 1, 0))

    def first_sends(i):
        return [
            (remote("qy", q_hbm.at[:, other_head(i)], qx.at[y, i], to_y, i), None),
            (remote("ky", k_hbm.at[:, other_head(i)], kv.at[y, i, 0], to_y, i), None),
            (remote("vy", v_hbm.at[:, other_head(i)], kv.at[y, i, 1], to_y, i), None),
            (remote("qz", q_hbm.at[:, own_head(i)], qu.at[y, i], down, i), has_down),
        ]

    for i in range(heads):
        for copy, cond in first_sends(i):
            when(cond, copy.start)
    send("wqy", wq_hbm.at[:, other], wfull.at[wrow, wq_c], to_y)
    send("woc0", wo_hbm.at[:, part(hc * width, width)], wo.at[c_at, 0], to_c)
    send("woc1", wo_hbm.at[:, part(hxc * width, width)], wo.at[c_at, 1], to_c)
    for item in locals_[:3]:
        near(*item).wait()
    third = wrows // heads

    def wthird(block, i):
        return wfull.at[part(block * wrows + i * third, third), :]

    def wb1_copy(i):
        return remote("wb1", wthird(s_at, i), wthird(s_at, i), down, i)

    def wf2_copy(i):
        piece = wthird(jnp.maximum(s_at - 2, 0), i)
        return remote("wf2", piece, piece, up, i)

    send("wf1", wfull.at[wrow, :], wfull.at[wrow, :], up, has_up)

    def block_of(j):
        return jnp.where(j < 2, 2 * z + j, jnp.where(j < 4, 2 * z - 4 + j, 2 * z - 3))

    def doc_of(block):
        return doc_ref[jnp.maximum(block, 0)]

    def live_of(block):
        following = jnp.minimum(block + 1, seq_size - 1)
        closing = jnp.logical_or(block == seq_size - 1, doc_ref[following] != doc_ref[block])
        return jnp.where(closing, jnp.minimum(tail_ref[block], rows), rows)

    ones = jnp.ones((rows, HEAD_DIM), jnp.bfloat16)

    def scores_of(q, k):
        return lax.dot_general(q, k, (((1,), (1,)), ((), ())), preferred_element_type=jnp.float32)

    def self_keys(j, i):
        return kv.at[j, i, 0], kv.at[j, i, 1]

    def cross_keys(j, i):
        return kvc.at[j, :, pl.ds(0, kvw)], kvc.at[j, :, pl.ds(kvw, kvw)]

    def diag(queries, keys_of, items):
        for r in range(0, rows, TILE):
            for b, i in items:
                live = live_of(2 * z + b)
                k_ref, v_ref = keys_of(b, i)
                here, keys = pl.ds(r, TILE), r + TILE
                s = scores_of(queries[b, i, here, :], k_ref[pl.ds(0, keys), :])
                q_at = r + lax.broadcasted_iota(jnp.int32, s.shape, 0)
                k_at = lax.broadcasted_iota(jnp.int32, s.shape, 1)
                s = jnp.where((k_at <= q_at) & (k_at < live), s, NEG)
                peak_row = jnp.max(s, axis=1, keepdims=True)
                w = jnp.exp2((s - peak_row) * SCALE).astype(jnp.bfloat16)
                va = jnp.concatenate([v_ref[pl.ds(0, keys), :], ones[:keys]], axis=1)
                acc[b, i, here, :] = jnp.dot(w, va, preferred_element_type=jnp.float32)
                peak[b, i, here, :] = jnp.broadcast_to(peak_row, (TILE, HEAD_DIM))

    def off(queries, keys_of, items, j, size=TILE):
        def tile(t, carry):
            here = part(t * size, size)
            for b, i in items:
                same = doc_of(2 * z + b) == doc_of(block_of(j))
                on = jnp.where(same, 1.0, 0.0)
                gone = jnp.where(same, 0.0, 1e30)
                gain = jnp.where(same, SCALE, 0.0)
                k_ref, v_ref = keys_of(j, i)
                s = scores_of(queries[b, i, here, :], k_ref[...])
                peak_row = jnp.max(s, axis=1, keepdims=True) * on - gone
                old = peak[b, i, here, :]
                new = jnp.maximum(old, peak_row)
                fade = jnp.exp2((old - new) * SCALE)
                w = jnp.exp2(s * gain - (new[:, :1] * gain + gone)).astype(jnp.bfloat16)
                va = jnp.concatenate([v_ref[...], ones], axis=1)
                more = jnp.dot(w, va, preferred_element_type=jnp.float32)
                fades = jnp.concatenate([fade, fade], axis=1)
                acc[b, i, here, :] = acc[b, i, here, :] * fades + more
                peak[b, i, here, :] = new
            return carry

        lax.fori_loop(0, rows // size, tile, 0)

    def all_heads(b):
        return [(b, i) for i in range(heads)]

    def finish(b, i):
        whole = acc[b, i]
        return (whole[:, :HEAD_DIM] / whole[:, HEAD_DIM:]).astype(jnp.bfloat16)

    ahead, ahead2 = jnp.minimum(z + 1, last), jnp.minimum(z + 2, last)
    behind, behind2 = jnp.maximum(z - 1, 0), jnp.maximum(z - 2, 0)
    has_far = z + 2 <= last

    def wpart(plane, side):
        return wfull.at[part((plane * 2 + side) * wrows, wrows), :]

    def pass_on(name, onward, piece, cond, to, to_cond):
        arrived(name, piece, cond)
        send(onward, piece, piece, to, jnp.logical_and(cond, to_cond))

    def qzy_copy(i):
        return remote("qzy", qx.at[yo, i], qu.at[yo, i], down, i)

    def ob_copy(name, i):
        here = pl.ds(0 if name == "ob" else rows // 2, rows // 2)
        return remote(name, osend.at[i, :, here, :], orecv.at[i, :, here, :], up, i)

    def lb_copy(i):
        return remote("lb", lsend.at[i], lrecv.at[i, pl.ds(0, 8), :], up, i)

    def above(i):
        def tile(t, carry):
            here = part(t * TILE, TILE)
            lane = lax.broadcasted_iota(jnp.int32, (TILE, HEAD_DIM), 1)
            logs = jnp.zeros((TILE, HEAD_DIM), jnp.float32)
            for b in range(2):
                query = qu[b, i, here, :]
                scores, tops, marks = [], [], []
                for k in range(2):
                    ahead_doc = doc_of(jnp.minimum(2 * z + 2 + b, seq_size - 1))
                    same = ahead_doc == doc_of(2 * z + k)
                    marks.append((jnp.where(same, SCALE, 0.0), jnp.where(same, 0.0, 1e30)))
                    s = scores_of(query, kv[k, i, 0])
                    scores.append(s)
                    tops.append(jnp.max(s, axis=1, keepdims=True) * jnp.where(same, 1.0, 0.0) - marks[k][1])
                top_row = jnp.maximum(tops[0], tops[1])
                total = None
                for k in range(2):
                    gain, gone = marks[k]
                    w = jnp.exp2(scores[k] * gain - (top_row * gain + gone)).astype(jnp.bfloat16)
                    va = jnp.concatenate([kv[k, i, 1], ones], axis=1)
                    more = jnp.dot(w, va, preferred_element_type=jnp.float32)
                    total = more if total is None else total + more
                weight = total[:, HEAD_DIM:]
                weight = jnp.where(weight > 0.0, weight, 1.0)
                osend[i, b, here, :] = (total[:, :HEAD_DIM] / weight).astype(jnp.bfloat16)
                logs = jnp.where(lane == b, top_row * SCALE + jnp.log2(weight), logs)
            lbuf[here, :] = logs
            when(t == rows // TILE // 2 - 1, ob_copy("ob", i).start)
            return carry

        lax.fori_loop(0, rows // TILE, tile, 0)
        lsend[i] = jnp.transpose(lbuf[...])[:8, :]

    def quu_copy(i):
        return remote("quu", qu.at[0, i], quu.at[i], down, i)

    def o2_copies(i):
        return [
            remote("o2", osend2.at[i], orecv2.at[i], up, i),
            remote("l2", lsend2(i), lrecv2.at[i, pl.ds(0, 8), :], up, i),
        ]

    def o3_copies(i):
        return [
            remote("o3", orecv2.at[i], orecv3.at[i], up, i),
            remote("l3", lrecv2.at[i, pl.ds(0, 8), :], lrecv3.at[i, pl.ds(0, 8), :], up, i),
        ]

    def lsend2(i):
        return lsend.at[heads + i]

    def above2(i):
        def tile(t, carry):
            here = part(t * TILE, TILE)
            lane = lax.broadcasted_iota(jnp.int32, (TILE, HEAD_DIM), 1)
            same = doc_of(jnp.minimum(2 * z + 4, seq_size - 1)) == doc_of(2 * z + 1)
            gain, gone = jnp.where(same, SCALE, 0.0), jnp.where(same, 0.0, 1e30)
            s = scores_of(quu[i, here, :], kv[1, i, 0])
            top_row = jnp.max(s, axis=1, keepdims=True) * jnp.where(same, 1.0, 0.0) - gone
            w = jnp.exp2(s * gain - (top_row * gain + gone)).astype(jnp.bfloat16)
            va = jnp.concatenate([kv[1, i, 1], ones], axis=1)
            total = jnp.dot(w, va, preferred_element_type=jnp.float32)
            weight = total[:, HEAD_DIM:]
            weight = jnp.where(weight > 0.0, weight, 1.0)
            osend2[i, here, :] = (total[:, :HEAD_DIM] / weight).astype(jnp.bfloat16)
            lbuf[here, :] = jnp.where(lane == 0, top_row * SCALE + jnp.log2(weight), 0.0)
            return carry

        lax.fori_loop(0, rows // TILE, tile, 0)
        lsend[heads + i] = jnp.transpose(lbuf[...])[:8, :]

    def merged(b, i, logs, logs3):
        def one(log_column, values, cond):
            log_row = jnp.where(cond, log_column, NEG)
            return log_row, jnp.where(cond, values.astype(jnp.float32), 0.0)

        pieces = [one(logs[:, b:b + 1], orecv[i, b], has_down)]
        if far and b == 0:
            pieces.append(one(logs3[:, :1], orecv3[i], far_down))
        whole, own_log = acc[b, i], peak[b, i] * SCALE
        most = own_log
        for log_row, _ in pieces:
            most = jnp.maximum(most, log_row)
        fade = jnp.exp2(own_log - most)
        value, weight = whole[:, :HEAD_DIM] * fade, whole[:, HEAD_DIM:] * fade
        for log_row, values in pieces:
            share = jnp.exp2(log_row - most)
            value, weight = value + values * share, weight + share
        return (value / weight).astype(jnp.bfloat16)

    def stage2(i):
        arrived("qy", qx.at[yo, i], None, i)
        when(has_down, qzy_copy(i).start)
        if not far:
            when(has_down, wb1_copy(i).start)
        arrived("ky", kv.at[yo, i, 0], None, i)
        arrived("vy", kv.at[yo, i, 1], None, i)

        @pl.when(has_up)
        def _():
            arrived("qz", qu.at[y, i], None, i)
            arrived("qzy", qu.at[yo, i], None, i)
            if far:
                when(has_down, quu_copy(i).start)
            above(i)
            ob_copy("obb", i).start()
            lb_copy(i).start()

        when(jnp.logical_and(i == 0, has_down), lambda: arrived("wf1", wpart(behind, y)))
        when(jnp.logical_and(mid, i == 0), wf2_copy(0).start)
        diag(qx, self_keys, [(yo, i)])
        off(qx, self_keys, [(1, i)], 0)

    def stage2_far(i):
        @pl.when(has_far)
        def _():
            arrived("quu", quu.at[i], None, i)
            above2(i)
            for copy in o2_copies(i):
                copy.start()

    def stage2_on(i):
        @pl.when(mid)
        def _():
            arrived("o2", orecv2.at[i], None, i)
            arrived("l2", lrecv2.at[i, pl.ds(0, 8), :], None, i)
            for copy in o3_copies(i):
                copy.start()

    def stage3(i):
        arrived("ob", orecv.at[i, :, pl.ds(0, rows // 2), :], has_down, i)
        arrived("obb", orecv.at[i, :, pl.ds(rows // 2, rows // 2), :], has_down, i)
        arrived("lb", lrecv.at[i, pl.ds(0, 8), :], has_down, i)
        logs, logs3 = jnp.transpose(lrecv[i]), None
        if far:
            arrived("o3", orecv3.at[i], far_down, i)
            arrived("l3", lrecv3.at[i, pl.ds(0, 8), :], far_down, i)
            logs3 = jnp.transpose(lrecv3[i])
        done = [merged(b, i, logs, logs3) for b in range(2)]
        ctxo[:, head_cols(i)] = jnp.where(y == 0, done[1], done[0])
        cy_copy(i).start()
        ctx[c_at, y, :, head_cols(i)] = jnp.where(y == 0, done[0], done[1])
        cc_copy(i).start()

    def cy_copy(i):
        return remote("cy", ctxo.at[:, head_cols(i)], ctx.at[c_at, y, :, head_cols(i)], to_y, i)

    def cc_copy(i):
        piece = ctx.at[c_at, y, :, head_cols(i)]
        return remote("cc", piece, piece, to_c, i)

    def cyc_copy(i):
        piece = ctx.at[c_at, yo, :, head_cols(i)]
        return remote("cyc", piece, piece, to_c, i)

    for i in range(heads):
        for copy in local_kvq(i):
            copy.wait()
    diag(qx, self_keys, all_heads(y))
    each_head(stage2)
    if far:
        for i in range(heads):
            when(has_down, wb1_copy(i).start)
        each_head(stage2_far)
        each_head(stage2_on)
    for i in range(1, heads):
        when(mid, wf2_copy(i).start)
    each_head(lambda i: arrived("wb1", wthird(jnp.minimum(s_at + 2, seq_size - 1), i), has_up, i))
    send("wb2", wpart(ahead, y), wpart(ahead, y), down, mid)
    each_head(stage3)
    send("wky", wc_hbm.at[:, kother], wfull.at[wrow, wk_c], to_y)
    send("wvy", wc_hbm.at[:, vother], wfull.at[wrow, wv_c], to_y)
    wkv_c = pl.ds(half, 2 * kvw)
    arrived("wqy", wfull.at[wrow_y, wq_c])
    send("wf1y", wfull.at[wrow_y, wq_c], wfull.at[wrow_y, wq_c], up, has_up)
    send("wb1y", wfull.at[wrow_y, wq_c], wfull.at[wrow_y, wq_c], down, has_down)

    for item in locals_[3:]:
        near(*item).wait()
    arrived("woc0", wo.at[co, 0])
    arrived("woc1", wo.at[co, 1])

    def project(here, side, column):
        total = None
        for core in range(2):
            more = jnp.dot(
                ctx[core, side, here, :], wo[core, column, part(side * half, half), :],
                preferred_element_type=jnp.float32,
            )
            total = more if total is None else total + more
        return total

    each_head(lambda i: arrived("cc", ctx.at[co, y, :, head_cols(i)], None, i))

    def near_side(t, carry):
        here = part(t * TILE, TILE)
        px[here, :] = project(here, y, 1)
        po[here, :] = project(here, y, 0)
        return carry

    lax.fori_loop(0, rows // TILE, near_side, 0)

    def relay_context(i):
        arrived("cy", ctx.at[c_at, yo, :, head_cols(i)], None, i)
        cyc_copy(i).start()

    each_head(relay_context)
    each_head(lambda i: arrived("cyc", ctx.at[co, yo, :, head_cols(i)], None, i))
    for p in range(4):
        here = pl.ds(p * quarter, quarter)
        pxb[here, :] = (px[here, :] + project(here, yo, 1)).astype(jnp.bfloat16)
        send(f"px{p}", pxb.at[here, :], pxr.at[here, :], to_x)

    arrived("wky", wfull.at[wrow_y, wk_c])
    arrived("wvy", wfull.at[wrow_y, wv_c])
    send("wf1k", wfull.at[wrow_y, wkv_c], wfull.at[wrow_y, wkv_c], up, has_up)
    send("wb1k", wfull.at[wrow_y, wkv_c], wfull.at[wrow_y, wkv_c], down, has_down)
    pass_on("wb2", "wb3", wpart(ahead2, y), has_far, down, has_down)
    each_head(lambda i: arrived("wf2", wthird(jnp.maximum(s_at - 4, 0), i), far_down, i))
    send("wf3", wpart(behind2, y), wpart(behind2, y), up, jnp.logical_and(far_down, has_up))

    def far_side(t, carry):
        here = part(t * TILE, TILE)
        po[here, :] = po[here, :] + project(here, yo, 0)
        return carry

    lax.fori_loop(0, rows // TILE, far_side, 0)

    def hpart(b, h, p):
        return hall.at[b, h, pl.ds(p * quarter, quarter), :]

    for p in range(4):
        here = pl.ds(p * quarter, quarter)
        arrived(f"px{p}", pxr.at[here, :])
        total = resv[here, :].astype(jnp.float32) + (po[here, :] + pxr[here, :].astype(jnp.float32))
        hall[y, h_at, here, :] = total.astype(jnp.bfloat16)
        piece = hpart(y, h_at, p)
        send(f"dx{p}", piece, piece, to_x)
        send(f"dy{p}", piece, piece, to_y)
        send(f"dc{p}", piece, piece, to_c)
        near(f"hid{p}", piece, hid_hbm.at[here, :]).start()
        if p == 1:
            arrived("wb1y", wfull.at[part((ahead * 2 + yo) * wrows, wrows), wq_c], has_up)
            arrived("wb1k", wfull.at[part((ahead * 2 + yo) * wrows, wrows), wkv_c], has_up)
            send("wb2y", wpart(ahead, yo), wpart(ahead, yo), down, mid)
        if p == 2:
            arrived("wf1y", wfull.at[part((behind * 2 + yo) * wrows, wrows), wq_c], has_down)
            arrived("wf1k", wfull.at[part((behind * 2 + yo) * wrows, wrows), wkv_c], has_down)
            send("wf2y", wpart(behind, yo), wpart(behind, yo), up, mid)

    def from_x(p):
        piece = hpart(y, hx, p)
        arrived(f"dx{p}", piece)
        send(f"dxc{p}", piece, piece, to_c)
        if p < 3:
            send(f"far{p}", piece, piece, to_y)

    def from_y(p):
        piece = hpart(yo, h_at, p)
        arrived(f"dy{p}", piece)
        send(f"dyc{p}", piece, piece, to_c)
        if p == 3:
            send("far3", piece, piece, to_x)

    def from_far(p):
        piece = hpart(yo, hx, p)
        arrived(f"far{p}", piece)
        send(f"farc{p}", piece, piece, to_c)

    def own_rows(p):
        arrived(f"dc{p}", hpart(y, hc, p))
        arrived(f"dxc{p}", hpart(y, hxc, p))

    def other_rows(p):
        arrived(f"dyc{p}", hpart(yo, hc, p))
        arrived(f"farc{p}", hpart(yo, hxc, p))

    for p in range(3):
        from_y(p)
    from_x(0)
    from_y(3)
    pass_on("wb2y", "wb3y", wpart(ahead2, yo), has_far, down, has_down)
    from_x(1)
    pass_on("wf2y", "wf3y", wpart(behind2, yo), far_down, up, has_up)

    def norm(b, at):
        square = jnp.zeros((quarter, 1), jnp.float32)
        here = part(at * quarter, quarter)
        for h in range(hall.shape[1]):
            wide = hall[b, h, here, :].astype(jnp.float32)
            square += jnp.sum(wide * wide, axis=1, keepdims=True)
        scale = lax.rsqrt(square / D + EPSILON)
        for h in range(hall.shape[1]):
            wide = hall[b, h, here, :].astype(jnp.float32)
            gains = gainv[:, pl.ds(h * width, width)]
            nrm[b, h, here, :] = (wide * scale * gains).astype(jnp.bfloat16)

    def norm_half(b, p):
        def step(n, carry):
            norm(b, 2 * p + n)
            return carry

        lax.fori_loop(0, 2, step, 0)

    def cross_tile(k, b, t, where, first):
        here = part(t * TILE, TILE)
        more = jnp.dot(
            nrm[b, k, here, :], wfull[part(k * 2 * wrows, 2 * wrows), where],
            preferred_element_type=jnp.float32,
        )
        proj[b, here, where] = more if first else proj[b, here, where] + more

    def cross_part(k, b, where, first):
        def tile(t, carry):
            cross_tile(k, b, t, where, first)
            return carry

        lax.fori_loop(0, rows // TILE, tile, 0)

    low = z < planes // 2
    order = [z, jnp.where(low, 1 - z, 5 - z), jnp.where(low, 2, 1), jnp.where(low, 3, 0)]
    every = pl.ds(0, cols)

    def chunks(b, t):
        def step(n, carry):
            cross_tile(jnp.where(n == 0, order[1], order[2]), b, t, every, False)
            return carry

        cross_tile(order[0], b, t, every, True)
        lax.fori_loop(0, 2, step, 0)

    own_rows(0)
    own_rows(1)
    norm_half(y, 0)
    chunks(y, 0)
    from_x(2)
    from_far(0)
    from_far(1)
    from_x(3)
    other_rows(0)
    other_rows(1)
    norm_half(yo, 0)
    chunks(yo, 0)
    from_far(2)
    own_rows(2)
    own_rows(3)
    norm_half(y, 1)
    from_far(3)
    chunks(y, 1)
    other_rows(2)
    other_rows(3)
    norm_half(yo, 1)
    chunks(yo, 1)
    for name, plane, cond in (("wf3", 0, z == last), ("wb3", last, z == 0)):
        arrived(name, wpart(plane, y), cond)
        arrived(name + "y", wpart(plane, yo), cond)

    cache_c, query_c = pl.ds(half, 2 * kvw), pl.ds(0, half)

    def cache_out(b):
        cross_part(order[3], b, cache_c, False)
        kvc[b] = proj[b, :, cache_c].astype(jnp.bfloat16)

    cache_out(1)
    send("e1", kvc.at[1], kvc.at[3], up, has_up)
    cache_out(0)
    send("e0", kvc.at[0], kvc.at[2], up, has_up)

    def query_out(b, carry):
        cross_part(order[3], b, query_c, False)
        for i in range(heads):
            cq[b, i] = proj[b, :, pl.ds(i * HEAD_DIM, HEAD_DIM)].astype(jnp.bfloat16)
        return carry

    lax.fori_loop(0, 2, query_out, 0)

    def own_diag(b, carry):
        diag(cq, cross_keys, all_heads(b))
        return carry

    lax.fori_loop(0, 2, own_diag, 0)

    def home_copy(i):
        return near("o", outs.at[y, i], out_hbm.at[:, own_head(i)], i)

    def away_copy(i):
        return remote("o", outs.at[yo, i], out_hbm.at[:, own_head(i)], to_y, i)

    plan = [(1, 0), (yo, 3), (y, 3)] + ([(0, 4)] if far else []) + [(yo, 2), (y, 2)]

    def look_up(n, which):
        value = plan[0][which]
        for at in range(1, len(plan)):
            value = jnp.where(n == at, plan[at][which], value)
        return value

    def step(n, carry):
        if far:
            @pl.when(jnp.logical_and(n == 0, has_down))
            def _():
                arrived("e1", kvc.at[3])
                when(has_up, remote("er", kvc.at[3], kvc.at[4], up).start)

            when(jnp.logical_and(n == 3, far_down), lambda: arrived("er", kvc.at[4]))
            runs = jnp.where(n == 3, far_down, jnp.logical_or(n == 0, has_down))
        else:
            when(jnp.logical_and(n == 1, has_down), lambda: arrived("e1", kvc.at[3]))
            runs = jnp.logical_or(n == 0, has_down)
        if far:
            when(jnp.logical_and(n == len(plan) - 2, has_down), lambda: arrived("e0", kvc.at[2]))
        b, j = look_up(n, 0), look_up(n, 1)
        when(runs, lambda: off(cq, cross_keys, all_heads(b), j, rows))

        if not far:
            return carry

        @pl.when(n >= len(plan) - 2)
        def _():
            for i in range(heads):
                outs[b, i] = finish(b, i)
                when(n == len(plan) - 2, away_copy(i).start)
                when(n == len(plan) - 1, home_copy(i).start)

        return carry

    if far:
        lax.fori_loop(0, len(plan), step, 0)
    else:
        lax.fori_loop(0, len(plan) - 2, step, 0)
        arrived("e0", kvc.at[2], has_down)

        def away(i):
            when(has_down, lambda: off(cq, cross_keys, [(yo, i)], 2, rows))
            outs[yo, i] = finish(yo, i)
            away_copy(i).start()

        each_head(away)
        when(has_down, lambda: off(cq, cross_keys, all_heads(y), 2, rows))
        for i in range(heads):
            outs[y, i] = finish(y, i)
            home_copy(i).start()
    if far:
        sends.append(("er", kvc.at[3], kvc.at[4], up, mid))

    for p in range(4):
        near(f"hid{p}", hpart(y, h_at, p), hid_hbm.at[pl.ds(p * quarter, quarter), :]).wait()
    for name, src, dst, device, cond in sends:
        when(cond, remote(name, src, dst, device).wait_send)

    def ended(i):
        for copy, cond in first_sends(i):
            when(cond, copy.wait_send)
        when(has_down, wb1_copy(i).wait_send)
        when(mid, wf2_copy(i).wait_send)
        when(has_down, qzy_copy(i).wait_send)
        when(has_up, ob_copy("ob", i).wait_send)
        when(has_up, ob_copy("obb", i).wait_send)
        when(has_up, lb_copy(i).wait_send)
        if far:
            when(mid, quu_copy(i).wait_send)
            for copy in o2_copies(i):
                when(has_far, copy.wait_send)
            for copy in o3_copies(i):
                when(mid, copy.wait_send)
        cy_copy(i).wait_send()
        cc_copy(i).wait_send()
        cyc_copy(i).wait_send()
        home_copy(i).wait()
        away_copy(i).wait_send()
        arrived("o", out_hbm.at[:, other_head(i)], None, i)

    each_head(ended)


def settle_kernel(hid_ref, out_ref, hid_to, out_to):
    hid_to[...] = hid_ref[...]
    out_to[...] = out_ref[...]


def settled(hid, out):
    rows, width = hid.shape
    spec = pl.BlockSpec((rows // 2, width), lambda i: (i, 0))
    return pl.pallas_call(
        settle_kernel,
        out_shape=(jax.ShapeDtypeStruct(hid.shape, hid.dtype),) * 2,
        grid=(2,),
        in_specs=[spec, spec],
        out_specs=(spec, spec),
        compiler_params=pltpu.CompilerParams(vmem_limit_bytes=60 * 1024 * 1024),
    )(hid, out)


def fused(far, residual, q_self, k_self, v_self, w_out, norm_gain, w_query, w_cache, block_doc, tail_len):
    rows, width = q_self.shape
    seq_size, head_size = lax.axis_size("seq"), lax.axis_size("head")
    half = width // 2
    heads = half // HEAD_DIM
    kvw = w_cache.shape[1] // 4
    cols = half + 2 * kvw
    bf, f32 = jnp.bfloat16, jnp.float32
    hbm = pl.BlockSpec(memory_space=pl.ANY)
    smem = pl.BlockSpec(memory_space=pltpu.SMEM)
    by_head = BY_HEAD + (FAR_BY_HEAD if far else ())
    copies = len(by_head) * heads + len(COPIES)
    scratch = [
        pltpu.VMEM((2, heads, rows, HEAD_DIM), bf),
        pltpu.VMEM((2, heads, 2, rows, HEAD_DIM), bf),
        pltpu.VMEM((2, heads, rows, HEAD_DIM), bf),
        pltpu.VMEM((heads, 2, rows, HEAD_DIM), bf),
        pltpu.VMEM((heads, 2, rows, HEAD_DIM), bf),
        pltpu.VMEM((rows, HEAD_DIM), f32),
        pltpu.VMEM((2 * heads, 8, rows), f32),
        pltpu.VMEM((heads, HEAD_DIM, rows), f32),
        pltpu.VMEM((heads, rows, HEAD_DIM), bf),
        pltpu.VMEM((heads, rows, HEAD_DIM), bf),
        pltpu.VMEM((heads, rows, HEAD_DIM), bf),
        pltpu.VMEM((heads, rows, HEAD_DIM), bf),
        pltpu.VMEM((heads, 8, rows), f32),
        pltpu.VMEM((heads, HEAD_DIM, rows), f32),
        pltpu.VMEM((2, heads, rows, 2 * HEAD_DIM), f32),
        pltpu.VMEM((2, heads, rows, HEAD_DIM), f32),
        pltpu.VMEM((2, 2, width, width), bf),
        pltpu.VMEM((w_query.shape[0] * seq_size, cols), bf),
        pltpu.VMEM((2, 2, rows, half), bf),
        pltpu.VMEM((rows, half), bf),
        pltpu.VMEM((rows, width), f32),
        pltpu.VMEM((rows, width), f32),
        pltpu.VMEM((rows, width), bf),
        pltpu.VMEM((rows, width), bf),
        pltpu.VMEM((2, head_size, rows, width), bf),
        pltpu.VMEM((2, head_size, rows, width), bf),
        pltpu.VMEM((rows, width), bf),
        pltpu.VMEM((1, head_size * width), f32),
        pltpu.VMEM((2, rows, cols), f32),
        pltpu.VMEM((2, heads, rows, HEAD_DIM), bf),
        pltpu.VMEM((5 if far else 4, rows, 2 * kvw), bf),
        pltpu.VMEM((2, heads, rows, HEAD_DIM), bf),
        pltpu.SemaphoreType.DMA((copies,)),
        pltpu.SemaphoreType.DMA((copies,)),
        pltpu.SemaphoreType.DMA((len(LOCALS) + len(LOCALS_BY_HEAD) * heads,)),
    ]
    wide = jax.ShapeDtypeStruct((rows, width), bf)
    return pl.pallas_call(
        functools.partial(fused_kernel, far),
        out_shape=(wide, wide),
        in_specs=[hbm] * 8 + [smem] * 2,
        out_specs=(hbm, hbm),
        scratch_shapes=scratch,
        compiler_params=pltpu.CompilerParams(
            collective_id=1 if far else 0, has_side_effects=True, vmem_limit_bytes=60 * 1024 * 1024
        ),
    )(
        residual, q_self, k_self, v_self, w_out, norm_gain.reshape(1, head_size * width),
        w_query, w_cache, block_doc, tail_len,
    )


def chosen(*args):
    block_doc = args[8]
    at = np.arange(block_doc.shape[0])
    apart = (at[None, :] - at[:, None] == 3) & (at[None, :] % 2 == 0)
    far = jnp.any((block_doc[:, None] == block_doc[None, :]) & apart)
    hid, out = lax.cond(far, functools.partial(fused, True), functools.partial(fused, False), *args)
    return settled(hid, out)


def stage_kernel(offsets, window, first, last, facts, q_ref, *refs):
    pairs = [(refs[2 * i], refs[2 * i + 1]) for i in range(len(offsets))]
    rest = refs[2 * len(offsets):]
    if not first:
        acc_in, peak_in, total_in = rest[:3]
        rest = rest[3:]
    if last:
        out_ref = rest[0]
        acc, peak, total = rest[1:]
    else:
        acc, peak, total = rest
    rows = q_ref.shape[0]
    tile = min(ROW_TILE, rows)
    scaling = math.log2(math.e) / math.sqrt(HEAD_DIM)

    def scores_of(r, k):
        return lax.dot_general(
            q_ref[pl.ds(r, tile), :], k, (((1,), (1,)), ((), ())),
            preferred_element_type=jnp.float32,
        )

    if not first:
        acc[...] = acc_in[...]
        peak[...] = peak_in[...]
        total[...] = total_in[...]

    for (k_ref, v_ref), (flag, offset) in zip(pairs, offsets):

        def one(offset=offset, k_ref=k_ref, v_ref=v_ref):
            for r in range(0, rows, tile):
                here = pl.ds(r, tile)
                keys = r + tile if offset == 0 else rows
                s = scores_of(r, k_ref[pl.ds(0, keys), :])
                if offset == 0:
                    q_at = r + lax.broadcasted_iota(jnp.int32, s.shape, 0)
                    k_at = lax.broadcasted_iota(jnp.int32, s.shape, 1)
                    s = jnp.where((k_at <= q_at) & (k_at < facts[0]), s, -1e30)
                elif offset * rows + rows - 1 >= window:
                    q_at = r + lax.broadcasted_iota(jnp.int32, s.shape, 0)
                    k_at = lax.broadcasted_iota(jnp.int32, s.shape, 1)
                    s = jnp.where(offset * rows + q_at - k_at < window, s, -1e30)
                top = jnp.max(s, axis=1, keepdims=True)
                if offset == 0:
                    w = jnp.exp2((s - top) * scaling)
                    part = jnp.dot(
                        w.astype(jnp.bfloat16), v_ref[pl.ds(0, keys), :],
                        preferred_element_type=jnp.float32,
                    )
                    acc[here, :] = part
                    total[here, :] = jnp.broadcast_to(
                        jnp.sum(w, axis=1, keepdims=True), (tile, HEAD_DIM)
                    )
                    peak[here, :] = jnp.broadcast_to(top, (tile, HEAD_DIM))
                else:
                    old = peak[here, :]
                    new = jnp.maximum(old, top)
                    w = jnp.exp2((s - new[:, :1]) * scaling)
                    fade = jnp.exp2((old - new) * scaling)
                    part = jnp.dot(
                        w.astype(jnp.bfloat16), v_ref[...], preferred_element_type=jnp.float32
                    )
                    acc[here, :] = acc[here, :] * fade + part
                    total[here, :] = total[here, :] * fade + jnp.sum(w, axis=1, keepdims=True)
                    peak[here, :] = new

        if offset == 0:
            one()
        else:
            pl.when(facts[flag] > 0)(one)

    if last:
        out_ref[...] = (acc[...] / total[...]).astype(jnp.bfloat16)


def attend_stage(facts, queries, blocks, offsets, kv_heads, state, window, last):
    rows, width = queries.shape
    heads = width // HEAD_DIM
    group = heads // kv_heads
    tall = pl.BlockSpec((rows, HEAD_DIM), lambda h, f: (0, h))
    key_spec = pl.BlockSpec((rows, HEAD_DIM), lambda h, f: (0, h // group))
    value_spec = pl.BlockSpec((rows, HEAD_DIM), lambda h, f: (0, kv_heads + h // group))
    operands, specs = [queries], [tall]
    for block in blocks:
        operands += [block, block]
        specs += [key_spec, value_spec]
    if state is not None:
        operands += list(state)
        specs += [tall] * 3
    wide = jax.ShapeDtypeStruct((rows, width), jnp.float32)
    if last:
        out_shape = jax.ShapeDtypeStruct((rows, width), jnp.bfloat16)
        out_specs = tall
        scratch = [pltpu.VMEM((rows, HEAD_DIM), jnp.float32)] * 3
    else:
        out_shape, out_specs, scratch = (wide,) * 3, (tall,) * 3, []
    flops = 4 * rows * rows * width * len(offsets) * 3
    return pl.pallas_call(
        functools.partial(stage_kernel, offsets, window, state is None, last),
        out_shape=out_shape,
        grid_spec=pltpu.PrefetchScalarGridSpec(
            num_scalar_prefetch=1, grid=(heads,), in_specs=specs, out_specs=out_specs,
            scratch_shapes=scratch,
        ),
        compiler_params=pltpu.CompilerParams(
            dimension_semantics=("arbitrary",), vmem_limit_bytes=32 * 1024 * 1024
        ),
        cost_estimate=pl.CostEstimate(
            flops=flops, bytes_accessed=rows * width * 2 * (2 + 2 * len(offsets)),
            transcendentals=0,
        ),
    )(facts, *operands)


def shared_over_head(block):
    size = lax.axis_size("head")
    held = [block]
    step = size // 2
    got = {0: block}
    while step >= 1:
        for flip in sorted(got):
            got[flip ^ step] = None if got[flip] is None else swapped(got[flip], "head", step)
        step //= 2
    held = [got[flip] for flip in range(size)]
    return held


def sent(block, routes):
    return lax.ppermute(block, "seq", routes)


def row_gather(block):
    size = lax.axis_size("seq")
    me = lax.axis_index("seq")
    ring = [(i, (i + 2) % size) for i in range(size)]
    steps = []
    moving = block
    for step in range(size // 2):
        owner = lax.rem(me - 2 * step + size, size)
        across = swapped(moving, "seq", 1)
        onward = sent(moving, ring) if step + 1 < size // 2 else None
        moving, across, onward = yield moving, across, onward, owner
        moving = onward


def placed(whole, piece, owner):
    return lax.dynamic_update_slice_in_dim(whole, piece, owner * piece.shape[0], 0)


def waves(block, odd, beside):
    size = lax.axis_size("seq")
    first = sent(block, [(i, i + 1) for i in range(size - 1)])
    second_even = sent(block, [(i, i + 2) for i in range(0, size - 2, 2)])
    if beside is not None:
        first, beside = lax.optimization_barrier((first, beside))
    mixed = jnp.where(odd, block, first)
    second = sent(mixed, [(i, i + 2) for i in range(size - 2)])
    third_odd = sent(second_even, [(i, i + 1) for i in range(2, size, 2)])
    return first, [second_even, second, third_odd], beside


def fits(q_self, w_cache):
    seq_size, head_size = lax.axis_size("seq"), lax.axis_size("head")
    return (
        seq_size == 8 and head_size == 4 and q_self.shape[1] == 6 * HEAD_DIM
        and w_cache.shape[1] == 4 * HEAD_DIM and q_self.shape[0] % TILE == 0
    )


def local(
    residual, q_self, k_self, v_self, w_out, norm_gain, w_query, w_cache, block_doc, tail_len
):
    rows, width = q_self.shape
    local_heads = width // HEAD_DIM
    if fits(q_self, w_cache):
        return chosen(
            residual, q_self, k_self, v_self, w_out, norm_gain, w_query, w_cache, block_doc, tail_len
        )
    local_kv = w_cache.shape[1] // (2 * HEAD_DIM)
    seq_size, head_size = lax.axis_size("seq"), lax.axis_size("head")
    span = min(DOC_BLOCKS, seq_size // 2)
    far = list(range(1, span))
    me, my_head = lax.axis_index("seq"), lax.axis_index("head")

    own_doc = block_doc[me]
    following = jnp.where(me == seq_size - 1, -1, block_doc[jnp.minimum(me + 1, seq_size - 1)])
    live = jnp.where(following != own_doc, jnp.minimum(tail_len[me], rows), rows)
    odd = lax.rem(me, 2) == 1
    small = span == 4 and seq_size % 2 == 0

    def together(distance):
        other = me - distance
        return jnp.logical_and(other >= 0, block_doc[jnp.maximum(other, 0)] == own_doc)

    if small:
        flags = [
            together(1),
            jnp.logical_and(jnp.logical_not(odd), together(2)),
            jnp.where(odd, together(2), together(3)),
            jnp.logical_and(odd, together(3)),
        ]
        distances = [1, 2, 3, 3]
    else:
        flags = [together(distance) for distance in far]
        distances = far
    facts = jnp.stack([live.astype(jnp.int32)] + [flag.astype(jnp.int32) for flag in flags])
    slots = [(1 + i, distance) for i, distance in enumerate(distances)]

    stacked = jnp.concatenate([k_self, v_self], axis=1)
    weight_rows = jnp.concatenate([w_query, w_cache], axis=1)
    state = attend_stage(facts, q_self, [stacked], [(0, 0)], local_heads, None, WINDOW, False)
    if small:
        near, late, state = waves(stacked, odd, state)
    else:
        near, *late = [passed_along(stacked, "seq", offset) for offset in far]

    own_columns = residual.shape[1]
    out_pieces = []
    for flip in range(head_size):
        piece = lax.dynamic_slice_in_dim(w_out, (my_head ^ flip) * own_columns, own_columns, 1)
        out_pieces.append(piece if flip == 0 else swapped(piece, "head", flip))

    state = attend_stage(facts, q_self, [near], slots[:1], local_heads, state, WINDOW, False)
    if small:
        weight_rows, state = lax.optimization_barrier((weight_rows, state))
        weights = jnp.zeros((weight_rows.shape[0] * seq_size, weight_rows.shape[1]), jnp.bfloat16)
        gather = row_gather(weight_rows)
        moving, across, onward, owner = next(gather)
        late, across, onward, out_pieces = lax.optimization_barrier(
            (late, across, onward, out_pieces)
        )
        weights = placed(placed(weights, moving, owner), across, owner ^ 1)
        moving, across, onward, owner = gather.send((moving, across, onward))
    else:
        weights = lax.all_gather(weight_rows, "seq", axis=0, tiled=True)
    context = attend_stage(facts, q_self, late, slots[1:], local_heads, state, WINDOW, True)
    if small:
        context, across, onward = lax.optimization_barrier((context, across, onward))
        weights = placed(placed(weights, moving, owner), across, owner ^ 1)
        moving, across, onward, owner = gather.send((moving, across, onward))

    contexts = shared_over_head(context)
    projected = jnp.dot(contexts[0], out_pieces[0], preferred_element_type=jnp.float32)
    for flip in range(1, head_size):
        projected += jnp.dot(contexts[flip], out_pieces[flip], preferred_element_type=jnp.float32)
    hidden = (residual.astype(jnp.float32) + projected).astype(jnp.bfloat16)
    if small:
        hidden, across, onward = lax.optimization_barrier((hidden, across, onward))
        weights = placed(placed(weights, moving, owner), across, owner ^ 1)
        while onward is not None:
            moving, across, onward, owner = gather.send((moving, across, onward))
            weights = placed(placed(weights, moving, owner), across, owner ^ 1)

    full = jnp.zeros((rows, own_columns * head_size), jnp.bfloat16)
    for flip, piece in enumerate(shared_over_head(hidden)):
        full = lax.dynamic_update_slice_in_dim(full, piece, (my_head ^ flip) * own_columns, 1)
    wide = full.astype(jnp.float32)
    mean_square = jnp.sum(wide * wide, axis=1, keepdims=True) / D
    normed = (wide * lax.rsqrt(mean_square + EPSILON) * norm_gain).astype(jnp.bfloat16)

    cache_rows = jnp.dot(
        normed, weights[:, width:], preferred_element_type=jnp.float32
    ).astype(jnp.bfloat16)
    if small:
        near, late, _ = waves(cache_rows, odd, None)
    else:
        near, *late = [passed_along(cache_rows, "seq", offset) for offset in far]
    cross_queries = jnp.dot(
        normed, weights[:, :width], preferred_element_type=jnp.float32
    ).astype(jnp.bfloat16)
    reach = DOC_BLOCKS * rows
    state = attend_stage(
        facts, cross_queries, [cache_rows, near], [(0, 0)] + slots[:1], local_kv, None, reach, False
    )
    cross_context = attend_stage(
        facts, cross_queries, late, slots[1:], local_kv, state, reach, True
    )
    return (hidden, cross_context)


def solution(mesh):
    in_specs = (
        P("seq", "head"),
        P("seq", "head"),
        P("seq", "head"),
        P("seq", "head"),
        P("head", None),
        P(),
        P("seq", "head"),
        P("seq", "head"),
        P(),
        P(),
    )
    out_specs = (P("seq", "head"), P("seq", "head"))
    return jax.shard_map(local, mesh=mesh, in_specs=in_specs, out_specs=out_specs, check_vma=False)
```

```python
import functools
import math

import jax
import jax.numpy as jnp
import numpy as np
from jax import lax
from jax.experimental import pallas as pl
from jax.experimental.pallas import tpu as pltpu
from jax.sharding import PartitionSpec as P

D = 3072
HEAD_DIM = 128
WINDOW = 2048
DOC_BLOCKS = 5
EPSILON = 1e-06
ROW_TILE = 256


def passed_along(block, axis, distance):
    devices = range(lax.axis_size(axis))
    route = [(i - distance, i) for i in devices if i - distance in devices]
    return lax.ppermute(block, axis, route)


def swapped(block, axis, flip):
    return lax.ppermute(block, axis, [(i, i ^ flip) for i in range(lax.axis_size(axis))])


MESH = pl.DeviceIdType.MESH
TILE = 256
NEG = -1e30
SCALE = math.log2(math.e) / math.sqrt(HEAD_DIM)

BY_HEAD = (
    "ky", "vy", "qy", "cy", "cc", "cyc", "o", "qz", "qzy", "ob", "obb", "lb", "wb1", "wf2",
)
FAR_BY_HEAD = ("quu", "o2", "l2", "o3", "l3")
COPIES = (
    "wqy", "wky", "wvy", "wf1", "wf1y", "wf1k", "wf2y", "wf3", "wf3y",
    "wb1y", "wb1k", "wb2", "wb2y", "wb3", "wb3y", "woc0", "woc1",
    "px0", "px1", "px2", "px3", "dx0", "dx1", "dx2", "dx3", "dy0", "dy1", "dy2", "dy3",
    "dc0", "dc1", "dc2", "dc3", "dxc0", "dxc1", "dxc2", "dxc3", "dyc0", "dyc1", "dyc2", "dyc3",
    "far0", "far1", "far2", "far3", "farc0", "farc1", "farc2", "farc3", "e1", "e0", "er",
)
LOCALS = ("wq", "wk", "wv", "res", "gain", "wo0", "wo1", "hid0", "hid1", "hid2", "hid3")
LOCALS_BY_HEAD = ("k", "v", "q", "o")


def fused_kernel(
    far, res_hbm, q_hbm, k_hbm, v_hbm, wo_hbm, gain_hbm, wq_hbm, wc_hbm, doc_ref, tail_ref,
    hid_hbm, out_hbm,
    qx, kv, qu, osend, orecv, lbuf, lsend, lrecv, quu, osend2, orecv2, orecv3, lrecv2, lrecv3, acc, peak, wo, wfull, ctx, ctxo, po, px, pxb, pxr, hall, nrm, resv, gainv, proj, cq, kvc, outs,
    ss, rs, ls,
):
    s_at, h_at = lax.axis_index("seq"), lax.axis_index("head")
    seq_size = lax.axis_size("seq")
    planes = seq_size // 2
    last = planes - 1
    z, y = s_at // 2, lax.rem(s_at, 2)
    yo = 1 - y
    c_at = lax.rem(h_at, 2)
    co = 1 - c_at
    hx, hc = lax.rem(h_at + 2, 4), h_at + 1 - 2 * c_at
    hxc = lax.rem(hc + 2, 4)
    rows, width = q_hbm.shape
    half = width // 2
    heads = half // HEAD_DIM
    wrows = wq_hbm.shape[0]
    kvw = wc_hbm.shape[1] // 4
    cols = half + 2 * kvw
    quarter = rows // 4
    to_y, to_x, to_c = (z * 2 + yo, h_at), (s_at, hx), (s_at, hc)
    up, down = (s_at + 2, h_at), (s_at - 2, h_at)
    has_up, has_down = z < last, z > 0
    mid = jnp.logical_and(has_up, has_down)
    far_down = z > 1

    by_head = BY_HEAD + (FAR_BY_HEAD if far else ())

    def part(at, size):
        return pl.ds(pl.multiple_of(at, size), size)

    def index_of(name, i):
        if i is None:
            return len(by_head) * heads + COPIES.index(name)
        return by_head.index(name) * heads + i

    def remote(name, src, dst, device, i=None):
        at = index_of(name, i)
        return pltpu.make_async_remote_copy(
            src_ref=src, dst_ref=dst, send_sem=ss.at[at], recv_sem=rs.at[at],
            device_id=device, device_id_type=MESH,
        )

    def near(name, src, dst, i=None):
        at = LOCALS.index(name) if i is None else len(LOCALS) + LOCALS_BY_HEAD.index(name) * heads + i
        return pltpu.make_async_copy(src, dst, ls.at[at])

    def when(cond, go):
        if cond is None:
            go()
        else:
            pl.when(cond)(go)

    sends = []

    def send(name, src, dst, device, cond=None):
        when(cond, lambda: remote(name, src, dst, device).start())
        sends.append((name, src, dst, device, cond))

    def arrived(name, dst, cond=None, i=None):
        def go():
            remote(name, dst, dst, to_y, i).wait_recv()

        when(cond, go)

    def each_head(body):
        def step(i, carry):
            body(i)
            return carry

        lax.fori_loop(0, heads, step, 0)

    mine, other = part(y * half, half), part(yo * half, half)
    kmine, kother = part(y * kvw, kvw), part(yo * kvw, kvw)
    vmine, vother = part((2 + y) * kvw, kvw), part((2 + yo) * kvw, kvw)
    wrow, wrow_y = part(s_at * wrows, wrows), part((z * 2 + yo) * wrows, wrows)
    wq_c, wk_c, wv_c = pl.ds(0, half), pl.ds(half, kvw), pl.ds(half + kvw, kvw)

    def wchunk(plane):
        return wfull.at[part(plane * 2 * wrows, 2 * wrows), :]

    def own_head(i):
        return part(y * half + i * HEAD_DIM, HEAD_DIM)

    def other_head(i):
        return part(yo * half + i * HEAD_DIM, HEAD_DIM)

    def head_cols(i):
        return part(i * HEAD_DIM, HEAD_DIM)

    barrier = pltpu.get_barrier_semaphore()
    for device in (to_y, to_x, to_c):
        pl.semaphore_signal(barrier, inc=1, device_id=device, device_id_type=MESH)

    @pl.when(has_up)
    def _():
        pl.semaphore_signal(barrier, inc=1, device_id=up, device_id_type=MESH)

    @pl.when(has_down)
    def _():
        pl.semaphore_signal(barrier, inc=1, device_id=down, device_id_type=MESH)

    locals_ = [
        ("wq", wq_hbm.at[:, mine], wfull.at[wrow, wq_c]),
        ("wk", wc_hbm.at[:, kmine], wfull.at[wrow, wk_c]),
        ("wv", wc_hbm.at[:, vmine], wfull.at[wrow, wv_c]),
        ("wo0", wo_hbm.at[:, part(h_at * width, width)], wo.at[c_at, 0]),
        ("wo1", wo_hbm.at[:, part(hx * width, width)], wo.at[c_at, 1]),
        ("res", res_hbm, resv),
        ("gain", gain_hbm, gainv),
    ]

    def local_kvq(i):
        return [
            near("k", k_hbm.at[:, own_head(i)], kv.at[y, i, 0], i),
            near("v", v_hbm.at[:, own_head(i)], kv.at[y, i, 1], i),
            near("q", q_hbm.at[:, own_head(i)], qx.at[y, i], i),
        ]

    for i in range(heads):
        for copy in local_kvq(i):
            copy.start()
    for item in locals_:
        near(*item).start()
    pl.semaphore_wait(barrier, 3 + jnp.where(has_up, 1, 0) + jnp.where(has_down, 1, 0))

    def first_sends(i):
        return [
            (remote("qy", q_hbm.at[:, other_head(i)], qx.at[y, i], to_y, i), None),
            (remote("ky", k_hbm.at[:, other_head(i)], kv.at[y, i, 0], to_y, i), None),
            (remote("vy", v_hbm.at[:, other_head(i)], kv.at[y, i, 1], to_y, i), None),
            (remote("qz", q_hbm.at[:, own_head(i)], qu.at[y, i], down, i), has_down),
        ]

    for i in range(heads):
        for copy, cond in first_sends(i):
            when(cond, copy.start)
    send("wqy", wq_hbm.at[:, other], wfull.at[wrow, wq_c], to_y)
    send("woc0", wo_hbm.at[:, part(hc * width, width)], wo.at[c_at, 0], to_c)
    send("woc1", wo_hbm.at[:, part(hxc * width, width)], wo.at[c_at, 1], to_c)
    for item in locals_[:3]:
        near(*item).wait()
    third = wrows // heads

    def wthird(block, i):
        return wfull.at[part(block * wrows + i * third, third), :]

    def wb1_copy(i):
        return remote("wb1", wthird(s_at, i), wthird(s_at, i), down, i)

    def wf2_copy(i):
        piece = wthird(jnp.maximum(s_at - 2, 0), i)
        return remote("wf2", piece, piece, up, i)

    send("wf1", wfull.at[wrow, :], wfull.at[wrow, :], up, has_up)

    def block_of(j):
        return jnp.where(j < 2, 2 * z + j, jnp.where(j < 4, 2 * z - 4 + j, 2 * z - 3))

    def doc_of(block):
        return doc_ref[jnp.maximum(block, 0)]

    def live_of(block):
        following = jnp.minimum(block + 1, seq_size - 1)
        closing = jnp.logical_or(block == seq_size - 1, doc_ref[following] != doc_ref[block])
        return jnp.where(closing, jnp.minimum(tail_ref[block], rows), rows)

    ones = jnp.ones((rows, HEAD_DIM), jnp.bfloat16)

    def scores_of(q, k):
        return lax.dot_general(q, k, (((1,), (1,)), ((), ())), preferred_element_type=jnp.float32)

    def self_keys(j, i):
        return kv.at[j, i, 0], kv.at[j, i, 1]

    def cross_keys(j, i):
        return kvc.at[j, :, pl.ds(0, kvw)], kvc.at[j, :, pl.ds(kvw, kvw)]

    def diag(queries, keys_of, items):
        for r in range(0, rows, TILE):
            for b, i in items:
                live = live_of(2 * z + b)
                k_ref, v_ref = keys_of(b, i)
                here, keys = pl.ds(r, TILE), r + TILE
                s = scores_of(queries[b, i, here, :], k_ref[pl.ds(0, keys), :])
                q_at = r + lax.broadcasted_iota(jnp.int32, s.shape, 0)
                k_at = lax.broadcasted_iota(jnp.int32, s.shape, 1)
                s = jnp.where((k_at <= q_at) & (k_at < live), s, NEG)
                peak_row = jnp.max(s, axis=1, keepdims=True)
                w = jnp.exp2((s - peak_row) * SCALE).astype(jnp.bfloat16)
                va = jnp.concatenate([v_ref[pl.ds(0, keys), :], ones[:keys]], axis=1)
                acc[b, i, here, :] = jnp.dot(w, va, preferred_element_type=jnp.float32)
                peak[b, i, here, :] = jnp.broadcast_to(peak_row, (TILE, HEAD_DIM))

    def off(queries, keys_of, items, j, size=TILE):
        def tile(t, carry):
            here = part(t * size, size)
            for b, i in items:
                same = doc_of(2 * z + b) == doc_of(block_of(j))
                on = jnp.where(same, 1.0, 0.0)
                gone = jnp.where(same, 0.0, 1e30)
                gain = jnp.where(same, SCALE, 0.0)
                k_ref, v_ref = keys_of(j, i)
                s = scores_of(queries[b, i, here, :], k_ref[...])
                peak_row = jnp.max(s, axis=1, keepdims=True) * on - gone
                old = peak[b, i, here, :]
                new = jnp.maximum(old, peak_row)
                fade = jnp.exp2((old - new) * SCALE)
                w = jnp.exp2(s * gain - (new[:, :1] * gain + gone)).astype(jnp.bfloat16)
                va = jnp.concatenate([v_ref[...], ones], axis=1)
                more = jnp.dot(w, va, preferred_element_type=jnp.float32)
                fades = jnp.concatenate([fade, fade], axis=1)
                acc[b, i, here, :] = acc[b, i, here, :] * fades + more
                peak[b, i, here, :] = new
            return carry

        lax.fori_loop(0, rows // size, tile, 0)

    def all_heads(b):
        return [(b, i) for i in range(heads)]

    def finish(b, i):
        whole = acc[b, i]
        return (whole[:, :HEAD_DIM] / whole[:, HEAD_DIM:]).astype(jnp.bfloat16)

    ahead, ahead2 = jnp.minimum(z + 1, last), jnp.minimum(z + 2, last)
    behind, behind2 = jnp.maximum(z - 1, 0), jnp.maximum(z - 2, 0)
    has_far = z + 2 <= last

    def wpart(plane, side):
        return wfull.at[part((plane * 2 + side) * wrows, wrows), :]

    def pass_on(name, onward, piece, cond, to, to_cond):
        arrived(name, piece, cond)
        send(onward, piece, piece, to, jnp.logical_and(cond, to_cond))

    def qzy_copy(i):
        return remote("qzy", qx.at[yo, i], qu.at[yo, i], down, i)

    def ob_copy(name, i):
        here = pl.ds(0 if name == "ob" else rows // 2, rows // 2)
        return remote(name, osend.at[i, :, here, :], orecv.at[i, :, here, :], up, i)

    def lb_copy(i):
        return remote("lb", lsend.at[i], lrecv.at[i, pl.ds(0, 8), :], up, i)

    def above(i):
        def tile(t, carry):
            here = part(t * TILE, TILE)
            lane = lax.broadcasted_iota(jnp.int32, (TILE, HEAD_DIM), 1)
            logs = jnp.zeros((TILE, HEAD_DIM), jnp.float32)
            for b in range(2):
                query = qu[b, i, here, :]
                scores, tops, marks = [], [], []
                for k in range(2):
                    ahead_doc = doc_of(jnp.minimum(2 * z + 2 + b, seq_size - 1))
                    same = ahead_doc == doc_of(2 * z + k)
                    marks.append((jnp.where(same, SCALE, 0.0), jnp.where(same, 0.0, 1e30)))
                    s = scores_of(query, kv[k, i, 0])
                    scores.append(s)
                    tops.append(jnp.max(s, axis=1, keepdims=True) * jnp.where(same, 1.0, 0.0) - marks[k][1])
                top_row = jnp.maximum(tops[0], tops[1])
                total = None
                for k in range(2):
                    gain, gone = marks[k]
                    w = jnp.exp2(scores[k] * gain - (top_row * gain + gone)).astype(jnp.bfloat16)
                    va = jnp.concatenate([kv[k, i, 1], ones], axis=1)
                    more = jnp.dot(w, va, preferred_element_type=jnp.float32)
                    total = more if total is None else total + more
                weight = total[:, HEAD_DIM:]
                weight = jnp.where(weight > 0.0, weight, 1.0)
                osend[i, b, here, :] = (total[:, :HEAD_DIM] / weight).astype(jnp.bfloat16)
                logs = jnp.where(lane == b, top_row * SCALE + jnp.log2(weight), logs)
            lbuf[here, :] = logs
            when(t == rows // TILE // 2 - 1, ob_copy("ob", i).start)
            return carry

        lax.fori_loop(0, rows // TILE, tile, 0)
        lsend[i] = jnp.transpose(lbuf[...])[:8, :]

    def quu_copy(i):
        return remote("quu", qu.at[0, i], quu.at[i], down, i)

    def o2_copies(i):
        return [
            remote("o2", osend2.at[i], orecv2.at[i], up, i),
            remote("l2", lsend2(i), lrecv2.at[i, pl.ds(0, 8), :], up, i),
        ]

    def o3_copies(i):
        return [
            remote("o3", orecv2.at[i], orecv3.at[i], up, i),
            remote("l3", lrecv2.at[i, pl.ds(0, 8), :], lrecv3.at[i, pl.ds(0, 8), :], up, i),
        ]

    def lsend2(i):
        return lsend.at[heads + i]

    def above2(i):
        def tile(t, carry):
            here = part(t * TILE, TILE)
            lane = lax.broadcasted_iota(jnp.int32, (TILE, HEAD_DIM), 1)
            same = doc_of(jnp.minimum(2 * z + 4, seq_size - 1)) == doc_of(2 * z + 1)
            gain, gone = jnp.where(same, SCALE, 0.0), jnp.where(same, 0.0, 1e30)
            s = scores_of(quu[i, here, :], kv[1, i, 0])
            top_row = jnp.max(s, axis=1, keepdims=True) * jnp.where(same, 1.0, 0.0) - gone
            w = jnp.exp2(s * gain - (top_row * gain + gone)).astype(jnp.bfloat16)
            va = jnp.concatenate([kv[1, i, 1], ones], axis=1)
            total = jnp.dot(w, va, preferred_element_type=jnp.float32)
            weight = total[:, HEAD_DIM:]
            weight = jnp.where(weight > 0.0, weight, 1.0)
            osend2[i, here, :] = (total[:, :HEAD_DIM] / weight).astype(jnp.bfloat16)
            lbuf[here, :] = jnp.where(lane == 0, top_row * SCALE + jnp.log2(weight), 0.0)
            return carry

        lax.fori_loop(0, rows // TILE, tile, 0)
        lsend[heads + i] = jnp.transpose(lbuf[...])[:8, :]

    def merged(b, i, logs, logs3):
        def one(log_column, values, cond):
            log_row = jnp.where(cond, log_column, NEG)
            return log_row, jnp.where(cond, values.astype(jnp.float32), 0.0)

        pieces = [one(logs[:, b:b + 1], orecv[i, b], has_down)]
        if far and b == 0:
            pieces.append(one(logs3[:, :1], orecv3[i], far_down))
        whole, own_log = acc[b, i], peak[b, i] * SCALE
        most = own_log
        for log_row, _ in pieces:
            most = jnp.maximum(most, log_row)
        fade = jnp.exp2(own_log - most)
        value, weight = whole[:, :HEAD_DIM] * fade, whole[:, HEAD_DIM:] * fade
        for log_row, values in pieces:
            share = jnp.exp2(log_row - most)
            value, weight = value + values * share, weight + share
        return (value / weight).astype(jnp.bfloat16)

    def stage2(i):
        arrived("qy", qx.at[yo, i], None, i)
        when(has_down, qzy_copy(i).start)
        if not far:
            when(has_down, wb1_copy(i).start)
        arrived("ky", kv.at[yo, i, 0], None, i)
        arrived("vy", kv.at[yo, i, 1], None, i)

        @pl.when(has_up)
        def _():
            arrived("qz", qu.at[y, i], None, i)
            arrived("qzy", qu.at[yo, i], None, i)
            if far:
                when(has_down, quu_copy(i).start)
            above(i)
            ob_copy("obb", i).start()
            lb_copy(i).start()

        when(jnp.logical_and(i == 0, has_down), lambda: arrived("wf1", wpart(behind, y)))
        when(jnp.logical_and(mid, i == 0), wf2_copy(0).start)
        diag(qx, self_keys, [(yo, i)])
        off(qx, self_keys, [(1, i)], 0)

    def stage2_far(i):
        @pl.when(has_far)
        def _():
            arrived("quu", quu.at[i], None, i)
            above2(i)
            for copy in o2_copies(i):
                copy.start()

    def stage2_on(i):
        @pl.when(mid)
        def _():
            arrived("o2", orecv2.at[i], None, i)
            arrived("l2", lrecv2.at[i, pl.ds(0, 8), :], None, i)
            for copy in o3_copies(i):
                copy.start()

    def stage3(i):
        arrived("ob", orecv.at[i, :, pl.ds(0, rows // 2), :], has_down, i)
        arrived("obb", orecv.at[i, :, pl.ds(rows // 2, rows // 2), :], has_down, i)
        arrived("lb", lrecv.at[i, pl.ds(0, 8), :], has_down, i)
        logs, logs3 = jnp.transpose(lrecv[i]), None
        if far:
            arrived("o3", orecv3.at[i], far_down, i)
            arrived("l3", lrecv3.at[i, pl.ds(0, 8), :], far_down, i)
            logs3 = jnp.transpose(lrecv3[i])
        done = [merged(b, i, logs, logs3) for b in range(2)]
        ctxo[:, head_cols(i)] = jnp.where(y == 0, done[1], done[0])
        cy_copy(i).start()
        ctx[c_at, y, :, head_cols(i)] = jnp.where(y == 0, done[0], done[1])
        cc_copy(i).start()

    def cy_copy(i):
        return remote("cy", ctxo.at[:, head_cols(i)], ctx.at[c_at, y, :, head_cols(i)], to_y, i)

    def cc_copy(i):
        piece = ctx.at[c_at, y, :, head_cols(i)]
        return remote("cc", piece, piece, to_c, i)

    def cyc_copy(i):
        piece = ctx.at[c_at, yo, :, head_cols(i)]
        return remote("cyc", piece, piece, to_c, i)

    for i in range(heads):
        for copy in local_kvq(i):
            copy.wait()
    diag(qx, self_keys, all_heads(y))
    each_head(stage2)
    if far:
        for i in range(heads):
            when(has_down, wb1_copy(i).start)
        each_head(stage2_far)
        each_head(stage2_on)
    for i in range(1, heads):
        when(mid, wf2_copy(i).start)
    each_head(lambda i: arrived("wb1", wthird(jnp.minimum(s_at + 2, seq_size - 1), i), has_up, i))
    send("wb2", wpart(ahead, y), wpart(ahead, y), down, mid)
    each_head(stage3)
    send("wky", wc_hbm.at[:, kother], wfull.at[wrow, wk_c], to_y)
    send("wvy", wc_hbm.at[:, vother], wfull.at[wrow, wv_c], to_y)
    wkv_c = pl.ds(half, 2 * kvw)
    arrived("wqy", wfull.at[wrow_y, wq_c])
    send("wf1y", wfull.at[wrow_y, wq_c], wfull.at[wrow_y, wq_c], up, has_up)
    send("wb1y", wfull.at[wrow_y, wq_c], wfull.at[wrow_y, wq_c], down, has_down)

    for item in locals_[3:]:
        near(*item).wait()
    arrived("woc0", wo.at[co, 0])
    arrived("woc1", wo.at[co, 1])

    def project(here, side, column):
        total = None
        for core in range(2):
            more = jnp.dot(
                ctx[core, side, here, :], wo[core, column, part(side * half, half), :],
                preferred_element_type=jnp.float32,
            )
            total = more if total is None else total + more
        return total

    each_head(lambda i: arrived("cc", ctx.at[co, y, :, head_cols(i)], None, i))

    def near_side(t, carry):
        here = part(t * TILE, TILE)
        px[here, :] = project(here, y, 1)
        po[here, :] = project(here, y, 0)
        return carry

    lax.fori_loop(0, rows // TILE, near_side, 0)

    def relay_context(i):
        arrived("cy", ctx.at[c_at, yo, :, head_cols(i)], None, i)
        cyc_copy(i).start()

    each_head(relay_context)
    each_head(lambda i: arrived("cyc", ctx.at[co, yo, :, head_cols(i)], None, i))
    for p in range(4):
        here = pl.ds(p * quarter, quarter)
        pxb[here, :] = (px[here, :] + project(here, yo, 1)).astype(jnp.bfloat16)
        send(f"px{p}", pxb.at[here, :], pxr.at[here, :], to_x)

    arrived("wky", wfull.at[wrow_y, wk_c])
    arrived("wvy", wfull.at[wrow_y, wv_c])
    send("wf1k", wfull.at[wrow_y, wkv_c], wfull.at[wrow_y, wkv_c], up, has_up)
    send("wb1k", wfull.at[wrow_y, wkv_c], wfull.at[wrow_y, wkv_c], down, has_down)
    pass_on("wb2", "wb3", wpart(ahead2, y), has_far, down, has_down)
    each_head(lambda i: arrived("wf2", wthird(jnp.maximum(s_at - 4, 0), i), far_down, i))
    send("wf3", wpart(behind2, y), wpart(behind2, y), up, jnp.logical_and(far_down, has_up))

    def far_side(t, carry):
        here = part(t * TILE, TILE)
        po[here, :] = po[here, :] + project(here, yo, 0)
        return carry

    lax.fori_loop(0, rows // TILE, far_side, 0)

    def hpart(b, h, p):
        return hall.at[b, h, pl.ds(p * quarter, quarter), :]

    for p in range(4):
        here = pl.ds(p * quarter, quarter)
        arrived(f"px{p}", pxr.at[here, :])
        total = resv[here, :].astype(jnp.float32) + (po[here, :] + pxr[here, :].astype(jnp.float32))
        hall[y, h_at, here, :] = total.astype(jnp.bfloat16)
        piece = hpart(y, h_at, p)
        send(f"dx{p}", piece, piece, to_x)
        send(f"dy{p}", piece, piece, to_y)
        send(f"dc{p}", piece, piece, to_c)
        near(f"hid{p}", piece, hid_hbm.at[here, :]).start()
        if p == 1:
            arrived("wb1y", wfull.at[part((ahead * 2 + yo) * wrows, wrows), wq_c], has_up)
            arrived("wb1k", wfull.at[part((ahead * 2 + yo) * wrows, wrows), wkv_c], has_up)
            send("wb2y", wpart(ahead, yo), wpart(ahead, yo), down, mid)
        if p == 2:
            arrived("wf1y", wfull.at[part((behind * 2 + yo) * wrows, wrows), wq_c], has_down)
            arrived("wf1k", wfull.at[part((behind * 2 + yo) * wrows, wrows), wkv_c], has_down)
            send("wf2y", wpart(behind, yo), wpart(behind, yo), up, mid)

    def from_x(p):
        piece = hpart(y, hx, p)
        arrived(f"dx{p}", piece)
        send(f"dxc{p}", piece, piece, to_c)
        if p < 3:
            send(f"far{p}", piece, piece, to_y)

    def from_y(p):
        piece = hpart(yo, h_at, p)
        arrived(f"dy{p}", piece)
        send(f"dyc{p}", piece, piece, to_c)
        if p == 3:
            send("far3", piece, piece, to_x)

    def from_far(p):
        piece = hpart(yo, hx, p)
        arrived(f"far{p}", piece)
        send(f"farc{p}", piece, piece, to_c)

    def own_rows(p):
        arrived(f"dc{p}", hpart(y, hc, p))
        arrived(f"dxc{p}", hpart(y, hxc, p))

    def other_rows(p):
        arrived(f"dyc{p}", hpart(yo, hc, p))
        arrived(f"farc{p}", hpart(yo, hxc, p))

    for p in range(3):
        from_y(p)
    from_x(0)
    from_y(3)
    pass_on("wb2y", "wb3y", wpart(ahead2, yo), has_far, down, has_down)
    from_x(1)
    pass_on("wf2y", "wf3y", wpart(behind2, yo), far_down, up, has_up)

    def norm(b, at):
        square = jnp.zeros((quarter, 1), jnp.float32)
        here = part(at * quarter, quarter)
        for h in range(hall.shape[1]):
            wide = hall[b, h, here, :].astype(jnp.float32)
            square += jnp.sum(wide * wide, axis=1, keepdims=True)
        scale = lax.rsqrt(square / D + EPSILON)
        for h in range(hall.shape[1]):
            wide = hall[b, h, here, :].astype(jnp.float32)
            gains = gainv[:, pl.ds(h * width, width)]
            nrm[b, h, here, :] = (wide * scale * gains).astype(jnp.bfloat16)

    def norm_half(b, p):
        def step(n, carry):
            norm(b, 2 * p + n)
            return carry

        lax.fori_loop(0, 2, step, 0)

    def cross_tile(k, b, t, where, first):
        here = part(t * TILE, TILE)
        more = jnp.dot(
            nrm[b, k, here, :], wfull[part(k * 2 * wrows, 2 * wrows), where],
            preferred_element_type=jnp.float32,
        )
        proj[b, here, where] = more if first else proj[b, here, where] + more

    def cross_part(k, b, where, first):
        def tile(t, carry):
            cross_tile(k, b, t, where, first)
            return carry

        lax.fori_loop(0, rows // TILE, tile, 0)

    low = z < planes // 2
    order = [z, jnp.where(low, 1 - z, 5 - z), jnp.where(low, 2, 1), jnp.where(low, 3, 0)]
    every = pl.ds(0, cols)

    def chunks(b, t):
        def step(n, carry):
            cross_tile(jnp.where(n == 0, order[1], order[2]), b, t, every, False)
            return carry

        cross_tile(order[0], b, t, every, True)
        lax.fori_loop(0, 2, step, 0)

    first, second = (1, 0) if far else (y, yo)
    cache_c, query_c = pl.ds(half, 2 * kvw), pl.ds(0, half)

    def cache_out(b):
        cross_part(order[3], b, cache_c, False)
        kvc[b] = proj[b, :, cache_c].astype(jnp.bfloat16)

    def cache_first():
        for name, plane, cond in (("wf3", 0, z == last), ("wb3", last, z == 0)):
            arrived(name, wpart(plane, y), cond)
            arrived(name + "y", wpart(plane, yo), cond)
        cache_out(first)
        send("e1", kvc.at[first], kvc.at[2 + first], up, has_up)

    own_rows(0)
    own_rows(1)
    norm_half(y, 0)
    chunks(y, 0)
    from_x(2)
    from_far(0)
    from_far(1)
    from_x(3)
    other_rows(0)
    other_rows(1)
    norm_half(yo, 0)
    chunks(yo, 0)
    from_far(2)
    own_rows(2)
    own_rows(3)
    norm_half(y, 1)
    from_far(3)
    chunks(y, 1)
    if not far:
        cache_first()
    other_rows(2)
    other_rows(3)
    norm_half(yo, 1)
    chunks(yo, 1)
    if far:
        cache_first()
    cache_out(second)
    send("e0", kvc.at[second], kvc.at[2 + second], up, has_up)

    def query_out(b, carry):
        cross_part(order[3], b, query_c, False)
        for i in range(heads):
            cq[b, i] = proj[b, :, pl.ds(i * HEAD_DIM, HEAD_DIM)].astype(jnp.bfloat16)
        return carry

    lax.fori_loop(0, 2, query_out, 0)

    def own_diag(b, carry):
        diag(cq, cross_keys, all_heads(b))
        return carry

    lax.fori_loop(0, 2, own_diag, 0)

    def home_copy(i):
        return near("o", outs.at[y, i], out_hbm.at[:, own_head(i)], i)

    def away_copy(i):
        return remote("o", outs.at[yo, i], out_hbm.at[:, own_head(i)], to_y, i)

    plan = [(1, 0), (yo, 2 + first), (y, 2 + first)] + ([(0, 4)] if far else []) + [(yo, 2), (y, 2)]

    def look_up(n, which):
        value = plan[0][which]
        for at in range(1, len(plan)):
            value = jnp.where(n == at, plan[at][which], value)
        return value

    def step(n, carry):
        if far:
            @pl.when(jnp.logical_and(n == 0, has_down))
            def _():
                arrived("e1", kvc.at[2 + first])
                when(has_up, remote("er", kvc.at[3], kvc.at[4], up).start)

            when(jnp.logical_and(n == 3, far_down), lambda: arrived("er", kvc.at[4]))
            runs = jnp.where(n == 3, far_down, jnp.logical_or(n == 0, has_down))
        else:
            when(jnp.logical_and(n == 1, has_down), lambda: arrived("e1", kvc.at[2 + first]))
            runs = jnp.logical_or(n == 0, has_down)
        if far:
            when(jnp.logical_and(n == len(plan) - 2, has_down), lambda: arrived("e0", kvc.at[2 + second]))
        b, j = look_up(n, 0), look_up(n, 1)
        when(runs, lambda: off(cq, cross_keys, all_heads(b), j, rows))

        if not far:
            return carry

        @pl.when(n >= len(plan) - 2)
        def _():
            for i in range(heads):
                outs[b, i] = finish(b, i)
                when(n == len(plan) - 2, away_copy(i).start)
                when(n == len(plan) - 1, home_copy(i).start)

        return carry

    if far:
        lax.fori_loop(0, len(plan), step, 0)
    else:
        lax.fori_loop(0, len(plan) - 2, step, 0)
        arrived("e0", kvc.at[2 + second], has_down)

        def away(i):
            when(has_down, lambda: off(cq, cross_keys, [(yo, i)], 2 + second, rows))
            outs[yo, i] = finish(yo, i)
            away_copy(i).start()

        each_head(away)
        when(has_down, lambda: off(cq, cross_keys, all_heads(y), 2 + second, rows))
        for i in range(heads):
            outs[y, i] = finish(y, i)
            home_copy(i).start()
    if far:
        sends.append(("er", kvc.at[3], kvc.at[4], up, mid))

    for p in range(4):
        near(f"hid{p}", hpart(y, h_at, p), hid_hbm.at[pl.ds(p * quarter, quarter), :]).wait()
    for name, src, dst, device, cond in sends:
        when(cond, remote(name, src, dst, device).wait_send)

    def ended(i):
        for copy, cond in first_sends(i):
            when(cond, copy.wait_send)
        when(has_down, wb1_copy(i).wait_send)
        when(mid, wf2_copy(i).wait_send)
        when(has_down, qzy_copy(i).wait_send)
        when(has_up, ob_copy("ob", i).wait_send)
        when(has_up, ob_copy("obb", i).wait_send)
        when(has_up, lb_copy(i).wait_send)
        if far:
            when(mid, quu_copy(i).wait_send)
            for copy in o2_copies(i):
                when(has_far, copy.wait_send)
            for copy in o3_copies(i):
                when(mid, copy.wait_send)
        cy_copy(i).wait_send()
        cc_copy(i).wait_send()
        cyc_copy(i).wait_send()
        home_copy(i).wait()
        away_copy(i).wait_send()
        arrived("o", out_hbm.at[:, other_head(i)], None, i)

    each_head(ended)


def settle_kernel(hid_ref, out_ref, hid_to, out_to):
    hid_to[...] = hid_ref[...]
    out_to[...] = out_ref[...]


def settled(hid, out):
    rows, width = hid.shape
    spec = pl.BlockSpec((rows // 2, width), lambda i: (i, 0))
    return pl.pallas_call(
        settle_kernel,
        out_shape=(jax.ShapeDtypeStruct(hid.shape, hid.dtype),) * 2,
        grid=(2,),
        in_specs=[spec, spec],
        out_specs=(spec, spec),
        compiler_params=pltpu.CompilerParams(vmem_limit_bytes=60 * 1024 * 1024),
    )(hid, out)


def fused(far, residual, q_self, k_self, v_self, w_out, norm_gain, w_query, w_cache, block_doc, tail_len):
    rows, width = q_self.shape
    seq_size, head_size = lax.axis_size("seq"), lax.axis_size("head")
    half = width // 2
    heads = half // HEAD_DIM
    kvw = w_cache.shape[1] // 4
    cols = half + 2 * kvw
    bf, f32 = jnp.bfloat16, jnp.float32
    hbm = pl.BlockSpec(memory_space=pl.ANY)
    smem = pl.BlockSpec(memory_space=pltpu.SMEM)
    by_head = BY_HEAD + (FAR_BY_HEAD if far else ())
    copies = len(by_head) * heads + len(COPIES)
    scratch = [
        pltpu.VMEM((2, heads, rows, HEAD_DIM), bf),
        pltpu.VMEM((2, heads, 2, rows, HEAD_DIM), bf),
        pltpu.VMEM((2, heads, rows, HEAD_DIM), bf),
        pltpu.VMEM((heads, 2, rows, HEAD_DIM), bf),
        pltpu.VMEM((heads, 2, rows, HEAD_DIM), bf),
        pltpu.VMEM((rows, HEAD_DIM), f32),
        pltpu.VMEM((2 * heads, 8, rows), f32),
        pltpu.VMEM((heads, HEAD_DIM, rows), f32),
        pltpu.VMEM((heads, rows, HEAD_DIM), bf),
        pltpu.VMEM((heads, rows, HEAD_DIM), bf),
        pltpu.VMEM((heads, rows, HEAD_DIM), bf),
        pltpu.VMEM((heads, rows, HEAD_DIM), bf),
        pltpu.VMEM((heads, 8, rows), f32),
        pltpu.VMEM((heads, HEAD_DIM, rows), f32),
        pltpu.VMEM((2, heads, rows, 2 * HEAD_DIM), f32),
        pltpu.VMEM((2, heads, rows, HEAD_DIM), f32),
        pltpu.VMEM((2, 2, width, width), bf),
        pltpu.VMEM((w_query.shape[0] * seq_size, cols), bf),
        pltpu.VMEM((2, 2, rows, half), bf),
        pltpu.VMEM((rows, half), bf),
        pltpu.VMEM((rows, width), f32),
        pltpu.VMEM((rows, width), f32),
        pltpu.VMEM((rows, width), bf),
        pltpu.VMEM((rows, width), bf),
        pltpu.VMEM((2, head_size, rows, width), bf),
        pltpu.VMEM((2, head_size, rows, width), bf),
        pltpu.VMEM((rows, width), bf),
        pltpu.VMEM((1, head_size * width), f32),
        pltpu.VMEM((2, rows, cols), f32),
        pltpu.VMEM((2, heads, rows, HEAD_DIM), bf),
        pltpu.VMEM((5 if far else 4, rows, 2 * kvw), bf),
        pltpu.VMEM((2, heads, rows, HEAD_DIM), bf),
        pltpu.SemaphoreType.DMA((copies,)),
        pltpu.SemaphoreType.DMA((copies,)),
        pltpu.SemaphoreType.DMA((len(LOCALS) + len(LOCALS_BY_HEAD) * heads,)),
    ]
    wide = jax.ShapeDtypeStruct((rows, width), bf)
    return pl.pallas_call(
        functools.partial(fused_kernel, far),
        out_shape=(wide, wide),
        in_specs=[hbm] * 8 + [smem] * 2,
        out_specs=(hbm, hbm),
        scratch_shapes=scratch,
        compiler_params=pltpu.CompilerParams(
            collective_id=1 if far else 0, has_side_effects=True, vmem_limit_bytes=60 * 1024 * 1024
        ),
    )(
        residual, q_self, k_self, v_self, w_out, norm_gain.reshape(1, head_size * width),
        w_query, w_cache, block_doc, tail_len,
    )


def chosen(*args):
    block_doc = args[8]
    at = np.arange(block_doc.shape[0])
    apart = (at[None, :] - at[:, None] == 3) & (at[None, :] % 2 == 0)
    far = jnp.any((block_doc[:, None] == block_doc[None, :]) & apart)
    hid, out = lax.cond(far, functools.partial(fused, True), functools.partial(fused, False), *args)
    return settled(hid, out)


def stage_kernel(offsets, window, first, last, facts, q_ref, *refs):
    pairs = [(refs[2 * i], refs[2 * i + 1]) for i in range(len(offsets))]
    rest = refs[2 * len(offsets):]
    if not first:
        acc_in, peak_in, total_in = rest[:3]
        rest = rest[3:]
    if last:
        out_ref = rest[0]
        acc, peak, total = rest[1:]
    else:
        acc, peak, total = rest
    rows = q_ref.shape[0]
    tile = min(ROW_TILE, rows)
    scaling = math.log2(math.e) / math.sqrt(HEAD_DIM)

    def scores_of(r, k):
        return lax.dot_general(
            q_ref[pl.ds(r, tile), :], k, (((1,), (1,)), ((), ())),
            preferred_element_type=jnp.float32,
        )

    if not first:
        acc[...] = acc_in[...]
        peak[...] = peak_in[...]
        total[...] = total_in[...]

    for (k_ref, v_ref), (flag, offset) in zip(pairs, offsets):

        def one(offset=offset, k_ref=k_ref, v_ref=v_ref):
            for r in range(0, rows, tile):
                here = pl.ds(r, tile)
                keys = r + tile if offset == 0 else rows
                s = scores_of(r, k_ref[pl.ds(0, keys), :])
                if offset == 0:
                    q_at = r + lax.broadcasted_iota(jnp.int32, s.shape, 0)
                    k_at = lax.broadcasted_iota(jnp.int32, s.shape, 1)
                    s = jnp.where((k_at <= q_at) & (k_at < facts[0]), s, -1e30)
                elif offset * rows + rows - 1 >= window:
                    q_at = r + lax.broadcasted_iota(jnp.int32, s.shape, 0)
                    k_at = lax.broadcasted_iota(jnp.int32, s.shape, 1)
                    s = jnp.where(offset * rows + q_at - k_at < window, s, -1e30)
                top = jnp.max(s, axis=1, keepdims=True)
                if offset == 0:
                    w = jnp.exp2((s - top) * scaling)
                    part = jnp.dot(
                        w.astype(jnp.bfloat16), v_ref[pl.ds(0, keys), :],
                        preferred_element_type=jnp.float32,
                    )
                    acc[here, :] = part
                    total[here, :] = jnp.broadcast_to(
                        jnp.sum(w, axis=1, keepdims=True), (tile, HEAD_DIM)
                    )
                    peak[here, :] = jnp.broadcast_to(top, (tile, HEAD_DIM))
                else:
                    old = peak[here, :]
                    new = jnp.maximum(old, top)
                    w = jnp.exp2((s - new[:, :1]) * scaling)
                    fade = jnp.exp2((old - new) * scaling)
                    part = jnp.dot(
                        w.astype(jnp.bfloat16), v_ref[...], preferred_element_type=jnp.float32
                    )
                    acc[here, :] = acc[here, :] * fade + part
                    total[here, :] = total[here, :] * fade + jnp.sum(w, axis=1, keepdims=True)
                    peak[here, :] = new

        if offset == 0:
            one()
        else:
            pl.when(facts[flag] > 0)(one)

    if last:
        out_ref[...] = (acc[...] / total[...]).astype(jnp.bfloat16)


def attend_stage(facts, queries, blocks, offsets, kv_heads, state, window, last):
    rows, width = queries.shape
    heads = width // HEAD_DIM
    group = heads // kv_heads
    tall = pl.BlockSpec((rows, HEAD_DIM), lambda h, f: (0, h))
    key_spec = pl.BlockSpec((rows, HEAD_DIM), lambda h, f: (0, h // group))
    value_spec = pl.BlockSpec((rows, HEAD_DIM), lambda h, f: (0, kv_heads + h // group))
    operands, specs = [queries], [tall]
    for block in blocks:
        operands += [block, block]
        specs += [key_spec, value_spec]
    if state is not None:
        operands += list(state)
        specs += [tall] * 3
    wide = jax.ShapeDtypeStruct((rows, width), jnp.float32)
    if last:
        out_shape = jax.ShapeDtypeStruct((rows, width), jnp.bfloat16)
        out_specs = tall
        scratch = [pltpu.VMEM((rows, HEAD_DIM), jnp.float32)] * 3
    else:
        out_shape, out_specs, scratch = (wide,) * 3, (tall,) * 3, []
    flops = 4 * rows * rows * width * len(offsets) * 3
    return pl.pallas_call(
        functools.partial(stage_kernel, offsets, window, state is None, last),
        out_shape=out_shape,
        grid_spec=pltpu.PrefetchScalarGridSpec(
            num_scalar_prefetch=1, grid=(heads,), in_specs=specs, out_specs=out_specs,
            scratch_shapes=scratch,
        ),
        compiler_params=pltpu.CompilerParams(
            dimension_semantics=("arbitrary",), vmem_limit_bytes=32 * 1024 * 1024
        ),
        cost_estimate=pl.CostEstimate(
            flops=flops, bytes_accessed=rows * width * 2 * (2 + 2 * len(offsets)),
            transcendentals=0,
        ),
    )(facts, *operands)


def shared_over_head(block):
    size = lax.axis_size("head")
    held = [block]
    step = size // 2
    got = {0: block}
    while step >= 1:
        for flip in sorted(got):
            got[flip ^ step] = None if got[flip] is None else swapped(got[flip], "head", step)
        step //= 2
    held = [got[flip] for flip in range(size)]
    return held


def sent(block, routes):
    return lax.ppermute(block, "seq", routes)


def row_gather(block):
    size = lax.axis_size("seq")
    me = lax.axis_index("seq")
    ring = [(i, (i + 2) % size) for i in range(size)]
    steps = []
    moving = block
    for step in range(size // 2):
        owner = lax.rem(me - 2 * step + size, size)
        across = swapped(moving, "seq", 1)
        onward = sent(moving, ring) if step + 1 < size // 2 else None
        moving, across, onward = yield moving, across, onward, owner
        moving = onward


def placed(whole, piece, owner):
    return lax.dynamic_update_slice_in_dim(whole, piece, owner * piece.shape[0], 0)


def waves(block, odd, beside):
    size = lax.axis_size("seq")
    first = sent(block, [(i, i + 1) for i in range(size - 1)])
    second_even = sent(block, [(i, i + 2) for i in range(0, size - 2, 2)])
    if beside is not None:
        first, beside = lax.optimization_barrier((first, beside))
    mixed = jnp.where(odd, block, first)
    second = sent(mixed, [(i, i + 2) for i in range(size - 2)])
    third_odd = sent(second_even, [(i, i + 1) for i in range(2, size, 2)])
    return first, [second_even, second, third_odd], beside


def fits(q_self, w_cache):
    seq_size, head_size = lax.axis_size("seq"), lax.axis_size("head")
    return (
        seq_size == 8 and head_size == 4 and q_self.shape[1] == 6 * HEAD_DIM
        and w_cache.shape[1] == 4 * HEAD_DIM and q_self.shape[0] % TILE == 0
    )


def local(
    residual, q_self, k_self, v_self, w_out, norm_gain, w_query, w_cache, block_doc, tail_len
):
    rows, width = q_self.shape
    local_heads = width // HEAD_DIM
    if fits(q_self, w_cache):
        return chosen(
            residual, q_self, k_self, v_self, w_out, norm_gain, w_query, w_cache, block_doc, tail_len
        )
    local_kv = w_cache.shape[1] // (2 * HEAD_DIM)
    seq_size, head_size = lax.axis_size("seq"), lax.axis_size("head")
    span = min(DOC_BLOCKS, seq_size // 2)
    far = list(range(1, span))
    me, my_head = lax.axis_index("seq"), lax.axis_index("head")

    own_doc = block_doc[me]
    following = jnp.where(me == seq_size - 1, -1, block_doc[jnp.minimum(me + 1, seq_size - 1)])
    live = jnp.where(following != own_doc, jnp.minimum(tail_len[me], rows), rows)
    odd = lax.rem(me, 2) == 1
    small = span == 4 and seq_size % 2 == 0

    def together(distance):
        other = me - distance
        return jnp.logical_and(other >= 0, block_doc[jnp.maximum(other, 0)] == own_doc)

    if small:
        flags = [
            together(1),
            jnp.logical_and(jnp.logical_not(odd), together(2)),
            jnp.where(odd, together(2), together(3)),
            jnp.logical_and(odd, together(3)),
        ]
        distances = [1, 2, 3, 3]
    else:
        flags = [together(distance) for distance in far]
        distances = far
    facts = jnp.stack([live.astype(jnp.int32)] + [flag.astype(jnp.int32) for flag in flags])
    slots = [(1 + i, distance) for i, distance in enumerate(distances)]

    stacked = jnp.concatenate([k_self, v_self], axis=1)
    weight_rows = jnp.concatenate([w_query, w_cache], axis=1)
    state = attend_stage(facts, q_self, [stacked], [(0, 0)], local_heads, None, WINDOW, False)
    if small:
        near, late, state = waves(stacked, odd, state)
    else:
        near, *late = [passed_along(stacked, "seq", offset) for offset in far]

    own_columns = residual.shape[1]
    out_pieces = []
    for flip in range(head_size):
        piece = lax.dynamic_slice_in_dim(w_out, (my_head ^ flip) * own_columns, own_columns, 1)
        out_pieces.append(piece if flip == 0 else swapped(piece, "head", flip))

    state = attend_stage(facts, q_self, [near], slots[:1], local_heads, state, WINDOW, False)
    if small:
        weight_rows, state = lax.optimization_barrier((weight_rows, state))
        weights = jnp.zeros((weight_rows.shape[0] * seq_size, weight_rows.shape[1]), jnp.bfloat16)
        gather = row_gather(weight_rows)
        moving, across, onward, owner = next(gather)
        late, across, onward, out_pieces = lax.optimization_barrier(
            (late, across, onward, out_pieces)
        )
        weights = placed(placed(weights, moving, owner), across, owner ^ 1)
        moving, across, onward, owner = gather.send((moving, across, onward))
    else:
        weights = lax.all_gather(weight_rows, "seq", axis=0, tiled=True)
    context = attend_stage(facts, q_self, late, slots[1:], local_heads, state, WINDOW, True)
    if small:
        context, across, onward = lax.optimization_barrier((context, across, onward))
        weights = placed(placed(weights, moving, owner), across, owner ^ 1)
        moving, across, onward, owner = gather.send((moving, across, onward))

    contexts = shared_over_head(context)
    projected = jnp.dot(contexts[0], out_pieces[0], preferred_element_type=jnp.float32)
    for flip in range(1, head_size):
        projected += jnp.dot(contexts[flip], out_pieces[flip], preferred_element_type=jnp.float32)
    hidden = (residual.astype(jnp.float32) + projected).astype(jnp.bfloat16)
    if small:
        hidden, across, onward = lax.optimization_barrier((hidden, across, onward))
        weights = placed(placed(weights, moving, owner), across, owner ^ 1)
        while onward is not None:
            moving, across, onward, owner = gather.send((moving, across, onward))
            weights = placed(placed(weights, moving, owner), across, owner ^ 1)

    full = jnp.zeros((rows, own_columns * head_size), jnp.bfloat16)
    for flip, piece in enumerate(shared_over_head(hidden)):
        full = lax.dynamic_update_slice_in_dim(full, piece, (my_head ^ flip) * own_columns, 1)
    wide = full.astype(jnp.float32)
    mean_square = jnp.sum(wide * wide, axis=1, keepdims=True) / D
    normed = (wide * lax.rsqrt(mean_square + EPSILON) * norm_gain).astype(jnp.bfloat16)

    cache_rows = jnp.dot(
        normed, weights[:, width:], preferred_element_type=jnp.float32
    ).astype(jnp.bfloat16)
    if small:
        near, late, _ = waves(cache_rows, odd, None)
    else:
        near, *late = [passed_along(cache_rows, "seq", offset) for offset in far]
    cross_queries = jnp.dot(
        normed, weights[:, :width], preferred_element_type=jnp.float32
    ).astype(jnp.bfloat16)
    reach = DOC_BLOCKS * rows
    state = attend_stage(
        facts, cross_queries, [cache_rows, near], [(0, 0)] + slots[:1], local_kv, None, reach, False
    )
    cross_context = attend_stage(
        facts, cross_queries, late, slots[1:], local_kv, state, reach, True
    )
    return (hidden, cross_context)


def solution(mesh):
    in_specs = (
        P("seq", "head"),
        P("seq", "head"),
        P("seq", "head"),
        P("seq", "head"),
        P("head", None),
        P(),
        P("seq", "head"),
        P("seq", "head"),
        P(),
        P(),
    )
    out_specs = (P("seq", "head"), P("seq", "head"))
    return jax.shard_map(local, mesh=mesh, in_specs=in_specs, out_specs=out_specs, check_vma=False)
```
